16 devices in a mesh: dp: 2 (over y, z), w: 8 (over x, core).
Axes of the slice: x: 4, y: 2, z: 1, core: 2. Of those that a mesh axis runs over, the one named last changes fastest.
The devices are a block of a 4x4x8 slice.
Arguments:
- hidden: bfloat16 [2048, 1152], P(('dp', 'w')), parts along dimension 0
- positions: int32 [2048], P(('dp', 'w')), parts along dimension 0
- k_cache: bfloat16 [2, 2048, 1, 128, 256], P(None, ('dp', 'w')), parts along dimension 1
- v_cache: bfloat16 [2, 2048, 1, 128, 256], P(None, ('dp', 'w')), parts along dimension 1
- attn_norm: float32 [2, 1152], P(None, 'w')
- w_query: bfloat16 [2, 1152, 1024], P(None, 'w')
- w_key: bfloat16 [2, 1152, 256], P(None, 'w')
- w_value: bfloat16 [2, 1152, 256], P(None, 'w')
- w_out: bfloat16 [2, 1024, 1152], P(None, 'w')
- mlp_norm: float32 [2, 1152], P(None, 'w')
- w_gate: bfloat16 [2, 1152, 6912], P(None, 'w')
- w_up: bfloat16 [2, 1152, 6912], P(None, 'w')
- w_down: bfloat16 [2, 6912, 1152], P(None, 'w')
Outputs:
- output 1: bfloat16 [2048, 1152], P(('dp', 'w')), parts along dimension 0
- output 2: bfloat16 [2, 2048, 1, 128, 256], P(None, ('dp', 'w')), parts along dimension 1
- output 3: bfloat16 [2, 2048, 1, 128, 256], P(None, ('dp', 'w')), parts along dimension 1
There are 2 independent parts. The reference program is written for one: setup_inputs(seed, part) draws one part's arguments, and reference() takes and returns one part's arrays. A program takes and returns all parts, laid end to end along the dimension named above; an argument that names none is the same for every part.
All inputs are finite; a program needn't handle non-finite values.
Results may differ from the reference program's by a relative error of at most 0.0169962.
Values are sent between devices in bfloat16 or wider.
A program may use at most 768 MiB of HBM per device.

```python
import jax
import jax.numpy as jnp
from jax import lax

D = 1152
HEADS = 4
KV_HEADS = 1
HEAD = 256
FF = 6912
BATCH = 1024
SMAX = 128
LAYERS = 2

EPS = 1e-6
ROPE_BASE = 10000.0
Q_DIM = HEADS * HEAD
KV_DIM = KV_HEADS * HEAD
GROUP = HEADS // KV_HEADS


def setup_inputs(seed: int = 0, part: int = 0) -> dict:
    base_key = jax.random.key(seed)
    part_keys = jax.random.split(jax.random.fold_in(base_key, part), 4)
    shared_keys = jax.random.split(jax.random.fold_in(base_key, 65537), 9)
    hidden = jax.random.normal(part_keys[0], (BATCH, D), jnp.float32).astype(jnp.bfloat16)
    positions = jax.random.randint(part_keys[1], (BATCH,), 0, SMAX, jnp.int32)
    positions = positions.at[0].set(SMAX - 1).at[1].set(0)
    cache_shape = (LAYERS, BATCH, KV_HEADS, SMAX, HEAD)
    k_cache = jax.random.normal(part_keys[2], cache_shape, jnp.float32).astype(jnp.bfloat16)
    v_cache = jax.random.normal(part_keys[3], cache_shape, jnp.float32).astype(jnp.bfloat16)

    def weight(key_w, n_rows, n_cols):
        raw_draw = jax.random.normal(key_w, (LAYERS, n_rows, n_cols), jnp.float32)
        return (raw_draw * n_rows ** -0.5).astype(jnp.bfloat16)

    return {
        "hidden": hidden,
        "positions": positions,
        "k_cache": k_cache,
        "v_cache": v_cache,
        "attn_norm": 0.3 * jax.random.normal(shared_keys[0], (LAYERS, D), jnp.float32),
        "w_query": weight(shared_keys[1], D, Q_DIM),
        "w_key": weight(shared_keys[2], D, KV_DIM),
        "w_value": weight(shared_keys[3], D, KV_DIM),
        "w_out": weight(shared_keys[4], Q_DIM, D),
        "mlp_norm": 0.3 * jax.random.normal(shared_keys[5], (LAYERS, D), jnp.float32),
        "w_gate": weight(shared_keys[6], D, FF),
        "w_up": weight(shared_keys[7], D, FF),
        "w_down": weight(shared_keys[8], FF, D),
    }


def rms_norm(hidden, gain):
    hid_f32 = hidden.astype(jnp.float32)
    mean_sq = jnp.mean(hid_f32 * hid_f32, axis=-1, keepdims=True)
    return (hid_f32 * lax.rsqrt(mean_sq + EPS) * (1.0 + gain)).astype(jnp.bfloat16)


def rope_tables(positions):
    half_dim = HEAD // 2
    inv_freq = ROPE_BASE ** (-2.0 * jnp.arange(half_dim, dtype=jnp.float32) / HEAD)
    angles = positions.astype(jnp.float32)[:, None] * inv_freq[None, :]
    return jnp.cos(angles), jnp.sin(angles)


def apply_rope(vectors, cos_tab, sin_tab):
    half_dim = vectors.shape[-1] // 2
    lead_half = vectors[..., :half_dim]
    tail_half = vectors[..., half_dim:]
    cos_b = cos_tab[:, None, :]
    sin_b = sin_tab[:, None, :]
    return jnp.concatenate([lead_half * cos_b - tail_half * sin_b, tail_half * cos_b + lead_half * sin_b], axis=-1)


def decoder_layer(hidden, params, positions, cos_tab, sin_tab):
    gain_attn, w_query, w_key, w_value, w_out, gain_mlp, w_gate, w_up, w_down, k_layer, v_layer = params
    batch_rows = hidden.shape[0]
    normed = rms_norm(hidden, gain_attn)
    q_proj = jnp.dot(normed, w_query, preferred_element_type=jnp.float32).reshape(batch_rows, HEADS, HEAD)
    k_proj = jnp.dot(normed, w_key, preferred_element_type=jnp.float32).reshape(batch_rows, KV_HEADS, HEAD)
    v_proj = jnp.dot(normed, w_value, preferred_element_type=jnp.float32).reshape(batch_rows, KV_HEADS, HEAD)
    q_rot = (apply_rope(q_proj, cos_tab, sin_tab) * HEAD ** -0.5).astype(jnp.bfloat16)
    q_rot = q_rot.reshape(batch_rows, KV_HEADS, GROUP, HEAD)
    k_rot = apply_rope(k_proj, cos_tab, sin_tab).astype(jnp.bfloat16)
    v_new = v_proj.astype(jnp.bfloat16)
    cache_steps = jnp.arange(SMAX)
    write_mask = (cache_steps[None, :] == positions[:, None])[:, None, :, None]
    k_layer = jnp.where(write_mask, k_rot[:, :, None, :], k_layer)
    v_layer = jnp.where(write_mask, v_new[:, :, None, :], v_layer)
    scores = jnp.einsum("bkge,bkse->bkgs", q_rot.astype(jnp.float32), k_layer.astype(jnp.float32))
    is_valid = cache_steps[None, None, None, :] <= positions[:, None, None, None]
    scores = jnp.where(is_valid, scores, -1e30)
    row_max = jnp.max(scores, axis=-1, keepdims=True)
    attn_prob = jnp.exp(scores - row_max)
    row_sum = jnp.sum(attn_prob, axis=-1, keepdims=True)
    attn_vals = jnp.einsum("bkgs,bkse->bkge", attn_prob.astype(jnp.bfloat16).astype(jnp.float32), v_layer.astype(jnp.float32))
    attn_vals = (attn_vals / row_sum).astype(jnp.bfloat16).reshape(batch_rows, Q_DIM)
    hid_mid = (hidden.astype(jnp.float32) + jnp.dot(attn_vals, w_out, preferred_element_type=jnp.float32)).astype(jnp.bfloat16)
    normed_mlp = rms_norm(hid_mid, gain_mlp)
    gate_pre = jnp.dot(normed_mlp, w_gate, preferred_element_type=jnp.float32)
    up_pre = jnp.dot(normed_mlp, w_up, preferred_element_type=jnp.float32)
    mlp_hidden = (jax.nn.gelu(gate_pre, approximate=True) * up_pre).astype(jnp.bfloat16)
    hid_out = (hid_mid.astype(jnp.float32) + jnp.dot(mlp_hidden, w_down, preferred_element_type=jnp.float32)).astype(jnp.bfloat16)
    return hid_out, (k_layer, v_layer)


def reference(hidden, positions, k_cache, v_cache, attn_norm, w_query, w_key, w_value, w_out, mlp_norm, w_gate, w_up, w_down):
    cos_tab, sin_tab = rope_tables(positions)

    def layer_step(hid_carry, params):
        return decoder_layer(hid_carry, params, positions, cos_tab, sin_tab)

    layer_params = (attn_norm, w_query, w_key, w_value, w_out, mlp_norm, w_gate, w_up, w_down, k_cache, v_cache)
    hidden_out, caches_out = lax.scan(layer_step, hidden, layer_params)
    return hidden_out, caches_out[0], caches_out[1]
```

```python
import functools

import jax
import jax.numpy as jnp
from jax import lax
from jax.experimental import pallas as pl
from jax.experimental.pallas import tpu as pltpu
from jax.sharding import PartitionSpec as P

EPS = 1e-6
ROPE_BASE = 10000.0
LANES = 128
CORES = 2
CHIPS = 4
SEQ_GROUP = 32
MESH = pl.DeviceIdType.MESH
F32 = jnp.float32
BF16 = jnp.bfloat16


def rope_tables(positions, head_dim):
    half_dim = head_dim // 2
    inv_freq = ROPE_BASE ** (-2.0 * jnp.arange(half_dim, dtype=jnp.float32) / head_dim)
    angles = positions.astype(jnp.float32)[:, None] * inv_freq[None, :]
    return jnp.cos(angles), jnp.sin(angles)


def dot(a, b):
    return jnp.dot(a, b, preferred_element_type=F32)


def dot_t(a, b):
    return lax.dot_general(a, b, (((1,), (1,)), ((), ())), preferred_element_type=F32)


def decode_kernel(
    dims,
    hid_ref, cos_ref, sin_ref, gain_ref, pos_ref, kc_ref, vc_ref,
    wq_ref, wk_ref, wv_ref, wo_ref, wg_ref, wu_ref, wd_ref,
    out_ref, knew_ref, vnew_ref,
    gbuf, abuf_w, bbuf_w, gu_w, wd_w, tr_w, y_all, m_buf, part, r_t, r_f,
    kbuf, vbuf, qbuf, abuf, hbuf,
    send_sem, recv_sem, loc_sem, kv_sem,
):
    layers, rows, width, heads, head_dim, cache_len, n_dev, ff = dims
    half = head_dim // 2
    piece = width // n_dev
    chip_cols = ff // CHIPS
    win = gu_w.shape[-1]
    pad = win - chip_cols
    wd_rows = wd_ref.shape[1]
    q_half = wq_ref.shape[-1] // 2
    kv_half = head_dim // 2
    groups = rows // SEQ_GROUP
    w = lax.axis_index("w")
    dp = lax.axis_index("dp")
    x, c = lax.div(w, CORES), lax.rem(w, CORES)
    h = lax.rem(dp, 2)
    xr, xo, xl = lax.rem(x + 1, CHIPS), lax.rem(x + 2, CHIPS), lax.rem(x + 3, CHIPS)
    right, left = (dp, xr * CORES + c), (dp, xl * CORES + c)
    twin = (dp, x * CORES + 1 - c)
    pair = (dp + 1 - 2 * h, w)

    msg_ids = {}
    pending = []

    def mid(name):
        return msg_ids.setdefault(name, len(msg_ids))

    def put(name, pairs, dev):
        for src, dst in pairs:
            pltpu.make_async_remote_copy(src, dst, send_sem.at[mid(name)], recv_sem.at[mid(name)], device_id=dev, device_id_type=MESH).start()

    def send(name, pairs, dev, view=None):
        put(name, pairs, dev)
        pending.append((name, pairs[0][0] if view is None else view))

    def got(name, view):
        pltpu.make_async_remote_copy(view, view, send_sem.at[mid(name)], recv_sem.at[mid(name)], device_id=right, device_id_type=MESH).wait_recv()

    def sent(name, view):
        pltpu.make_async_remote_copy(view, view, send_sem.at[mid(name)], recv_sem.at[mid(name)], device_id=right, device_id_type=MESH).wait_send()

    def drain():
        for name, view in pending:
            sent(name, view)
        pending.clear()

    def col_start(xx):
        return pl.multiple_of(lax.div(chip_cols * xx, LANES) * LANES, LANES)

    def wd_at(layer, cc):
        offset = lax.rem(chip_cols * x, LANES) + wd_rows * cc
        return wd_w.at[layer, pl.ds(pl.multiple_of(offset, 32), wd_rows), :]

    def a_pairs(l):
        out = []
        for hf in range(2):
            dst = abuf_w.at[l, hf, x, c]
            out.append((wq_ref.at[l, :, pl.ds(hf * q_half, q_half)], dst.at[:, pl.ds(0, q_half)]))
            out.append((wk_ref.at[l, :, pl.ds(hf * kv_half, kv_half)], dst.at[:, pl.ds(q_half, kv_half)]))
            out.append((wv_ref.at[l, :, pl.ds(hf * kv_half, kv_half)], dst.at[:, pl.ds(q_half + kv_half, kv_half)]))
        return out

    def local_start(sem, pairs):
        for src, dst in pairs:
            pltpu.make_async_copy(src, dst, loc_sem.at[sem]).start()

    def local_wait(sem, view):
        pltpu.make_async_copy(view, view, loc_sem.at[sem]).wait()

    def kv_copies(i, slot):
        layer, group = lax.div(i, groups), lax.rem(i, groups)
        seqs = pl.ds(group * SEQ_GROUP, SEQ_GROUP)
        return (
            pltpu.make_async_copy(kc_ref.at[layer, seqs, 0], kbuf.at[slot], kv_sem.at[slot, 0]),
            pltpu.make_async_copy(vc_ref.at[layer, seqs, 0], vbuf.at[slot], kv_sem.at[slot, 1]),
        )

    def kv_start(i, slot):
        for copy in kv_copies(i, slot):
            copy.start()

    def a_own(l):
        for name, dev in (("aR", right), ("aL", left)):
            send(f"{name}{l}", a_pairs(l), dev, abuf_w.at[l, :, x, c])

    def a_forward(l):
        got(f"aR{l}", abuf_w.at[l, :, xl, c])
        view = abuf_w.at[l, 0, xl, c]
        send(f"afR{l}", [(view, view)], right)
        got(f"aL{l}", abuf_w.at[l, :, xr, c])
        view = abuf_w.at[l, 1, xr, c]
        send(f"afL{l}", [(view, view)], left)

    def a_twin(l):
        got(f"afR{l}", abuf_w.at[l, 0, xo, c])
        got(f"afL{l}", abuf_w.at[l, 1, xo, c])
        local_wait(4 * l, abuf_w.at[l, :, x, c])
        view = abuf_w.at[l, :, :, c]
        send(f"aT{l}", [(view, view)], twin)

    def a_ready(l):
        got(f"aT{l}", abuf_w.at[l, :, :, 1 - c])

    def b_own(l):
        dst = bbuf_w.at[l, x, c]
        for name, dev in (("bR", right), ("bL", left)):
            send(f"{name}{l}", [(wo_ref.at[l], dst)], dev)

    def b_forward(l):
        mid_row = bbuf_w.shape[3] // 2
        got(f"bR{l}", bbuf_w.at[l, xl, c])
        view = bbuf_w.at[l, xl, c, pl.ds(0, mid_row)]
        send(f"bfR{l}", [(view, view)], right)
        got(f"bL{l}", bbuf_w.at[l, xr, c])
        view = bbuf_w.at[l, xr, c, pl.ds(mid_row, mid_row)]
        send(f"bfL{l}", [(view, view)], left)

    def b_twin(l):
        mid_row = bbuf_w.shape[3] // 2
        got(f"bfR{l}", bbuf_w.at[l, xo, c, pl.ds(0, mid_row)])
        got(f"bfL{l}", bbuf_w.at[l, xo, c, pl.ds(mid_row, mid_row)])
        local_wait(4 * l + 1, bbuf_w.at[l, x, c])
        view = bbuf_w.at[l, :, c]
        send(f"bT{l}", [(view, view)], twin)

    def b_ready(l):
        got(f"bT{l}", bbuf_w.at[l, :, 1 - c])

    def by_matrix(l, name, xx, lo, size, dst, dev):
        cols = pl.ds(pl.multiple_of(col_start(xx) + lo, LANES), size)
        for value, ref in ((0, wg_ref), (1, wu_ref)):
            @pl.when(h == value)
            def _():
                put(name, [(ref.at[l, :, cols], dst)], dev)
        pending.append((name, dst))

    def c_direct(l):
        by_matrix(l, f"cR{l}", xr, 0, win, gu_w.at[l, h, x, c], right)
        by_matrix(l, f"cL{l}", xl, 0, win, gu_w.at[l, h, x, c], left)

    def c_transit(l):
        by_matrix(l, f"tR{l}", xo, 0, win // 2, tr_w.at[l, 0], right)
        by_matrix(l, f"tL{l}", xo, win // 2, win // 2, tr_w.at[l, 1], left)

    def c_forward(l):
        got(f"tR{l}", tr_w.at[l, 0])
        send(f"cfR{l}", [(tr_w.at[l, 0], gu_w.at[l, h, xl, c, :, pl.ds(0, win // 2)])], right)
        got(f"tL{l}", tr_w.at[l, 1])
        send(f"cfL{l}", [(tr_w.at[l, 1], gu_w.at[l, h, xr, c, :, pl.ds(win // 2, win // 2)])], left)

    def c_pair_near(l):
        for name, xx in (("cR", xl), ("cL", xr)):
            view = gu_w.at[l, h, xx, c]
            got(f"{name}{l}", view)
            send(f"p{name}{l}", [(view, view)], pair)

    def c_pair_far(l):
        got(f"cfR{l}", gu_w.at[l, h, xo, c, :, pl.ds(0, win // 2)])
        got(f"cfL{l}", gu_w.at[l, h, xo, c, :, pl.ds(win // 2, win // 2)])
        view = gu_w.at[l, h, xo, c]
        send(f"pcF{l}", [(view, view)], pair)
        local_wait(4 * l + 2, gu_w.at[l, :, x, c])
        view = gu_w.at[l, h, :, c]
        send(f"cT0{l}", [(view, view)], twin)

    def c_twin(l):
        got(f"pcR{l}", gu_w.at[l, 1 - h, xl, c])
        got(f"pcL{l}", gu_w.at[l, 1 - h, xr, c])
        got(f"pcF{l}", gu_w.at[l, 1 - h, xo, c])
        view = gu_w.at[l, 1 - h, :, c]
        send(f"cT1{l}", [(view, view)], twin)

    def c_ready(l):
        got(f"cT0{l}", gu_w.at[l, h, :, 1 - c])
        got(f"cT1{l}", gu_w.at[l, 1 - h, :, 1 - c])

    def d_twin(l):
        send(f"dT{l}", [(wd_ref.at[l], wd_at(l, c))], twin)

    def d_ready(l):
        local_wait(4 * l + 3, wd_at(l, c))
        got(f"dT{l}", wd_at(l, 1 - c))

    for l in range(layers):
        start = pl.multiple_of(jnp.where(lax.rem(x, 2) == 0, chip_cols, 0), 64)
        wd_w[l, pl.ds(start, pad), :] = jnp.zeros((pad, width), BF16)
    barrier = pltpu.get_barrier_semaphore()
    for i in range(1, n_dev):
        pl.semaphore_signal(barrier, inc=1, device_id=(dp, lax.rem(w + i, n_dev)), device_id_type=MESH)
    pl.semaphore_signal(barrier, inc=1, device_id=pair, device_id_type=MESH)
    pl.semaphore_wait(barrier, n_dev)

    for i in range(1, n_dev):
        put("gain", [(gain_ref, gbuf.at[w])], (dp, lax.rem(w + i, n_dev)))
    pending.append(("gain", gbuf.at[pl.ds(0, n_dev - 1)]))
    a_own(0)
    b_own(0)
    gain_copy = pltpu.make_async_copy(gain_ref, gbuf.at[w], loc_sem.at[4 * layers])
    gain_copy.start()
    kv_start(0, 0)
    for l in range(layers):
        local_start(4 * l, a_pairs(l))
        local_start(4 * l + 1, [(wo_ref.at[l], bbuf_w.at[l, x, c])])
        cols = pl.ds(col_start(x), win)
        local_start(4 * l + 2, [(wg_ref.at[l, :, cols], gu_w.at[l, 0, x, c]), (wu_ref.at[l, :, cols], gu_w.at[l, 1, x, c])])
        local_start(4 * l + 3, [(wd_ref.at[l], wd_at(l, c))])
        d_twin(l)
    kv_start(1, 1)

    gain_copy.wait()
    got("gain", gbuf.at[pl.ds(0, n_dev - 1)])
    tiles = []
    for j in range(width // LANES):
        total = None
        for s in range(n_dev):
            lo = (s * piece) // LANES
            for k in range(2):
                if lo + k == j:
                    block = gbuf[s, :, k * LANES:(k + 1) * LANES]
                    total = block if total is None else total + block
        tiles.append(total)
    gains = 1.0 + jnp.concatenate(tiles, axis=1)

    def rms(hid, row):
        mean_sq = jnp.sum(hid * hid, axis=-1, keepdims=True) / width
        return (hid * lax.rsqrt(mean_sq + EPS) * gains[row:row + 1, :]).astype(BF16)

    lane_seq = lax.rem(lax.broadcasted_iota(jnp.int32, (cache_len, LANES), 1), SEQ_GROUP)
    row_seq = lax.rem(lax.broadcasted_iota(jnp.int32, (LANES, cache_len), 0), SEQ_GROUP)
    row_t = lax.broadcasted_iota(jnp.int32, (cache_len, LANES), 0)
    lane_new = lax.rem(lax.broadcasted_iota(jnp.int32, (SEQ_GROUP, LANES), 1), SEQ_GROUP)
    row_new = lax.broadcasted_iota(jnp.int32, (SEQ_GROUP, LANES), 0)
    chunk = 4

    def attend(l, group):
        i = l * groups + group
        slot = lax.rem(group, 2)
        for copy in kv_copies(i, slot):
            copy.wait()
        seqs = pl.ds(pl.multiple_of(group * SEQ_GROUP, SEQ_GROUP), SEQ_GROUP)
        query = jnp.concatenate([qbuf[j, seqs, :] for j in range(heads)], axis=0)
        scores = jnp.zeros((cache_len, LANES), F32)
        for b in range(0, SEQ_GROUP, chunk):
            block = kbuf[slot, b:b + chunk].reshape(chunk * cache_len, head_dim)
            prod = dot_t(block, query)
            for j in range(chunk):
                scores = jnp.where(lane_seq == b + j, prod[j * cache_len:(j + 1) * cache_len], scores)
        k_new = knew_ref[l, seqs, :]
        v_new = vnew_ref[l, seqs, :]
        new_score = jnp.sum(jnp.where(row_new == lane_new, dot_t(k_new, query), 0.0), axis=0, keepdims=True)
        pos = pos_ref[group]
        scores = jnp.where(row_t < pos, scores, -1e30)
        top = jnp.maximum(jnp.max(scores, axis=0, keepdims=True), new_score)
        prob = jnp.exp(scores - top)
        prob_new = jnp.exp(new_score - top)
        total = jnp.sum(prob, axis=0, keepdims=True) + prob_new
        prob_t = prob.T
        total_t = jnp.broadcast_to(total, (LANES, LANES)).T
        new_t = jnp.broadcast_to(prob_new, (LANES, LANES)).T.astype(BF16).astype(F32)
        v_rep = jnp.concatenate([v_new] * heads, axis=0).astype(F32)
        acc = jnp.concatenate([new_t] * (head_dim // LANES), axis=1) * v_rep
        for b in range(0, SEQ_GROUP, chunk):
            spread = jnp.concatenate([jnp.where(row_seq == b + j, prob_t, 0.0).astype(BF16) for j in range(chunk)], axis=1)
            acc = acc + dot(spread, vbuf[slot, b:b + chunk].reshape(chunk * cache_len, head_dim))
        attn = (acc / jnp.concatenate([total_t] * (head_dim // LANES), axis=1)).astype(BF16)
        for j in range(heads):
            abuf[seqs, j * head_dim:(j + 1) * head_dim] = attn[j * SEQ_GROUP:(j + 1) * SEQ_GROUP, :]

        @pl.when(i + 2 < layers * groups)
        def _():
            kv_start(i + 2, slot)

    hbuf[...] = hid_ref[...]
    cos_tab, sin_tab = cos_ref[...], sin_ref[...]

    def qkv(l):
        normed = rms(hbuf[...].astype(F32), l)
        halves = [dot(normed, abuf_w[l, hf].reshape(width, abuf_w.shape[-1])) for hf in range(2)]

        def rope(lead, tail):
            return jnp.concatenate([lead * cos_tab - tail * sin_tab, tail * cos_tab + lead * sin_tab], axis=1)

        for j in range(heads):
            out, lo = halves[j // (heads // 2)], (j % (heads // 2)) * head_dim
            qbuf[j] = (rope(out[:, lo:lo + half], out[:, lo + half:lo + head_dim]) * head_dim ** -0.5).astype(BF16)
        knew_ref[l] = rope(halves[0][:, q_half:q_half + half], halves[1][:, q_half:q_half + half]).astype(BF16)
        vnew_ref[l] = jnp.concatenate([hv[:, q_half + half:q_half + 2 * half] for hv in halves], axis=1).astype(BF16)

    r2 = rows // 2

    def y_send(l):
        top, bottom = y_all.at[l, x, pl.ds(0, r2)], y_all.at[l, x, pl.ds(r2, r2)]
        send(f"yR1{l}", [(top, top)], right)
        send(f"yL1{l}", [(bottom, bottom)], left)
        send(f"yR2{l}", [(bottom, bottom)], right)
        send(f"yL2{l}", [(top, top)], left)

    def y_forward(l):
        view = y_all.at[l, xl, pl.ds(0, r2)]
        got(f"yR1{l}", view)
        send(f"yfR{l}", [(view, view)], right)
        view = y_all.at[l, xr, pl.ds(r2, r2)]
        got(f"yL1{l}", view)
        send(f"yfL{l}", [(view, view)], left)

    def y_ready(l):
        got(f"yR2{l}", y_all.at[l, xl, pl.ds(r2, r2)])
        got(f"yL2{l}", y_all.at[l, xr, pl.ds(0, r2)])
        got(f"yfR{l}", y_all.at[l, xo, pl.ds(0, r2)])
        got(f"yfL{l}", y_all.at[l, xo, pl.ds(r2, r2)])

    n_tile = 2 * LANES

    def gate_up(l):
        @pl.loop(0, win // n_tile)
        def _(n):
            cols = pl.ds(pl.multiple_of(n * n_tile, n_tile), n_tile)
            w_g = gu_w[l, 0, :, :, :, cols].reshape(width, n_tile)
            w_u = gu_w[l, 1, :, :, :, cols].reshape(width, n_tile)
            for r in range(0, CHIPS, 2):
                act = y_all[l, r:r + 2].reshape(2 * rows, width)
                gate = dot(act, w_g)
                up = dot(act, w_u)
                m_buf[r:r + 2, :, cols] = (jax.nn.gelu(gate, approximate=True) * up).astype(BF16).reshape(2, rows, n_tile)

    def down(l, xx):
        part[xx] = dot(m_buf[xx], wd_w[l])

    def reduce_far(l):
        down(l, xo)
        send(f"eR1{l}", [(part.at[xo, pl.ds(0, r2)], r_t.at[l, 0])], right)
        send(f"eL1{l}", [(part.at[xo, pl.ds(r2, r2)], r_t.at[l, 1])], left)

    def reduce_near(l):
        down(l, xr)
        send(f"eR2{l}", [(part.at[xr, pl.ds(r2, r2)], r_f.at[l, 0, pl.ds(r2, r2)])], right)
        down(l, xl)
        send(f"eL2{l}", [(part.at[xl, pl.ds(0, r2)], r_f.at[l, 1, pl.ds(0, r2)])], left)

    def reduce_relay(l):
        got(f"eR1{l}", r_t.at[l, 0])
        part[xr, 0:r2] = part[xr, 0:r2] + r_t[l, 0]
        send(f"eR3{l}", [(part.at[xr, pl.ds(0, r2)], r_f.at[l, 0, pl.ds(0, r2)])], right)
        got(f"eL1{l}", r_t.at[l, 1])
        part[xl, r2:rows] = part[xl, r2:rows] + r_t[l, 1]
        send(f"eL3{l}", [(part.at[xl, pl.ds(r2, r2)], r_f.at[l, 1, pl.ds(r2, r2)])], left)

    def reduce_done(l):
        got(f"eR2{l}", r_f.at[l, 0, pl.ds(r2, r2)])
        got(f"eL2{l}", r_f.at[l, 1, pl.ds(0, r2)])
        got(f"eR3{l}", r_f.at[l, 0, pl.ds(0, r2)])
        got(f"eL3{l}", r_f.at[l, 1, pl.ds(r2, r2)])
        return part[x] + r_f[l, 0] + r_f[l, 1]

    def attention(l, lo, hi):
        @pl.loop(lo, hi)
        def _(group):
            attend(l, group)

    def mix_out(l):
        mixed = dot(abuf[...], bbuf_w[l].reshape(heads * head_dim, width))
        hid_mid = (hbuf[...].astype(F32) + mixed).astype(BF16)
        hbuf[...] = hid_mid
        y_all[l, x] = rms(hid_mid.astype(F32), layers + l)

    a_forward(0)
    c_direct(0)
    c_transit(0)
    b_forward(0)
    a_twin(0)
    a_ready(0)
    qkv(0)
    attention(0, 0, groups // 2)
    b_twin(0)
    c_pair_near(0)
    c_forward(0)
    attention(0, groups // 2, groups)
    b_ready(0)
    mix_out(0)
    y_send(0)
    c_pair_far(0)
    y_forward(0)
    a_own(1)
    b_own(1)
    y_ready(0)
    c_twin(0)
    c_ready(0)
    d_ready(0)
    c_direct(1)
    a_forward(1)
    gate_up(0)
    reduce_far(0)
    reduce_near(0)
    b_forward(1)
    reduce_relay(0)
    c_transit(1)
    a_twin(1)
    c_pair_near(1)
    down(0, x)
    hbuf[...] = (hbuf[...].astype(F32) + reduce_done(0)).astype(BF16)
    a_ready(1)
    qkv(1)
    c_forward(1)
    b_twin(1)
    attention(1, 0, groups // 2)
    c_pair_far(1)
    attention(1, groups // 2, groups)
    b_ready(1)
    mix_out(1)
    y_send(1)
    c_twin(1)
    y_forward(1)
    y_ready(1)
    c_ready(1)
    d_ready(1)
    gate_up(1)
    drain()
    reduce_far(1)
    reduce_near(1)
    reduce_relay(1)
    down(1, x)
    out_ref[...] = (hbuf[...].astype(F32) + reduce_done(1)).astype(BF16)
    drain()
    assert len(msg_ids) <= send_sem.shape[0]


def decode(hidden, positions, k_cache, v_cache, attn_norm, w_query, w_key, w_value, w_out, mlp_norm, w_gate, w_up, w_down):
    layers, rows, _, cache_len, head_dim = k_cache.shape
    width = hidden.shape[1]
    n_dev = lax.axis_size("w")
    ff = w_gate.shape[-1]
    heads = w_query.shape[-1] // head_dim
    chip_cols = ff // CHIPS
    win = -(-(chip_cols + LANES // 2) // LANES) * LANES
    piece = width // n_dev
    groups = rows // SEQ_GROUP
    assert n_dev == CHIPS * CORES and heads * SEQ_GROUP == LANES and cache_len == LANES
    cos_tab, sin_tab = rope_tables(positions, head_dim)
    offset = lax.rem(lax.axis_index("w") * piece, LANES)
    gain = lax.dynamic_update_slice(jnp.zeros((8, 2 * LANES), F32), jnp.concatenate([attn_norm, mlp_norm], axis=0), (0, offset))
    pos_lane = jnp.tile(positions.reshape(groups, 1, SEQ_GROUP), (1, 1, heads))
    dims = (layers, rows, width, heads, head_dim, cache_len, n_dev, ff)
    vmem, anym = pl.BlockSpec(memory_space=pltpu.VMEM), pl.BlockSpec(memory_space=pl.ANY)
    new_shape = jax.ShapeDtypeStruct((layers, rows, head_dim), BF16)
    n_msg = 96
    return pl.pallas_call(
        functools.partial(decode_kernel, dims),
        out_shape=(jax.ShapeDtypeStruct(hidden.shape, BF16), new_shape, new_shape),
        in_specs=[vmem] * 5 + [anym] * 9,
        out_specs=(vmem,) * 3,
        scratch_shapes=[
            pltpu.VMEM((n_dev, 8, 2 * LANES), F32),
            pltpu.VMEM((layers, 2, CHIPS, CORES, piece, w_query.shape[-1] // 2 + head_dim), BF16),
            pltpu.VMEM((layers, CHIPS, CORES, w_out.shape[1], width), BF16),
            pltpu.VMEM((layers, 2, CHIPS, CORES, piece, win), BF16),
            pltpu.VMEM((layers, win, width), BF16),
            pltpu.VMEM((layers, 2, piece, win // 2), BF16),
            pltpu.VMEM((layers, CHIPS, rows, width), BF16),
            pltpu.VMEM((CHIPS, rows, win), BF16),
            pltpu.VMEM((CHIPS, rows, width), F32),
            pltpu.VMEM((layers, 2, rows // 2, width), F32),
            pltpu.VMEM((layers, 2, rows, width), F32),
            pltpu.VMEM((2, SEQ_GROUP, cache_len, head_dim), BF16),
            pltpu.VMEM((2, SEQ_GROUP, cache_len, head_dim), BF16),
            pltpu.VMEM((heads, rows, head_dim), BF16),
            pltpu.VMEM((rows, heads * head_dim), BF16),
            pltpu.VMEM((rows, width), BF16),
            pltpu.SemaphoreType.DMA((n_msg,)),
            pltpu.SemaphoreType.DMA((n_msg,)),
            pltpu.SemaphoreType.DMA((4 * layers + 1,)),
            pltpu.SemaphoreType.DMA((2, 2)),
        ],
        compiler_params=pltpu.CompilerParams(collective_id=0, has_side_effects=True, vmem_limit_bytes=67043328),
        name="decode",
    )(hidden, cos_tab, sin_tab, gain, pos_lane, k_cache, v_cache, w_query, w_key, w_value, w_out, w_gate, w_up, w_down)


TILE_ROWS = 16
CACHE_BLOCK = 16
CACHE_SLOTS = 6


def cache_kernel(pos_ref, kc_ref, vc_ref, kn_ref, vn_ref, ko_ref, vo_ref, buf, in_sem, out_sem):
    layers, rows = kc_ref.shape[:2]
    blocks = rows // CACHE_BLOCK
    steps = [(src, new, dst, l, b) for l in range(layers) for src, new, dst in ((kc_ref, kn_ref, ko_ref), (vc_ref, vn_ref, vo_ref)) for b in range(blocks)]

    def load(i):
        src, _, _, l, b = steps[i]
        slot = i % CACHE_SLOTS
        return pltpu.make_async_copy(src.at[l, pl.ds(b * CACHE_BLOCK, CACHE_BLOCK), 0], buf.at[slot], in_sem.at[slot])

    def store(i):
        _, _, dst, l, b = steps[i]
        slot = i % CACHE_SLOTS
        return pltpu.make_async_copy(buf.at[slot], dst.at[l, pl.ds(b * CACHE_BLOCK, CACHE_BLOCK), 0], out_sem.at[slot])

    ahead = CACHE_SLOTS // 2
    for i in range(ahead):
        load(i).start()
    row = lax.broadcasted_iota(jnp.int32, (TILE_ROWS, buf.shape[-1]), 0)
    for i in range(len(steps)):
        load(i).wait()
        _, new, _, l, b = steps[i]
        slot = i % CACHE_SLOTS

        @pl.loop(0, CACHE_BLOCK)
        def _(s):
            pos = pos_ref[b * CACHE_BLOCK + s]
            base = pl.multiple_of(pos // TILE_ROWS * TILE_ROWS, TILE_ROWS)
            tile = buf[slot, s, pl.ds(base, TILE_ROWS), :].astype(F32)
            fresh = new[l, pl.ds(b * CACHE_BLOCK + s, 1), :]
            buf[slot, s, pl.ds(base, TILE_ROWS), :] = jnp.where(row == pos - base, fresh, tile).astype(BF16)

        store(i).start()
        nxt = i + ahead
        if nxt < len(steps):
            if nxt >= CACHE_SLOTS:
                store(nxt - CACHE_SLOTS).wait()
            load(nxt).start()
    for i in range(max(0, len(steps) - CACHE_SLOTS), len(steps)):
        store(i).wait()


def write_caches(positions, k_cache, v_cache, k_new, v_new):
    cache_len, head_dim = k_cache.shape[-2:]
    vmem, anym = pl.BlockSpec(memory_space=pltpu.VMEM), pl.BlockSpec(memory_space=pl.ANY)
    shape = jax.ShapeDtypeStruct(k_cache.shape, BF16)
    return pl.pallas_call(
        cache_kernel,
        out_shape=(shape, shape),
        in_specs=[pl.BlockSpec(memory_space=pltpu.SMEM), anym, anym, vmem, vmem],
        out_specs=(anym, anym),
        scratch_shapes=[
            pltpu.VMEM((CACHE_SLOTS, CACHE_BLOCK, cache_len, head_dim), BF16),
            pltpu.SemaphoreType.DMA((CACHE_SLOTS,)),
            pltpu.SemaphoreType.DMA((CACHE_SLOTS,)),
        ],
        compiler_params=pltpu.CompilerParams(vmem_limit_bytes=60 * 2**20),
        name="caches",
    )(positions, k_cache, v_cache, k_new.astype(F32), v_new.astype(F32))


def solution(mesh):
    batch_spec = P(("dp", "w"))
    cache_spec = P(None, ("dp", "w"))
    gain_spec = P(None, "w")
    weight_spec = P(None, "w", None)

    def per_device(hidden, positions, k_cache, v_cache, *weights):
        hidden_out, k_new, v_new = decode(hidden, positions, k_cache, v_cache, *weights)
        k_out, v_out = write_caches(positions, k_cache, v_cache, k_new, v_new)
        return hidden_out, k_out, v_out

    in_specs = (batch_spec, batch_spec, cache_spec, cache_spec, gain_spec, weight_spec, weight_spec, weight_spec, weight_spec, gain_spec, weight_spec, weight_spec, weight_spec)
    out_specs = (batch_spec, cache_spec, cache_spec)
    return jax.shard_map(per_device, mesh=mesh, in_specs=in_specs, out_specs=out_specs, check_vma=False)
```

```python
import functools

import jax
import jax.numpy as jnp
from jax import lax
from jax.experimental import pallas as pl
from jax.experimental.pallas import tpu as pltpu
from jax.sharding import PartitionSpec as P

EPS = 1e-6
ROPE_BASE = 10000.0
LANES = 128
CORES = 2
CHIPS = 4
SEQ_GROUP = 32
MESH = pl.DeviceIdType.MESH
F32 = jnp.float32
BF16 = jnp.bfloat16


def rope_tables(positions, head_dim):
    half_dim = head_dim // 2
    inv_freq = ROPE_BASE ** (-2.0 * jnp.arange(half_dim, dtype=jnp.float32) / head_dim)
    angles = positions.astype(jnp.float32)[:, None] * inv_freq[None, :]
    return jnp.cos(angles), jnp.sin(angles)


def dot(a, b):
    return jnp.dot(a, b, preferred_element_type=F32)


def dot_t(a, b):
    return lax.dot_general(a, b, (((1,), (1,)), ((), ())), preferred_element_type=F32)


ORDER = (
    "bo0", "ao0", "ct0", "bf0", "af0", "cf0", "cd0", "ct1", "bx0", "ax0", "cx0", "aw0", "dt0", "qkv0",
    "att0", "bw0", "ao1", "att0", "att0", "cd1", "cn0", "af1", "att0", "mix0", "yf0", "cf1", "cw0", "ax1", "dt1",
    "gua0", "near0", "cn1", "gub0", "far0", "bo1", "er0", "own0", "bf1", "aw1", "cx1", "done0", "qkv1",
    "att1", "att1", "bx1", "att1", "att1", "mix1", "cw1", "yf1", "gua1", "near1", "gub1", "far1", "er1", "own1", "done1",
)
SHARE_A = (True, True)
SHARE_B = (True, False)


def decode_kernel(
    dims,
    hid_ref, cos_ref, sin_ref, an_ref, mn_ref, pos_ref, kc_ref, vc_ref,
    wq_ref, wk_ref, wv_ref, wo_ref, wg_ref, wu_ref, wd_ref,
    out_ref, knew_ref, vnew_ref,
    gsrc, gbuf, pos_buf, abuf_w, bbuf_w, gu_w, wd_w, tr_w, y_all, m_buf, part, r_t, r_f,
    kbuf, vbuf, qbuf, abuf, hbuf,
    send_sem, recv_sem, loc_sem, kv_sem,
):
    layers, rows, width, heads, head_dim, cache_len, n_dev, ff = dims
    half = head_dim // 2
    piece = width // n_dev
    chip_cols = ff // CHIPS
    win = gu_w.shape[-1]
    pad = win - chip_cols
    wd_rows = wd_ref.shape[1]
    wo_rows = wo_ref.shape[1]
    q_half = wq_ref.shape[-1] // 2
    kv_half = half
    a_cols = abuf_w.shape[-1]
    groups = rows // SEQ_GROUP
    w = lax.axis_index("w")
    dp = lax.axis_index("dp")
    x, c = lax.div(w, CORES), lax.rem(w, CORES)
    h = lax.rem(dp, 2)
    xr, xo, xl = lax.rem(x + 1, CHIPS), lax.rem(x + 2, CHIPS), lax.rem(x + 3, CHIPS)
    cc = 1 - c
    hh = 1 - h
    right, left = (dp, xr * CORES + c), (dp, xl * CORES + c)
    twin = (dp, x * CORES + cc)
    pair = (dp + 1 - 2 * h, w)
    b_half, b_quarter = wo_rows // 2, wo_rows // 4
    b_mine = pl.multiple_of(h * b_half, b_quarter)
    b_mid = pl.multiple_of(h * b_half + b_quarter, b_quarter)
    b_other = pl.multiple_of(hh * b_half, b_quarter)
    q_mine = pl.multiple_of(h * q_half, LANES)
    kv_mine = pl.multiple_of(h * kv_half, LANES)
    starts = [pl.multiple_of(lax.div(chip_cols * xx, LANES) * LANES, LANES) for xx in (x, xr, xo, xl)]
    x_start, xr_start, xo_start, xl_start = starts
    xo_mid = pl.multiple_of(xo_start + win // 2, LANES)
    shift = lax.rem(chip_cols * x, LANES)
    wd_mine = pl.ds(pl.multiple_of(shift + wd_rows * c, 32), wd_rows)
    wd_twin = pl.ds(pl.multiple_of(shift + wd_rows * cc, 32), wd_rows)

    msg_ids = {}
    pending = {}

    def copy_of(name, src, dst, dev):
        i = msg_ids.setdefault(name, len(msg_ids))
        return pltpu.make_async_remote_copy(src, dst, send_sem.at[i], recv_sem.at[i], device_id=dev, device_id_type=MESH)

    def send(name, pairs, dev, view=None):
        for src, dst in pairs:
            copy_of(name, src, dst, dev).start()
        pending[name] = pairs[0][0] if view is None else view

    def got(name, view):
        copy_of(name, view, view, right).wait_recv()

    def drain(names):
        for name in names:
            view = pending.pop(name)
            copy_of(name, view, view, right).wait_send()

    def local_start(sem, pairs):
        for src, dst in pairs:
            pltpu.make_async_copy(src, dst, loc_sem.at[sem]).start()

    def local_wait(sem, view):
        pltpu.make_async_copy(view, view, loc_sem.at[sem]).wait()

    def kv_copies(i, slot):
        layer, group = lax.div(i, groups), lax.rem(i, groups)
        seqs = pl.ds(group * SEQ_GROUP, SEQ_GROUP)
        return (
            pltpu.make_async_copy(kc_ref.at[layer, seqs, 0], kbuf.at[slot], kv_sem.at[slot, 0]),
            pltpu.make_async_copy(vc_ref.at[layer, seqs, 0], vbuf.at[slot], kv_sem.at[slot, 1]),
        )

    def kv_start(i, slot):
        for copy in kv_copies(i, slot):
            copy.start()

    def a_pairs(l, hf, q_lo, kv_lo):
        dst = abuf_w.at[l, hf, x, c]
        return [
            (wq_ref.at[l, :, pl.ds(q_lo, q_half)], dst.at[:, pl.ds(0, q_half)]),
            (wk_ref.at[l, :, pl.ds(kv_lo, kv_half)], dst.at[:, pl.ds(q_half, kv_half)]),
            (wv_ref.at[l, :, pl.ds(kv_lo, kv_half)], dst.at[:, pl.ds(q_half + kv_half, kv_half)]),
        ]

    def a_both(l):
        return a_pairs(l, 0, 0, 0) + a_pairs(l, 1, q_half, kv_half)

    def a_block(l, xx):
        return abuf_w.at[l, h, xx, c] if SHARE_A[l] else abuf_w.at[l, :, xx, c]

    def a_lead(l, xx):
        return abuf_w.at[l, h, xx, c, :, pl.ds(0, a_cols // 2)] if SHARE_A[l] else abuf_w.at[l, 0, xx, c]

    def a_tail(l, xx):
        return abuf_w.at[l, h, xx, c, :, pl.ds(a_cols // 2, a_cols // 2)] if SHARE_A[l] else abuf_w.at[l, 1, xx, c]

    def ao(l):
        pairs = a_pairs(l, h, q_mine, kv_mine) if SHARE_A[l] else a_both(l)
        send(f"aR{l}", pairs, right, a_block(l, x))
        send(f"aL{l}", pairs, left, a_block(l, x))

    def to_pair(name, view):
        send(name, [(view, view)], pair)

    def af(l):
        got(f"aR{l}", a_block(l, xl))
        send(f"afR{l}", [(a_lead(l, xl), a_lead(l, xl))], right)
        got(f"aL{l}", a_block(l, xr))
        send(f"afL{l}", [(a_tail(l, xr), a_tail(l, xr))], left)
        if SHARE_A[l]:
            to_pair(f"paR{l}", a_block(l, xl))
            to_pair(f"paL{l}", a_block(l, xr))

    def ax(l):
        got(f"afR{l}", a_lead(l, xo))
        got(f"afL{l}", a_tail(l, xo))
        if SHARE_A[l]:
            to_pair(f"paF{l}", a_block(l, xo))
        local_wait(4 * l, abuf_w.at[l, :, x, c])
        view = abuf_w.at[l, h, :, c] if SHARE_A[l] else abuf_w.at[l, :, :, c]
        send(f"aT{l}", [(view, view)], twin)

    def aw(l):
        for name, xx in (("paR", xl), ("paL", xr), ("paF", xo)):
            got(f"{name}{l}", abuf_w.at[l, hh, xx, c])
        view = abuf_w.at[l, hh, :, c]
        send(f"aT1{l}", [(view, view)], twin)

    def a_ready(l):
        if SHARE_A[l]:
            got(f"aT{l}", abuf_w.at[l, h, :, cc])
            got(f"aT1{l}", abuf_w.at[l, hh, :, cc])
        else:
            got(f"aT{l}", abuf_w.at[l, :, :, cc])

    def b_block(l, xx):
        return bbuf_w.at[l, xx, c, pl.ds(b_mine, b_half)] if SHARE_B[l] else bbuf_w.at[l, xx, c]

    def b_lead(l, xx):
        return bbuf_w.at[l, xx, c, pl.ds(b_mine, b_quarter)] if SHARE_B[l] else bbuf_w.at[l, xx, c, pl.ds(0, b_half)]

    def b_tail(l, xx):
        return bbuf_w.at[l, xx, c, pl.ds(b_mid, b_quarter)] if SHARE_B[l] else bbuf_w.at[l, xx, c, pl.ds(b_half, b_half)]

    def bo(l):
        src = wo_ref.at[l, pl.ds(b_mine, b_half)] if SHARE_B[l] else wo_ref.at[l]
        send(f"bR{l}", [(src, b_block(l, x))], right)
        send(f"bL{l}", [(src, b_block(l, x))], left)

    def bf(l):
        got(f"bR{l}", b_block(l, xl))
        send(f"bfR{l}", [(b_lead(l, xl), b_lead(l, xl))], right)
        got(f"bL{l}", b_block(l, xr))
        send(f"bfL{l}", [(b_tail(l, xr), b_tail(l, xr))], left)
        if SHARE_B[l]:
            to_pair(f"pbR{l}", b_block(l, xl))
            to_pair(f"pbL{l}", b_block(l, xr))

    def bx(l):
        got(f"bfR{l}", b_lead(l, xo))
        got(f"bfL{l}", b_tail(l, xo))
        if SHARE_B[l]:
            to_pair(f"pbF{l}", b_block(l, xo))
        local_wait(4 * l + 1, bbuf_w.at[l, x, c])
        view = bbuf_w.at[l, :, c, pl.ds(b_mine, b_half)] if SHARE_B[l] else bbuf_w.at[l, :, c]
        send(f"bT{l}", [(view, view)], twin)

    def bw(l):
        for name, xx in (("pbR", xl), ("pbL", xr), ("pbF", xo)):
            got(f"{name}{l}", bbuf_w.at[l, xx, c, pl.ds(b_other, b_half)])
        view = bbuf_w.at[l, :, c, pl.ds(b_other, b_half)]
        send(f"bT1{l}", [(view, view)], twin)

    def b_ready(l):
        if SHARE_B[l]:
            got(f"bT{l}", bbuf_w.at[l, :, cc, pl.ds(b_mine, b_half)])
            got(f"bT1{l}", bbuf_w.at[l, :, cc, pl.ds(b_other, b_half)])
        else:
            got(f"bT{l}", bbuf_w.at[l, :, cc])

    def by_matrix(l, name, lo, size, dst, dev):
        for value, ref in ((0, wg_ref), (1, wu_ref)):
            @pl.when(h == value)
            def _():
                copy_of(name, ref.at[l, :, pl.ds(lo, size)], dst, dev).start()
        pending[name] = dst

    def cd(l):
        by_matrix(l, f"cR{l}", xr_start, win, gu_w.at[l, h, x, c], right)
        by_matrix(l, f"cL{l}", xl_start, win, gu_w.at[l, h, x, c], left)

    def ct(l):
        by_matrix(l, f"tR{l}", xo_start, win // 2, tr_w.at[l, 0], right)
        by_matrix(l, f"tL{l}", xo_mid, win // 2, tr_w.at[l, 1], left)

    def cf(l):
        got(f"tR{l}", tr_w.at[l, 0])
        send(f"cfR{l}", [(tr_w.at[l, 0], gu_w.at[l, h, xl, c, :, pl.ds(0, win // 2)])], right)
        got(f"tL{l}", tr_w.at[l, 1])
        send(f"cfL{l}", [(tr_w.at[l, 1], gu_w.at[l, h, xr, c, :, pl.ds(win // 2, win // 2)])], left)

    def cn(l):
        for name, xx in (("cR", xl), ("cL", xr)):
            got(f"{name}{l}", gu_w.at[l, h, xx, c])
            to_pair(f"p{name}{l}", gu_w.at[l, h, xx, c])

    def cx(l):
        got(f"cfR{l}", gu_w.at[l, h, xo, c, :, pl.ds(0, win // 2)])
        got(f"cfL{l}", gu_w.at[l, h, xo, c, :, pl.ds(win // 2, win // 2)])
        to_pair(f"pcF{l}", gu_w.at[l, h, xo, c])

    def cw(l):
        local_wait(4 * l + 2, gu_w.at[l, :, x, c])
        view = gu_w.at[l, h, :, c]
        send(f"cT{l}", [(view, view)], twin)
        for name, xx in (("pcR", xl), ("pcL", xr), ("pcF", xo)):
            got(f"{name}{l}", gu_w.at[l, hh, xx, c])
        view = gu_w.at[l, hh, :, c]
        send(f"cT1{l}", [(view, view)], twin)

    def c_ready(l):
        got(f"cT{l}", gu_w.at[l, h, :, cc])
        got(f"cT1{l}", gu_w.at[l, hh, :, cc])

    def dt(l):
        send(f"dT{l}", [(wd_ref.at[l], wd_w.at[l, wd_mine])], twin)

    def d_ready(l):
        local_wait(4 * l + 3, wd_w.at[l, wd_mine])
        got(f"dT{l}", wd_w.at[l, wd_twin])

    for l in range(layers):
        start = pl.multiple_of(jnp.where(lax.rem(x, 2) == 0, chip_cols, 0), 64)
        wd_w[l, pl.ds(start, pad), :] = jnp.zeros((pad, width), BF16)
    gsrc[...] = jnp.zeros_like(gsrc)
    gsrc[0:layers, 0:piece] = an_ref[...]
    gsrc[layers:2 * layers, 0:piece] = mn_ref[...]
    gsrc[...] = pltpu.roll(gsrc[...], lax.rem(w * piece, LANES), 1)
    barrier = pltpu.get_barrier_semaphore()
    for i in range(1, n_dev):
        pl.semaphore_signal(barrier, inc=1, device_id=(dp, lax.rem(w + i, n_dev)), device_id_type=MESH)
    pl.semaphore_signal(barrier, inc=1, device_id=pair, device_id_type=MESH)
    pl.semaphore_wait(barrier, n_dev)

    def entry():
        for i in range(1, n_dev):
            copy_of("gain", gsrc, gbuf.at[w], (dp, lax.rem(w + i, n_dev))).start()
        pending["gain"] = gbuf.at[pl.ds(0, n_dev - 1)]
        gbuf[w] = gsrc[...]
        kv_start(0, 0)
        for l in range(layers):
            local_start(4 * l, a_both(l))
            local_start(4 * l + 1, [(wo_ref.at[l], bbuf_w.at[l, x, c])])
            cols = pl.ds(x_start, win)
            local_start(4 * l + 2, [(wg_ref.at[l, :, cols], gu_w.at[l, 0, x, c]), (wu_ref.at[l, :, cols], gu_w.at[l, 1, x, c])])
            local_start(4 * l + 3, [(wd_ref.at[l], wd_w.at[l, wd_mine])])
        kv_start(1, 1)
        hbuf[...] = hid_ref[...]
        lane_block = lax.div(lax.broadcasted_iota(jnp.int32, (1, LANES), 1), SEQ_GROUP)
        for g in range(groups):
            line = pos_ref[...]
            for j in range(heads):
                moved = pltpu.roll(pos_ref[...], lax.rem(w * 0 + (j - g + heads) * SEQ_GROUP, LANES), 1)
                line = jnp.where(lane_block == j, moved, line)
            pos_buf[g] = line

    def all_gains():
        tiles = []
        for j in range(width // LANES):
            total = None
            for s in range(n_dev):
                lo = (s * piece) // LANES
                for k in range(2):
                    if lo + k == j:
                        block = gbuf[s, :, k * LANES:(k + 1) * LANES]
                        total = block if total is None else total + block
            tiles.append(total)
        return 1.0 + jnp.concatenate(tiles, axis=1)

    def rms(hid, row):
        mean_sq = jnp.sum(hid * hid, axis=-1, keepdims=True) / width
        return (hid * lax.rsqrt(mean_sq + EPS) * all_gains()[row:row + 1, :]).astype(BF16)

    chunk = 4

    def attend(l, group):
        lane_seq = lax.rem(lax.broadcasted_iota(jnp.int32, (cache_len, LANES), 1), SEQ_GROUP)
        row_seq = lax.rem(lax.broadcasted_iota(jnp.int32, (LANES, cache_len), 0), SEQ_GROUP)
        row_t = lax.broadcasted_iota(jnp.int32, (cache_len, LANES), 0)
        lane_new = lax.rem(lax.broadcasted_iota(jnp.int32, (SEQ_GROUP, LANES), 1), SEQ_GROUP)
        row_new = lax.broadcasted_iota(jnp.int32, (SEQ_GROUP, LANES), 0)
        i = l * groups + group
        slot = lax.rem(group, 2)
        for copy in kv_copies(i, slot):
            copy.wait()
        seqs = pl.ds(pl.multiple_of(group * SEQ_GROUP, SEQ_GROUP), SEQ_GROUP)
        query = jnp.concatenate([qbuf[j, seqs, :] for j in range(heads)], axis=0)
        scores = jnp.zeros((cache_len, LANES), F32)
        for b in range(0, SEQ_GROUP, chunk):
            block = kbuf[slot, b:b + chunk].reshape(chunk * cache_len, head_dim)
            prod = dot_t(block, query)
            for j in range(chunk):
                scores = jnp.where(lane_seq == b + j, prod[j * cache_len:(j + 1) * cache_len], scores)
        k_new = knew_ref[l, seqs, :].astype(BF16)
        v_new = vnew_ref[l, seqs, :]
        new_score = jnp.sum(jnp.where(row_new == lane_new, dot_t(k_new, query), 0.0), axis=0, keepdims=True)
        scores = jnp.where(row_t < pos_buf[group], scores, -1e30)
        top = jnp.maximum(jnp.max(scores, axis=0, keepdims=True), new_score)
        prob = jnp.exp(scores - top)
        prob_new = jnp.exp(new_score - top)
        total = jnp.sum(prob, axis=0, keepdims=True) + prob_new
        prob_t = prob.T
        total_t = jnp.broadcast_to(total, (LANES, LANES)).T
        new_t = jnp.broadcast_to(prob_new, (LANES, LANES)).T.astype(BF16).astype(F32)
        v_rep = jnp.concatenate([v_new] * heads, axis=0)
        acc = jnp.concatenate([new_t] * (head_dim // LANES), axis=1) * v_rep
        for b in range(0, SEQ_GROUP, chunk):
            spread = jnp.concatenate([jnp.where(row_seq == b + j, prob_t, 0.0).astype(BF16) for j in range(chunk)], axis=1)
            acc = acc + dot(spread, vbuf[slot, b:b + chunk].reshape(chunk * cache_len, head_dim))
        attn = (acc / jnp.concatenate([total_t] * (head_dim // LANES), axis=1)).astype(BF16)
        for j in range(heads):
            abuf[seqs, j * head_dim:(j + 1) * head_dim] = attn[j * SEQ_GROUP:(j + 1) * SEQ_GROUP, :]

        @pl.when(i + 2 < layers * groups)
        def _():
            kv_start(i + 2, slot)

    def qkv(l):
        a_ready(l)
        if l == 0:
            got("gain", gbuf.at[pl.ds(0, n_dev - 1)])
        cos_tab, sin_tab = cos_ref[...], sin_ref[...]
        normed = rms(hbuf[...].astype(F32), l)
        halves = [dot(normed, abuf_w[l, hf].reshape(width, a_cols)) for hf in range(2)]

        def rope(lead, tail):
            return jnp.concatenate([lead * cos_tab - tail * sin_tab, tail * cos_tab + lead * sin_tab], axis=1)

        for j in range(heads):
            out, lo = halves[j // (heads // 2)], (j % (heads // 2)) * head_dim
            qbuf[j] = (rope(out[:, lo:lo + half], out[:, lo + half:lo + head_dim]) * head_dim ** -0.5).astype(BF16)
        knew_ref[l] = rope(halves[0][:, q_half:q_half + half], halves[1][:, q_half:q_half + half]).astype(BF16).astype(F32)
        vnew_ref[l] = jnp.concatenate([hv[:, q_half + half:q_half + 2 * half] for hv in halves], axis=1).astype(BF16).astype(F32)

    r2 = rows // 2
    upper, lower = pl.ds(0, r2), pl.ds(r2, r2)

    def mix(l):
        b_ready(l)
        mixed = dot(abuf[...], bbuf_w[l].reshape(heads * head_dim, width))
        hid_mid = (hbuf[...].astype(F32) + mixed).astype(BF16)
        hbuf[...] = hid_mid
        y_all[l, x] = rms(hid_mid.astype(F32), layers + l)
        top, bottom = y_all.at[l, x, upper], y_all.at[l, x, lower]
        send(f"yR1{l}", [(top, top)], right)
        send(f"yL1{l}", [(bottom, bottom)], left)
        send(f"yR2{l}", [(bottom, bottom)], right)
        send(f"yL2{l}", [(top, top)], left)

    def yf(l):
        view = y_all.at[l, xl, upper]
        got(f"yR1{l}", view)
        send(f"yfR{l}", [(view, view)], right)
        view = y_all.at[l, xr, lower]
        got(f"yL1{l}", view)
        send(f"yfL{l}", [(view, view)], left)

    n_tile = 2 * LANES

    def gate_up(l, blocks):
        @pl.loop(0, win // n_tile)
        def _(n):
            cols = pl.ds(pl.multiple_of(n * n_tile, n_tile), n_tile)
            act = jnp.concatenate([y_all[l, b] for b in blocks], axis=0)
            gate = dot(act, gu_w[l, 0, :, :, :, cols].reshape(width, n_tile))
            up = dot(act, gu_w[l, 1, :, :, :, cols].reshape(width, n_tile))
            mid = (jax.nn.gelu(gate, approximate=True) * up).astype(BF16)
            for k, b in enumerate(blocks):
                m_buf[b, :, cols] = mid[k * rows:(k + 1) * rows]

    def gua(l):
        got(f"yR2{l}", y_all.at[l, xl, lower])
        got(f"yL2{l}", y_all.at[l, xr, upper])
        c_ready(l)
        gate_up(l, (xl, xr))

    def gub(l):
        got(f"yfR{l}", y_all.at[l, xo, upper])
        got(f"yfL{l}", y_all.at[l, xo, lower])
        gate_up(l, (xo, x))

    def down(l, xx):
        part[xx] = dot(m_buf[xx], wd_w[l])

    def near(l):
        d_ready(l)
        if l:
            drain([f"{name}{l - 1}" for name in ("eR1", "eL1", "eR2", "eL2", "eR3", "eL3")])
        down(l, xr)
        send(f"eR2{l}", [(part.at[xr, lower], r_f.at[l, 0, lower])], right)
        down(l, xl)
        send(f"eL2{l}", [(part.at[xl, upper], r_f.at[l, 1, upper])], left)

    def far(l):
        down(l, xo)
        send(f"eR1{l}", [(part.at[xo, upper], r_t.at[l, 0])], right)
        send(f"eL1{l}", [(part.at[xo, lower], r_t.at[l, 1])], left)

    def er(l):
        got(f"eR1{l}", r_t.at[l, 0])
        part[xr, 0:r2] = part[xr, 0:r2] + r_t[l, 0]
        send(f"eR3{l}", [(part.at[xr, upper], r_f.at[l, 0, upper])], right)
        got(f"eL1{l}", r_t.at[l, 1])
        part[xl, r2:rows] = part[xl, r2:rows] + r_t[l, 1]
        send(f"eL3{l}", [(part.at[xl, lower], r_f.at[l, 1, lower])], left)

    def own(l):
        down(l, x)

    def done(l):
        got(f"eR2{l}", r_f.at[l, 0, lower])
        got(f"eL2{l}", r_f.at[l, 1, upper])
        got(f"eR3{l}", r_f.at[l, 0, upper])
        got(f"eL3{l}", r_f.at[l, 1, lower])
        hid_next = (hbuf[...].astype(F32) + (part[x] + r_f[l, 0] + r_f[l, 1])).astype(BF16)
        if l + 1 < layers:
            hbuf[...] = hid_next
        else:
            out_ref[...] = hid_next

    table = dict(
        ao=ao, af=af, ax=ax, aw=aw, bo=bo, bf=bf, bx=bx, bw=bw, cd=cd, ct=ct, cf=cf, cn=cn, cx=cx, cw=cw, dt=dt,
        qkv=qkv, mix=mix, yf=yf, gua=gua, gub=gub, near=near, far=far, er=er, own=own, done=done,
    )

    def run(step):
        table[step[:-1]](int(step[-1]))

    entry()
    at = 0
    reached = [0] * layers
    while at < len(ORDER):
        step = ORDER[at]
        if not step.startswith("att"):
            run(step)
            at += 1
            continue
        l, count = int(step[-1]), 0
        while ORDER[at] == step:
            count += 1
            at += 1
        first = reached[l]
        reached[l] += count

        @pl.loop(first, first + count)
        def _(group):
            attend(l, group)

    drain(list(pending))
    assert len(msg_ids) <= send_sem.shape[0]


def decode(hidden, positions, k_cache, v_cache, attn_norm, w_query, w_key, w_value, w_out, mlp_norm, w_gate, w_up, w_down):
    layers, rows, _, cache_len, head_dim = k_cache.shape
    width = hidden.shape[1]
    n_dev = lax.axis_size("w")
    ff = w_gate.shape[-1]
    heads = w_query.shape[-1] // head_dim
    chip_cols = ff // CHIPS
    win = -(-(chip_cols + LANES // 2) // LANES) * LANES
    piece = width // n_dev
    groups = rows // SEQ_GROUP
    assert n_dev == CHIPS * CORES and heads * SEQ_GROUP == LANES and cache_len == LANES and rows == LANES
    assert lax.axis_size("dp") % 2 == 0
    cos_tab, sin_tab = rope_tables(positions, head_dim)
    dims = (layers, rows, width, heads, head_dim, cache_len, n_dev, ff)
    vmem, anym = pl.BlockSpec(memory_space=pltpu.VMEM), pl.BlockSpec(memory_space=pl.ANY)
    new_shape = jax.ShapeDtypeStruct((layers, rows, head_dim), F32)
    n_msg = 96
    return pl.pallas_call(
        functools.partial(decode_kernel, dims),
        out_shape=(jax.ShapeDtypeStruct(hidden.shape, BF16), new_shape, new_shape),
        in_specs=[vmem] * 6 + [anym] * 9,
        out_specs=(vmem,) * 3,
        scratch_shapes=[
            pltpu.VMEM((8, 2 * LANES), F32),
            pltpu.VMEM((n_dev, 8, 2 * LANES), F32),
            pltpu.VMEM((groups, 1, LANES), jnp.int32),
            pltpu.VMEM((layers, 2, CHIPS, CORES, piece, w_query.shape[-1] // 2 + head_dim), BF16),
            pltpu.VMEM((layers, CHIPS, CORES, w_out.shape[1], width), BF16),
            pltpu.VMEM((layers, 2, CHIPS, CORES, piece, win), BF16),
            pltpu.VMEM((layers, win, width), BF16),
            pltpu.VMEM((layers, 2, piece, win // 2), BF16),
            pltpu.VMEM((layers, CHIPS, rows, width), BF16),
            pltpu.VMEM((CHIPS, rows, win), BF16),
            pltpu.VMEM((CHIPS, rows, width), F32),
            pltpu.VMEM((layers, 2, rows // 2, width), F32),
            pltpu.VMEM((layers, 2, rows, width), F32),
            pltpu.VMEM((2, SEQ_GROUP, cache_len, head_dim), BF16),
            pltpu.VMEM((2, SEQ_GROUP, cache_len, head_dim), BF16),
            pltpu.VMEM((heads, rows, head_dim), BF16),
            pltpu.VMEM((rows, heads * head_dim), BF16),
            pltpu.VMEM((rows, width), BF16),
            pltpu.SemaphoreType.DMA((n_msg,)),
            pltpu.SemaphoreType.DMA((n_msg,)),
            pltpu.SemaphoreType.DMA((4 * layers,)),
            pltpu.SemaphoreType.DMA((2, 2)),
        ],
        compiler_params=pltpu.CompilerParams(collective_id=0, has_side_effects=True, vmem_limit_bytes=67043328),
        name="decode",
    )(hidden, cos_tab, sin_tab, attn_norm, mlp_norm, positions.reshape(1, rows), k_cache, v_cache, w_query, w_key, w_value, w_out, w_gate, w_up, w_down)


TILE_ROWS = 16
CACHE_BLOCK = 32
CACHE_SLOTS = 6


def cache_kernel(pos_ref, kc_ref, vc_ref, kn_ref, vn_ref, ko_ref, vo_ref, buf, in_sem, out_sem):
    layers, rows = kc_ref.shape[:2]
    blocks = rows // CACHE_BLOCK
    steps = [(src, new, dst, l, b) for l in range(layers) for src, new, dst in ((kc_ref, kn_ref, ko_ref), (vc_ref, vn_ref, vo_ref)) for b in range(blocks)]

    def load(i):
        src, _, _, l, b = steps[i]
        slot = i % CACHE_SLOTS
        return pltpu.make_async_copy(src.at[l, pl.ds(b * CACHE_BLOCK, CACHE_BLOCK), 0], buf.at[slot], in_sem.at[slot])

    def store(i):
        _, _, dst, l, b = steps[i]
        slot = i % CACHE_SLOTS
        return pltpu.make_async_copy(buf.at[slot], dst.at[l, pl.ds(b * CACHE_BLOCK, CACHE_BLOCK), 0], out_sem.at[slot])

    ahead = CACHE_SLOTS // 2
    for i in range(ahead):
        load(i).start()
    row = lax.broadcasted_iota(jnp.int32, (TILE_ROWS, buf.shape[-1]), 0)
    for i in range(len(steps)):
        load(i).wait()
        _, new, _, l, b = steps[i]
        slot = i % CACHE_SLOTS

        @pl.loop(0, CACHE_BLOCK)
        def _(s):
            pos = pos_ref[b * CACHE_BLOCK + s]
            base = pl.multiple_of(pos // TILE_ROWS * TILE_ROWS, TILE_ROWS)
            tile = buf[slot, s, pl.ds(base, TILE_ROWS), :].astype(F32)
            fresh = new[l, pl.ds(b * CACHE_BLOCK + s, 1), :]
            buf[slot, s, pl.ds(base, TILE_ROWS), :] = jnp.where(row == pos - base, fresh, tile).astype(BF16)

        store(i).start()
        nxt = i + ahead
        if nxt < len(steps):
            if nxt >= CACHE_SLOTS:
                store(nxt - CACHE_SLOTS).wait()
            load(nxt).start()
    for i in range(max(0, len(steps) - CACHE_SLOTS), len(steps)):
        store(i).wait()


def write_caches(positions, k_cache, v_cache, k_new, v_new):
    cache_len, head_dim = k_cache.shape[-2:]
    vmem, anym = pl.BlockSpec(memory_space=pltpu.VMEM), pl.BlockSpec(memory_space=pl.ANY)
    shape = jax.ShapeDtypeStruct(k_cache.shape, BF16)
    return pl.pallas_call(
        cache_kernel,
        out_shape=(shape, shape),
        in_specs=[pl.BlockSpec(memory_space=pltpu.SMEM), anym, anym, vmem, vmem],
        out_specs=(anym, anym),
        scratch_shapes=[
            pltpu.VMEM((CACHE_SLOTS, CACHE_BLOCK, cache_len, head_dim), BF16),
            pltpu.SemaphoreType.DMA((CACHE_SLOTS,)),
            pltpu.SemaphoreType.DMA((CACHE_SLOTS,)),
        ],
        compiler_params=pltpu.CompilerParams(vmem_limit_bytes=60 * 2**20),
        name="caches",
    )(positions, k_cache, v_cache, k_new, v_new)


def solution(mesh):
    batch_spec = P(("dp", "w"))
    cache_spec = P(None, ("dp", "w"))
    gain_spec = P(None, "w")
    weight_spec = P(None, "w", None)

    def per_device(hidden, positions, k_cache, v_cache, *weights):
        hidden_out, k_new, v_new = decode(hidden, positions, k_cache, v_cache, *weights)
        k_out, v_out = write_caches(positions, k_cache, v_cache, k_new, v_new)
        return hidden_out, k_out, v_out

    in_specs = (batch_spec, batch_spec, cache_spec, cache_spec, gain_spec, weight_spec, weight_spec, weight_spec, weight_spec, gain_spec, weight_spec, weight_spec, weight_spec)
    out_specs = (batch_spec, cache_spec, cache_spec)
    return jax.shard_map(per_device, mesh=mesh, in_specs=in_specs, out_specs=out_specs, check_vma=False)
```

```python
import functools

import jax
import jax.numpy as jnp
from jax import lax
from jax.experimental import pallas as pl
from jax.experimental.pallas import tpu as pltpu
from jax.sharding import PartitionSpec as P

EPS = 1e-6
ROPE_BASE = 10000.0
LANES = 128
CORES = 2
CHIPS = 4
SEQ_GROUP = 32
MESH = pl.DeviceIdType.MESH
F32 = jnp.float32
BF16 = jnp.bfloat16


def rope_tables(positions, head_dim):
    half_dim = head_dim // 2
    inv_freq = ROPE_BASE ** (-2.0 * jnp.arange(half_dim, dtype=jnp.float32) / head_dim)
    angles = positions.astype(jnp.float32)[:, None] * inv_freq[None, :]
    return jnp.cos(angles), jnp.sin(angles)


def dot(a, b):
    return jnp.dot(a, b, preferred_element_type=F32)


def dot_t(a, b):
    return lax.dot_general(a, b, (((1,), (1,)), ((), ())), preferred_element_type=F32)


ORDER = (
    "bo0", "ao0", "ct0", "bf0", "af0", "cf0", "cd0", "ct1", "bx0", "ax0", "cx0", "aw0", "dt0", "qkv0",
    "att0", "bw0", "ao1", "att0", "att0", "cd1", "cn0", "af1", "att0", "mix0", "yf0", "cf1", "cw0", "ax1", "dt1", "dr0",
    "gua0", "near0", "cn1", "gub0", "far0", "bo1", "er0", "guo0", "own0", "bf1", "aw1", "cx1", "done0", "qkv1",
    "att1", "att1", "bx1", "att1", "att1", "mix1", "cw1", "yf1", "guo1", "dr1", "own1", "gua1", "near1", "gub1", "far1",
)
SHARE_A = (True, True)
SHARE_B = (True, False)


def decode_kernel(
    dims,
    hid_ref, cos_ref, sin_ref, an_ref, mn_ref, pos_ref, kc_ref, vc_ref,
    wq_ref, wk_ref, wv_ref, wo_ref, wg_ref, wu_ref, wd_ref,
    hid_out, knew_ref, vnew_ref, far_r, far_l, near_r, near_l, next_r, next_l, own_out,
    gsrc, gbuf, pos_buf, abuf_w, bbuf_w, gu_w, wd_w, tr_w, y_all, m_buf, part, r_t, r_f,
    kbuf, vbuf, qbuf, abuf, hbuf,
    send_sem, recv_sem, loc_sem, kv_sem, out_sem,
):
    layers, rows, width, heads, head_dim, cache_len, n_dev, ff = dims
    half = head_dim // 2
    piece = width // n_dev
    chip_cols = ff // CHIPS
    win = gu_w.shape[-1]
    pad = win - chip_cols
    wd_rows = wd_ref.shape[1]
    wo_rows = wo_ref.shape[1]
    q_half = wq_ref.shape[-1] // 2
    kv_half = half
    a_cols = abuf_w.shape[-1]
    groups = rows // SEQ_GROUP
    w = lax.axis_index("w")
    dp = lax.axis_index("dp")
    x, c = lax.div(w, CORES), lax.rem(w, CORES)
    h = lax.rem(dp, 2)
    xr, xo, xl = lax.rem(x + 1, CHIPS), lax.rem(x + 2, CHIPS), lax.rem(x + 3, CHIPS)
    cc = 1 - c
    hh = 1 - h
    right, left = (dp, xr * CORES + c), (dp, xl * CORES + c)
    twin = (dp, x * CORES + cc)
    pair = (dp + 1 - 2 * h, w)
    b_half, b_quarter = wo_rows // 2, wo_rows // 4
    b_mine = pl.multiple_of(h * b_half, b_quarter)
    b_mid = pl.multiple_of(h * b_half + b_quarter, b_quarter)
    b_other = pl.multiple_of(hh * b_half, b_quarter)
    q_mine = pl.multiple_of(h * q_half, LANES)
    kv_mine = pl.multiple_of(h * kv_half, LANES)
    starts = [pl.multiple_of(lax.div(chip_cols * xx, LANES) * LANES, LANES) for xx in (x, xr, xo, xl)]
    x_start, xr_start, xo_start, xl_start = starts
    xo_mid = pl.multiple_of(xo_start + win // 2, LANES)
    shift = lax.rem(chip_cols * x, LANES)
    wd_mine = pl.ds(pl.multiple_of(shift + wd_rows * c, 32), wd_rows)
    wd_twin = pl.ds(pl.multiple_of(shift + wd_rows * cc, 32), wd_rows)

    msg_ids = {}
    pending = {}

    def copy_of(name, src, dst, dev):
        i = msg_ids.setdefault(name, len(msg_ids))
        return pltpu.make_async_remote_copy(src, dst, send_sem.at[i], recv_sem.at[i], device_id=dev, device_id_type=MESH)

    def send(name, pairs, dev, view=None):
        for src, dst in pairs:
            copy_of(name, src, dst, dev).start()
        pending[name] = pairs[0][0] if view is None else view

    def got(name, view):
        copy_of(name, view, view, right).wait_recv()

    def drain(names):
        for name in names:
            view = pending.pop(name)
            copy_of(name, view, view, right).wait_send()

    def local_start(sem, pairs):
        for src, dst in pairs:
            pltpu.make_async_copy(src, dst, loc_sem.at[sem]).start()

    def local_wait(sem, view):
        pltpu.make_async_copy(view, view, loc_sem.at[sem]).wait()

    def kv_copies(i, slot):
        layer, group = lax.div(i, groups), lax.rem(i, groups)
        seqs = pl.ds(group * SEQ_GROUP, SEQ_GROUP)
        return (
            pltpu.make_async_copy(kc_ref.at[layer, seqs, 0], kbuf.at[slot], kv_sem.at[slot, 0]),
            pltpu.make_async_copy(vc_ref.at[layer, seqs, 0], vbuf.at[slot], kv_sem.at[slot, 1]),
        )

    def kv_start(i, slot):
        for copy in kv_copies(i, slot):
            copy.start()

    def a_pairs(l, hf, q_lo, kv_lo):
        dst = abuf_w.at[l, hf, x, c]
        return [
            (wq_ref.at[l, :, pl.ds(q_lo, q_half)], dst.at[:, pl.ds(0, q_half)]),
            (wk_ref.at[l, :, pl.ds(kv_lo, kv_half)], dst.at[:, pl.ds(q_half, kv_half)]),
            (wv_ref.at[l, :, pl.ds(kv_lo, kv_half)], dst.at[:, pl.ds(q_half + kv_half, kv_half)]),
        ]

    def a_both(l):
        return a_pairs(l, 0, 0, 0) + a_pairs(l, 1, q_half, kv_half)

    def a_block(l, xx):
        return abuf_w.at[l, h, xx, c] if SHARE_A[l] else abuf_w.at[l, :, xx, c]

    def a_lead(l, xx):
        return abuf_w.at[l, h, xx, c, :, pl.ds(0, a_cols // 2)] if SHARE_A[l] else abuf_w.at[l, 0, xx, c]

    def a_tail(l, xx):
        return abuf_w.at[l, h, xx, c, :, pl.ds(a_cols // 2, a_cols // 2)] if SHARE_A[l] else abuf_w.at[l, 1, xx, c]

    def ao(l):
        pairs = a_pairs(l, h, q_mine, kv_mine) if SHARE_A[l] else a_both(l)
        send(f"aR{l}", pairs, right, a_block(l, x))
        send(f"aL{l}", pairs, left, a_block(l, x))

    def to_pair(name, view):
        send(name, [(view, view)], pair)

    def af(l):
        got(f"aR{l}", a_block(l, xl))
        send(f"afR{l}", [(a_lead(l, xl), a_lead(l, xl))], right)
        got(f"aL{l}", a_block(l, xr))
        send(f"afL{l}", [(a_tail(l, xr), a_tail(l, xr))], left)
        if SHARE_A[l]:
            to_pair(f"paR{l}", a_block(l, xl))
            to_pair(f"paL{l}", a_block(l, xr))

    def ax(l):
        got(f"afR{l}", a_lead(l, xo))
        got(f"afL{l}", a_tail(l, xo))
        if SHARE_A[l]:
            to_pair(f"paF{l}", a_block(l, xo))
        local_wait(4 * l, abuf_w.at[l, :, x, c])
        view = abuf_w.at[l, h, :, c] if SHARE_A[l] else abuf_w.at[l, :, :, c]
        send(f"aT{l}", [(view, view)], twin)

    def aw(l):
        for name, xx in (("paR", xl), ("paL", xr), ("paF", xo)):
            got(f"{name}{l}", abuf_w.at[l, hh, xx, c])
        view = abuf_w.at[l, hh, :, c]
        send(f"aT1{l}", [(view, view)], twin)

    def a_ready(l):
        if SHARE_A[l]:
            got(f"aT{l}", abuf_w.at[l, h, :, cc])
            got(f"aT1{l}", abuf_w.at[l, hh, :, cc])
        else:
            got(f"aT{l}", abuf_w.at[l, :, :, cc])

    def b_block(l, xx):
        return bbuf_w.at[l, xx, c, pl.ds(b_mine, b_half)] if SHARE_B[l] else bbuf_w.at[l, xx, c]

    def b_lead(l, xx):
        return bbuf_w.at[l, xx, c, pl.ds(b_mine, b_quarter)] if SHARE_B[l] else bbuf_w.at[l, xx, c, pl.ds(0, b_half)]

    def b_tail(l, xx):
        return bbuf_w.at[l, xx, c, pl.ds(b_mid, b_quarter)] if SHARE_B[l] else bbuf_w.at[l, xx, c, pl.ds(b_half, b_half)]

    def bo(l):
        src = wo_ref.at[l, pl.ds(b_mine, b_half)] if SHARE_B[l] else wo_ref.at[l]
        send(f"bR{l}", [(src, b_block(l, x))], right)
        send(f"bL{l}", [(src, b_block(l, x))], left)

    def bf(l):
        got(f"bR{l}", b_block(l, xl))
        send(f"bfR{l}", [(b_lead(l, xl), b_lead(l, xl))], right)
        got(f"bL{l}", b_block(l, xr))
        send(f"bfL{l}", [(b_tail(l, xr), b_tail(l, xr))], left)
        if SHARE_B[l]:
            to_pair(f"pbR{l}", b_block(l, xl))
            to_pair(f"pbL{l}", b_block(l, xr))

    def bx(l):
        got(f"bfR{l}", b_lead(l, xo))
        got(f"bfL{l}", b_tail(l, xo))
        if SHARE_B[l]:
            to_pair(f"pbF{l}", b_block(l, xo))
        local_wait(4 * l + 1, bbuf_w.at[l, x, c])
        view = bbuf_w.at[l, :, c, pl.ds(b_mine, b_half)] if SHARE_B[l] else bbuf_w.at[l, :, c]
        send(f"bT{l}", [(view, view)], twin)

    def bw(l):
        for name, xx in (("pbR", xl), ("pbL", xr), ("pbF", xo)):
            got(f"{name}{l}", bbuf_w.at[l, xx, c, pl.ds(b_other, b_half)])
        view = bbuf_w.at[l, :, c, pl.ds(b_other, b_half)]
        send(f"bT1{l}", [(view, view)], twin)

    def b_ready(l):
        if SHARE_B[l]:
            got(f"bT{l}", bbuf_w.at[l, :, cc, pl.ds(b_mine, b_half)])
            got(f"bT1{l}", bbuf_w.at[l, :, cc, pl.ds(b_other, b_half)])
        else:
            got(f"bT{l}", bbuf_w.at[l, :, cc])

    def by_matrix(l, name, lo, size, dst, dev):
        for value, ref in ((0, wg_ref), (1, wu_ref)):
            @pl.when(h == value)
            def _():
                copy_of(name, ref.at[l, :, pl.ds(lo, size)], dst, dev).start()
        pending[name] = dst

    def cd(l):
        by_matrix(l, f"cR{l}", xr_start, win, gu_w.at[l, h, x, c], right)
        by_matrix(l, f"cL{l}", xl_start, win, gu_w.at[l, h, x, c], left)

    def ct(l):
        by_matrix(l, f"tR{l}", xo_start, win // 2, tr_w.at[l, 0], right)
        by_matrix(l, f"tL{l}", xo_mid, win // 2, tr_w.at[l, 1], left)

    def cf(l):
        got(f"tR{l}", tr_w.at[l, 0])
        send(f"cfR{l}", [(tr_w.at[l, 0], gu_w.at[l, h, xl, c, :, pl.ds(0, win // 2)])], right)
        got(f"tL{l}", tr_w.at[l, 1])
        send(f"cfL{l}", [(tr_w.at[l, 1], gu_w.at[l, h, xr, c, :, pl.ds(win // 2, win // 2)])], left)

    def cn(l):
        for name, xx in (("cR", xl), ("cL", xr)):
            got(f"{name}{l}", gu_w.at[l, h, xx, c])
            to_pair(f"p{name}{l}", gu_w.at[l, h, xx, c])

    def cx(l):
        got(f"cfR{l}", gu_w.at[l, h, xo, c, :, pl.ds(0, win // 2)])
        got(f"cfL{l}", gu_w.at[l, h, xo, c, :, pl.ds(win // 2, win // 2)])
        to_pair(f"pcF{l}", gu_w.at[l, h, xo, c])

    def cw(l):
        local_wait(4 * l + 2, gu_w.at[l, :, x, c])
        view = gu_w.at[l, h, :, c]
        send(f"cT{l}", [(view, view)], twin)
        for name, xx in (("pcR", xl), ("pcL", xr), ("pcF", xo)):
            got(f"{name}{l}", gu_w.at[l, hh, xx, c])
        view = gu_w.at[l, hh, :, c]
        send(f"cT1{l}", [(view, view)], twin)

    def c_ready(l):
        got(f"cT{l}", gu_w.at[l, h, :, cc])
        got(f"cT1{l}", gu_w.at[l, hh, :, cc])

    def dt(l):
        send(f"dT{l}", [(wd_ref.at[l], wd_w.at[l, wd_mine])], twin)

    def d_ready(l):
        local_wait(4 * l + 3, wd_w.at[l, wd_mine])
        got(f"dT{l}", wd_w.at[l, wd_twin])

    for l in range(layers):
        start = pl.multiple_of(jnp.where(lax.rem(x, 2) == 0, chip_cols, 0), 64)
        wd_w[l, pl.ds(start, pad), :] = jnp.zeros((pad, width), BF16)
    gsrc[...] = jnp.zeros_like(gsrc)
    gsrc[0:layers, 0:piece] = an_ref[...]
    gsrc[layers:2 * layers, 0:piece] = mn_ref[...]
    gsrc[...] = pltpu.roll(gsrc[...], lax.rem(w * piece, LANES), 1)
    barrier = pltpu.get_barrier_semaphore()
    for i in range(1, n_dev):
        pl.semaphore_signal(barrier, inc=1, device_id=(dp, lax.rem(w + i, n_dev)), device_id_type=MESH)
    pl.semaphore_signal(barrier, inc=1, device_id=pair, device_id_type=MESH)
    pl.semaphore_wait(barrier, n_dev)

    def entry():
        for i in range(1, n_dev):
            copy_of("gain", gsrc, gbuf.at[w], (dp, lax.rem(w + i, n_dev))).start()
        pending["gain"] = gbuf.at[pl.ds(0, n_dev - 1)]
        gbuf[w] = gsrc[...]
        kv_start(0, 0)
        for l in range(layers):
            local_start(4 * l, a_both(l))
            local_start(4 * l + 1, [(wo_ref.at[l], bbuf_w.at[l, x, c])])
            cols = pl.ds(x_start, win)
            local_start(4 * l + 2, [(wg_ref.at[l, :, cols], gu_w.at[l, 0, x, c]), (wu_ref.at[l, :, cols], gu_w.at[l, 1, x, c])])
            local_start(4 * l + 3, [(wd_ref.at[l], wd_w.at[l, wd_mine])])
        kv_start(1, 1)
        hbuf[...] = hid_ref[...]
        lane_block = lax.div(lax.broadcasted_iota(jnp.int32, (1, LANES), 1), SEQ_GROUP)
        for g in range(groups):
            line = pos_ref[...]
            for j in range(heads):
                moved = pltpu.roll(pos_ref[...], lax.rem(w * 0 + (j - g + heads) * SEQ_GROUP, LANES), 1)
                line = jnp.where(lane_block == j, moved, line)
            pos_buf[g] = line

    def all_gains():
        tiles = []
        for j in range(width // LANES):
            total = None
            for s in range(n_dev):
                lo = (s * piece) // LANES
                for k in range(2):
                    if lo + k == j:
                        block = gbuf[s, :, k * LANES:(k + 1) * LANES]
                        total = block if total is None else total + block
            tiles.append(total)
        return 1.0 + jnp.concatenate(tiles, axis=1)

    def rms(hid, row):
        mean_sq = jnp.sum(hid * hid, axis=-1, keepdims=True) / width
        return (hid * lax.rsqrt(mean_sq + EPS) * all_gains()[row:row + 1, :]).astype(BF16)

    chunk = 4

    def attend(l, group):
        lane_seq = lax.rem(lax.broadcasted_iota(jnp.int32, (cache_len, LANES), 1), SEQ_GROUP)
        row_seq = lax.rem(lax.broadcasted_iota(jnp.int32, (LANES, cache_len), 0), SEQ_GROUP)
        row_t = lax.broadcasted_iota(jnp.int32, (cache_len, LANES), 0)
        lane_new = lax.rem(lax.broadcasted_iota(jnp.int32, (SEQ_GROUP, LANES), 1), SEQ_GROUP)
        row_new = lax.broadcasted_iota(jnp.int32, (SEQ_GROUP, LANES), 0)
        i = l * groups + group
        slot = lax.rem(group, 2)
        for copy in kv_copies(i, slot):
            copy.wait()
        seqs = pl.ds(pl.multiple_of(group * SEQ_GROUP, SEQ_GROUP), SEQ_GROUP)
        query = jnp.concatenate([qbuf[j, seqs, :] for j in range(heads)], axis=0)
        scores = jnp.zeros((cache_len, LANES), F32)
        for b in range(0, SEQ_GROUP, chunk):
            block = kbuf[slot, b:b + chunk].reshape(chunk * cache_len, head_dim)
            prod = dot_t(block, query)
            for j in range(chunk):
                scores = jnp.where(lane_seq == b + j, prod[j * cache_len:(j + 1) * cache_len], scores)
        k_new = knew_ref[l, seqs, :].astype(BF16)
        v_new = vnew_ref[l, seqs, :]
        new_score = jnp.sum(jnp.where(row_new == lane_new, dot_t(k_new, query), 0.0), axis=0, keepdims=True)
        scores = jnp.where(row_t < pos_buf[group], scores, -1e30)
        top = jnp.maximum(jnp.max(scores, axis=0, keepdims=True), new_score)
        prob = jnp.exp(scores - top)
        prob_new = jnp.exp(new_score - top)
        total = jnp.sum(prob, axis=0, keepdims=True) + prob_new
        prob_t = prob.T
        total_t = jnp.broadcast_to(total, (LANES, LANES)).T
        new_t = jnp.broadcast_to(prob_new, (LANES, LANES)).T.astype(BF16).astype(F32)
        v_rep = jnp.concatenate([v_new] * heads, axis=0)
        acc = jnp.concatenate([new_t] * (head_dim // LANES), axis=1) * v_rep
        for b in range(0, SEQ_GROUP, chunk):
            spread = jnp.concatenate([jnp.where(row_seq == b + j, prob_t, 0.0).astype(BF16) for j in range(chunk)], axis=1)
            acc = acc + dot(spread, vbuf[slot, b:b + chunk].reshape(chunk * cache_len, head_dim))
        attn = (acc / jnp.concatenate([total_t] * (head_dim // LANES), axis=1)).astype(BF16)
        for j in range(heads):
            abuf[seqs, j * head_dim:(j + 1) * head_dim] = attn[j * SEQ_GROUP:(j + 1) * SEQ_GROUP, :]

        @pl.when(i + 2 < layers * groups)
        def _():
            kv_start(i + 2, slot)

    def qkv(l):
        a_ready(l)
        if l == 0:
            got("gain", gbuf.at[pl.ds(0, n_dev - 1)])
        cos_tab, sin_tab = cos_ref[...], sin_ref[...]
        normed = rms(hbuf[...].astype(F32), l)
        halves = [dot(normed, abuf_w[l, hf].reshape(width, a_cols)) for hf in range(2)]

        def rope(lead, tail):
            return jnp.concatenate([lead * cos_tab - tail * sin_tab, tail * cos_tab + lead * sin_tab], axis=1)

        for j in range(heads):
            out, lo = halves[j // (heads // 2)], (j % (heads // 2)) * head_dim
            qbuf[j] = (rope(out[:, lo:lo + half], out[:, lo + half:lo + head_dim]) * head_dim ** -0.5).astype(BF16)
        knew_ref[l] = rope(halves[0][:, q_half:q_half + half], halves[1][:, q_half:q_half + half]).astype(BF16).astype(F32)
        vnew_ref[l] = jnp.concatenate([hv[:, q_half + half:q_half + 2 * half] for hv in halves], axis=1).astype(BF16).astype(F32)

    r2 = rows // 2
    upper, lower = pl.ds(0, r2), pl.ds(r2, r2)

    def mix(l):
        b_ready(l)
        mixed = dot(abuf[...], bbuf_w[l].reshape(heads * head_dim, width))
        hid_mid = (hbuf[...].astype(F32) + mixed).astype(BF16)
        hbuf[...] = hid_mid
        y_all[l, x] = rms(hid_mid.astype(F32), layers + l)
        top, bottom = y_all.at[l, x, upper], y_all.at[l, x, lower]
        send(f"yR1{l}", [(top, top)], right)
        send(f"yL1{l}", [(bottom, bottom)], left)
        send(f"yR2{l}", [(bottom, bottom)], right)
        send(f"yL2{l}", [(top, top)], left)

    def yf(l):
        view = y_all.at[l, xl, upper]
        got(f"yR1{l}", view)
        send(f"yfR{l}", [(view, view)], right)
        view = y_all.at[l, xr, lower]
        got(f"yL1{l}", view)
        send(f"yfL{l}", [(view, view)], left)

    n_tile = 2 * LANES

    def gate_up(l, blocks):
        @pl.loop(0, win // n_tile)
        def _(n):
            cols = pl.ds(pl.multiple_of(n * n_tile, n_tile), n_tile)
            act = jnp.concatenate([y_all[l, b] for b in blocks], axis=0)
            gate = dot(act, gu_w[l, 0, :, :, :, cols].reshape(width, n_tile))
            up = dot(act, gu_w[l, 1, :, :, :, cols].reshape(width, n_tile))
            mid = (jax.nn.gelu(gate, approximate=True) * up).astype(BF16)
            for k, b in enumerate(blocks):
                m_buf[b, :, cols] = mid[k * rows:(k + 1) * rows]

    def guo(l):
        if l:
            c_ready(l)
        gate_up(l, (x,))

    def gua(l):
        got(f"yR2{l}", y_all.at[l, xl, lower])
        got(f"yL2{l}", y_all.at[l, xr, upper])
        if not l:
            c_ready(l)
        gate_up(l, (xl, xr))

    def gub(l):
        got(f"yfR{l}", y_all.at[l, xo, upper])
        got(f"yfL{l}", y_all.at[l, xo, lower])
        gate_up(l, (xo,))

    def down(l, xx):
        part[xx] = dot(m_buf[xx], wd_w[l])

    last = layers - 1

    def export(src, dst):
        pltpu.make_async_copy(src, dst, out_sem.at[len(exports)]).start()
        exports.append((src, dst))

    exports = []

    def near(l):
        if l:
            drain([f"{name}{l - 1}" for name in ("eR2", "eL2", "eR3", "eL3")])
        down(l, xr)
        if l == last:
            export(part.at[xr, lower], near_r)
            export(part.at[xr, upper], next_r)
        else:
            send(f"eR2{l}", [(part.at[xr, lower], r_f.at[l, 0, lower])], right)
        down(l, xl)
        if l == last:
            export(part.at[xl, upper], near_l)
            export(part.at[xl, lower], next_l)
        else:
            send(f"eL2{l}", [(part.at[xl, upper], r_f.at[l, 1, upper])], left)

    def far(l):
        if l:
            drain([f"{name}{l - 1}" for name in ("eR1", "eL1")])
        down(l, xo)
        if l == last:
            export(part.at[xo, upper], far_r)
            export(part.at[xo, lower], far_l)
        else:
            send(f"eR1{l}", [(part.at[xo, upper], r_t.at[l, 0])], right)
            send(f"eL1{l}", [(part.at[xo, lower], r_t.at[l, 1])], left)

    def er(l):
        got(f"eR1{l}", r_t.at[l, 0])
        part[xr, 0:r2] = part[xr, 0:r2] + r_t[l, 0]
        send(f"eR3{l}", [(part.at[xr, upper], r_f.at[l, 0, upper])], right)
        got(f"eL1{l}", r_t.at[l, 1])
        part[xl, r2:rows] = part[xl, r2:rows] + r_t[l, 1]
        send(f"eL3{l}", [(part.at[xl, lower], r_f.at[l, 1, lower])], left)

    def own(l):
        down(l, x)
        if l == last:
            export(part.at[x], own_out)
            hid_out[...] = hbuf[...]

    def done(l):
        got(f"eR2{l}", r_f.at[l, 0, lower])
        got(f"eL2{l}", r_f.at[l, 1, upper])
        got(f"eR3{l}", r_f.at[l, 0, upper])
        got(f"eL3{l}", r_f.at[l, 1, lower])
        hbuf[...] = (hbuf[...].astype(F32) + (part[x] + r_f[l, 0] + r_f[l, 1])).astype(BF16)

    table = dict(
        ao=ao, af=af, ax=ax, aw=aw, bo=bo, bf=bf, bx=bx, bw=bw, cd=cd, ct=ct, cf=cf, cn=cn, cx=cx, cw=cw, dt=dt,
        qkv=qkv, mix=mix, yf=yf, guo=guo, gua=gua, gub=gub, dr=d_ready, near=near, far=far, er=er, own=own, done=done,
    )

    def run(step):
        table[step[:-1]](int(step[-1]))

    entry()
    at = 0
    reached = [0] * layers
    while at < len(ORDER):
        step = ORDER[at]
        if not step.startswith("att"):
            run(step)
            at += 1
            continue
        l, count = int(step[-1]), 0
        while ORDER[at] == step:
            count += 1
            at += 1
        first = reached[l]
        reached[l] += count

        @pl.loop(first, first + count)
        def _(group):
            attend(l, group)

    drain(list(pending))
    for i, (src, dst) in enumerate(exports):
        pltpu.make_async_copy(src, dst, out_sem.at[i]).wait()
    assert len(msg_ids) <= send_sem.shape[0]


def decode(hidden, positions, k_cache, v_cache, attn_norm, w_query, w_key, w_value, w_out, mlp_norm, w_gate, w_up, w_down):
    layers, rows, _, cache_len, head_dim = k_cache.shape
    width = hidden.shape[1]
    n_dev = lax.axis_size("w")
    ff = w_gate.shape[-1]
    heads = w_query.shape[-1] // head_dim
    chip_cols = ff // CHIPS
    win = -(-(chip_cols + LANES // 2) // LANES) * LANES
    piece = width // n_dev
    groups = rows // SEQ_GROUP
    assert n_dev == CHIPS * CORES and heads * SEQ_GROUP == LANES and cache_len == LANES and rows == LANES
    assert lax.axis_size("dp") % 2 == 0
    cos_tab, sin_tab = rope_tables(positions, head_dim)
    dims = (layers, rows, width, heads, head_dim, cache_len, n_dev, ff)
    vmem, anym = pl.BlockSpec(memory_space=pltpu.VMEM), pl.BlockSpec(memory_space=pl.ANY)
    new_shape = jax.ShapeDtypeStruct((layers, rows, head_dim), F32)
    half_sum = jax.ShapeDtypeStruct((rows // 2, width), F32)
    n_msg = 96
    return pl.pallas_call(
        functools.partial(decode_kernel, dims),
        out_shape=(jax.ShapeDtypeStruct(hidden.shape, BF16), new_shape, new_shape) + (half_sum,) * 6 + (jax.ShapeDtypeStruct(hidden.shape, F32),),
        in_specs=[vmem] * 6 + [anym] * 9,
        out_specs=(vmem,) * 3 + (anym,) * 7,
        scratch_shapes=[
            pltpu.VMEM((8, 2 * LANES), F32),
            pltpu.VMEM((n_dev, 8, 2 * LANES), F32),
            pltpu.VMEM((groups, 1, LANES), jnp.int32),
            pltpu.VMEM((layers, 2, CHIPS, CORES, piece, w_query.shape[-1] // 2 + head_dim), BF16),
            pltpu.VMEM((layers, CHIPS, CORES, w_out.shape[1], width), BF16),
            pltpu.VMEM((layers, 2, CHIPS, CORES, piece, win), BF16),
            pltpu.VMEM((layers, win, width), BF16),
            pltpu.VMEM((layers, 2, piece, win // 2), BF16),
            pltpu.VMEM((layers, CHIPS, rows, width), BF16),
            pltpu.VMEM((CHIPS, rows, win), BF16),
            pltpu.VMEM((CHIPS, rows, width), F32),
            pltpu.VMEM((layers - 1, 2, rows // 2, width), F32),
            pltpu.VMEM((layers - 1, 2, rows, width), F32),
            pltpu.VMEM((2, SEQ_GROUP, cache_len, head_dim), BF16),
            pltpu.VMEM((2, SEQ_GROUP, cache_len, head_dim), BF16),
            pltpu.VMEM((heads, rows, head_dim), BF16),
            pltpu.VMEM((rows, heads * head_dim), BF16),
            pltpu.VMEM((rows, width), BF16),
            pltpu.SemaphoreType.DMA((n_msg,)),
            pltpu.SemaphoreType.DMA((n_msg,)),
            pltpu.SemaphoreType.DMA((4 * layers,)),
            pltpu.SemaphoreType.DMA((2, 2)),
            pltpu.SemaphoreType.DMA((7,)),
        ],
        compiler_params=pltpu.CompilerParams(collective_id=0, has_side_effects=True, vmem_limit_bytes=67043328),
        name="decode",
    )(hidden, cos_tab, sin_tab, attn_norm, mlp_norm, positions.reshape(1, rows), k_cache, v_cache, w_query, w_key, w_value, w_out, w_gate, w_up, w_down)


TILE_ROWS = 16
CACHE_BLOCK = 32
CACHE_SLOTS = 6


def cache_kernel(pos_ref, old_ref, new_ref, out_ref, buf, in_sem, out_sem):
    layers, rows = old_ref.shape[:2]
    blocks = rows // CACHE_BLOCK
    steps = [(l, b) for l in range(layers) for b in range(blocks)]

    def load(i):
        l, b = steps[i]
        slot = i % CACHE_SLOTS
        return pltpu.make_async_copy(old_ref.at[l, pl.ds(b * CACHE_BLOCK, CACHE_BLOCK), 0], buf.at[slot], in_sem.at[slot])

    def store(i):
        l, b = steps[i]
        slot = i % CACHE_SLOTS
        return pltpu.make_async_copy(buf.at[slot], out_ref.at[l, pl.ds(b * CACHE_BLOCK, CACHE_BLOCK), 0], out_sem.at[slot])

    ahead = CACHE_SLOTS // 2
    for i in range(ahead):
        load(i).start()
    row = lax.broadcasted_iota(jnp.int32, (TILE_ROWS, buf.shape[-1]), 0)
    for i in range(len(steps)):
        load(i).wait()
        l, b = steps[i]
        slot = i % CACHE_SLOTS

        @pl.loop(0, CACHE_BLOCK)
        def _(s):
            pos = pos_ref[b * CACHE_BLOCK + s]
            base = pl.multiple_of(pos // TILE_ROWS * TILE_ROWS, TILE_ROWS)
            tile = buf[slot, s, pl.ds(base, TILE_ROWS), :].astype(F32)
            fresh = new_ref[l, pl.ds(b * CACHE_BLOCK + s, 1), :]
            buf[slot, s, pl.ds(base, TILE_ROWS), :] = jnp.where(row == pos - base, fresh, tile).astype(BF16)

        store(i).start()
        nxt = i + ahead
        if nxt < len(steps):
            if nxt >= CACHE_SLOTS:
                store(nxt - CACHE_SLOTS).wait()
            load(nxt).start()
    for i in range(max(0, len(steps) - CACHE_SLOTS), len(steps)):
        store(i).wait()


def write_cache(positions, cache, new_rows):
    cache_len, head_dim = cache.shape[-2:]
    vmem, anym = pl.BlockSpec(memory_space=pltpu.VMEM), pl.BlockSpec(memory_space=pl.ANY)
    return pl.pallas_call(
        cache_kernel,
        out_shape=jax.ShapeDtypeStruct(cache.shape, BF16),
        in_specs=[pl.BlockSpec(memory_space=pltpu.SMEM), anym, vmem],
        out_specs=anym,
        scratch_shapes=[
            pltpu.VMEM((CACHE_SLOTS, CACHE_BLOCK, cache_len, head_dim), BF16),
            pltpu.SemaphoreType.DMA((CACHE_SLOTS,)),
            pltpu.SemaphoreType.DMA((CACHE_SLOTS,)),
        ],
        cost_estimate=pl.CostEstimate(flops=10**11, bytes_accessed=4 * cache.size, transcendentals=0),
        compiler_params=pltpu.CompilerParams(vmem_limit_bytes=60 * 2**20),
        name="cache",
    )(positions, cache, new_rows)


def solution(mesh):
    batch_spec = P(("dp", "w"))
    cache_spec = P(None, ("dp", "w"))
    gain_spec = P(None, "w")
    weight_spec = P(None, "w", None)

    def per_device(hidden, positions, k_cache, v_cache, *weights):
        hid_mid, k_new, v_new, far_r, far_l, near_r, near_l, next_r, next_l, own = decode(hidden, positions, k_cache, v_cache, *weights)
        n_dev = mesh.shape["w"]
        ahead = [(i, (i + CORES) % n_dev) for i in range(n_dev)]
        back = [(i, (i - CORES) % n_dev) for i in range(n_dev)]
        got_r = lax.ppermute(far_r, "w", ahead)
        got_l = lax.ppermute(far_l, "w", back)
        low = lax.ppermute(near_r, "w", ahead)
        high = lax.ppermute(near_l, "w", back)
        k_out = write_cache(positions, k_cache, k_new)
        far_high = lax.ppermute(next_r + got_r, "w", ahead)
        far_low = lax.ppermute(next_l + got_l, "w", back)
        v_out = write_cache(positions, v_cache, v_new)
        total = own + jnp.concatenate([high + far_high, low + far_low], axis=0)
        hidden_out = (hid_mid.astype(F32) + total).astype(BF16)
        return hidden_out, k_out, v_out

    in_specs = (batch_spec, batch_spec, cache_spec, cache_spec, gain_spec, weight_spec, weight_spec, weight_spec, weight_spec, gain_spec, weight_spec, weight_spec, weight_spec)
    out_specs = (batch_spec, cache_spec, cache_spec)
    return jax.shard_map(per_device, mesh=mesh, in_specs=in_specs, out_specs=out_specs, check_vma=False)
```

```python
import functools

import jax
import jax.numpy as jnp
from jax import lax
from jax.experimental import pallas as pl
from jax.experimental.pallas import tpu as pltpu
from jax.sharding import PartitionSpec as P

EPS = 1e-6
ROPE_BASE = 10000.0
LANES = 128
CORES = 2
CHIPS = 4
SEQ_GROUP = 32
MESH = pl.DeviceIdType.MESH
F32 = jnp.float32
BF16 = jnp.bfloat16


def dot(a, b):
    return jnp.dot(a, b, preferred_element_type=F32)


def dot_t(a, b):
    return lax.dot_general(a, b, (((1,), (1,)), ((), ())), preferred_element_type=F32)


ORDER = (
    "bo0", "ao0", "ct0", "bf0", "af0", "cf0", "cd0", "ct1", "bx0", "ax0", "cx0", "aw0", "dt0", "qkv0",
    "att0", "bw0", "ao1", "att0", "att0", "cd1", "cn0", "af1", "att0", "mix0", "yf0", "cf1", "cw0", "ax1", "dt1", "dr0",
    "gua0", "near0", "cn1", "gub0", "far0", "bo1", "er0", "guo0", "own0", "bf1", "aw1", "cx1", "done0", "qkv1",
    "att1", "att1", "bx1", "att1", "att1", "mix1", "cw1", "yf1", "guo1", "dr1", "own1", "gua1", "near1", "gub1", "far1",
)
SHARE_A = (True, True)
SHARE_B = (True, False)


def decode_kernel(
    dims,
    hid_ref, freq_ref, an_ref, mn_ref, pos_ref, kc_ref, vc_ref,
    wq_ref, wk_ref, wv_ref, wo_ref, wg_ref, wu_ref, wd_ref,
    hid_out, knew_ref, vnew_ref, first_r, first_l, next_r, next_l, own_out,
    cos_buf, sin_buf, act_buf, gsrc, gbuf, pos_buf, abuf_w, bbuf_w, gu_w, wd_w, tr_w, y_all, m_buf, part, r_t, r_f,
    kbuf, vbuf, qbuf, abuf, hbuf,
    send_sem, recv_sem, loc_sem, kv_sem, out_sem,
):
    layers, rows, width, heads, head_dim, cache_len, n_dev, ff = dims
    half = head_dim // 2
    piece = width // n_dev
    chip_cols = ff // CHIPS
    win = gu_w.shape[-1]
    pad = win - chip_cols
    wd_rows = wd_ref.shape[1]
    wo_rows = wo_ref.shape[1]
    q_half = wq_ref.shape[-1] // 2
    kv_half = half
    a_cols = abuf_w.shape[-1]
    groups = rows // SEQ_GROUP
    w = lax.axis_index("w")
    dp = lax.axis_index("dp")
    x, c = lax.div(w, CORES), lax.rem(w, CORES)
    h = lax.rem(dp, 2)
    xr, xo, xl = lax.rem(x + 1, CHIPS), lax.rem(x + 2, CHIPS), lax.rem(x + 3, CHIPS)
    cc = 1 - c
    hh = 1 - h
    right, left = (dp, xr * CORES + c), (dp, xl * CORES + c)
    twin = (dp, x * CORES + cc)
    pair = (dp + 1 - 2 * h, w)
    b_half, b_quarter = wo_rows // 2, wo_rows // 4
    b_mine = pl.multiple_of(h * b_half, b_quarter)
    b_mid = pl.multiple_of(h * b_half + b_quarter, b_quarter)
    b_other = pl.multiple_of(hh * b_half, b_quarter)
    q_mine = pl.multiple_of(h * q_half, LANES)
    kv_mine = pl.multiple_of(h * kv_half, LANES)
    starts = [pl.multiple_of(lax.div(chip_cols * xx, LANES) * LANES, LANES) for xx in (x, xr, xo, xl)]
    x_start, xr_start, xo_start, xl_start = starts
    xo_mid = pl.multiple_of(xo_start + win // 2, LANES)
    shift = lax.rem(chip_cols * x, LANES)
    wd_mine = pl.ds(pl.multiple_of(shift + wd_rows * c, 32), wd_rows)
    wd_twin = pl.ds(pl.multiple_of(shift + wd_rows * cc, 32), wd_rows)

    msg_ids = {}
    pending = {}

    def copy_of(name, src, dst, dev):
        i = msg_ids.setdefault(name, len(msg_ids))
        return pltpu.make_async_remote_copy(src, dst, send_sem.at[i], recv_sem.at[i], device_id=dev, device_id_type=MESH)

    def send(name, pairs, dev, view=None):
        for src, dst in pairs:
            copy_of(name, src, dst, dev).start()
        pending[name] = pairs[0][0] if view is None else view

    def got(name, view):
        copy_of(name, view, view, right).wait_recv()

    def drain(names):
        for name in names:
            view = pending.pop(name)
            copy_of(name, view, view, right).wait_send()

    def local_start(sem, pairs):
        for src, dst in pairs:
            pltpu.make_async_copy(src, dst, loc_sem.at[sem]).start()

    def local_wait(sem, view):
        pltpu.make_async_copy(view, view, loc_sem.at[sem]).wait()

    def kv_copies(i, slot):
        layer, group = lax.div(i, groups), lax.rem(i, groups)
        seqs = pl.ds(group * SEQ_GROUP, SEQ_GROUP)
        return (
            pltpu.make_async_copy(kc_ref.at[layer, seqs, 0], kbuf.at[slot], kv_sem.at[slot, 0]),
            pltpu.make_async_copy(vc_ref.at[layer, seqs, 0], vbuf.at[slot], kv_sem.at[slot, 1]),
        )

    def kv_start(i, slot):
        for copy in kv_copies(i, slot):
            copy.start()

    def a_pairs(l, hf, q_lo, kv_lo):
        dst = abuf_w.at[l, hf, x, c]
        return [
            (wq_ref.at[l, :, pl.ds(q_lo, q_half)], dst.at[:, pl.ds(0, q_half)]),
            (wk_ref.at[l, :, pl.ds(kv_lo, kv_half)], dst.at[:, pl.ds(q_half, kv_half)]),
            (wv_ref.at[l, :, pl.ds(kv_lo, kv_half)], dst.at[:, pl.ds(q_half + kv_half, kv_half)]),
        ]

    def a_both(l):
        return a_pairs(l, 0, 0, 0) + a_pairs(l, 1, q_half, kv_half)

    def a_block(l, xx):
        return abuf_w.at[l, h, xx, c] if SHARE_A[l] else abuf_w.at[l, :, xx, c]

    def a_lead(l, xx):
        return abuf_w.at[l, h, xx, c, :, pl.ds(0, a_cols // 2)] if SHARE_A[l] else abuf_w.at[l, 0, xx, c]

    def a_tail(l, xx):
        return abuf_w.at[l, h, xx, c, :, pl.ds(a_cols // 2, a_cols // 2)] if SHARE_A[l] else abuf_w.at[l, 1, xx, c]

    def ao(l):
        pairs = a_pairs(l, h, q_mine, kv_mine) if SHARE_A[l] else a_both(l)
        send(f"aR{l}", pairs, right, a_block(l, x))
        send(f"aL{l}", pairs, left, a_block(l, x))

    def to_pair(name, view):
        send(name, [(view, view)], pair)

    def af(l):
        got(f"aR{l}", a_block(l, xl))
        send(f"afR{l}", [(a_lead(l, xl), a_lead(l, xl))], right)
        got(f"aL{l}", a_block(l, xr))
        send(f"afL{l}", [(a_tail(l, xr), a_tail(l, xr))], left)
        if SHARE_A[l]:
            to_pair(f"paR{l}", a_block(l, xl))
            to_pair(f"paL{l}", a_block(l, xr))

    def ax(l):
        got(f"afR{l}", a_lead(l, xo))
        got(f"afL{l}", a_tail(l, xo))
        if SHARE_A[l]:
            to_pair(f"paF{l}", a_block(l, xo))
        local_wait(4 * l, abuf_w.at[l, :, x, c])
        view = abuf_w.at[l, h, :, c] if SHARE_A[l] else abuf_w.at[l, :, :, c]
        send(f"aT{l}", [(view, view)], twin)

    def aw(l):
        for name, xx in (("paR", xl), ("paL", xr), ("paF", xo)):
            got(f"{name}{l}", abuf_w.at[l, hh, xx, c])
        view = abuf_w.at[l, hh, :, c]
        send(f"aT1{l}", [(view, view)], twin)

    def a_ready(l):
        if SHARE_A[l]:
            got(f"aT{l}", abuf_w.at[l, h, :, cc])
            got(f"aT1{l}", abuf_w.at[l, hh, :, cc])
        else:
            got(f"aT{l}", abuf_w.at[l, :, :, cc])

    def b_block(l, xx):
        return bbuf_w.at[l, xx, c, pl.ds(b_mine, b_half)] if SHARE_B[l] else bbuf_w.at[l, xx, c]

    def b_lead(l, xx):
        return bbuf_w.at[l, xx, c, pl.ds(b_mine, b_quarter)] if SHARE_B[l] else bbuf_w.at[l, xx, c, pl.ds(0, b_half)]

    def b_tail(l, xx):
        return bbuf_w.at[l, xx, c, pl.ds(b_mid, b_quarter)] if SHARE_B[l] else bbuf_w.at[l, xx, c, pl.ds(b_half, b_half)]

    def bo(l):
        src = wo_ref.at[l, pl.ds(b_mine, b_half)] if SHARE_B[l] else wo_ref.at[l]
        send(f"bR{l}", [(src, b_block(l, x))], right)
        send(f"bL{l}", [(src, b_block(l, x))], left)

    def bf(l):
        got(f"bR{l}", b_block(l, xl))
        send(f"bfR{l}", [(b_lead(l, xl), b_lead(l, xl))], right)
        got(f"bL{l}", b_block(l, xr))
        send(f"bfL{l}", [(b_tail(l, xr), b_tail(l, xr))], left)
        if SHARE_B[l]:
            to_pair(f"pbR{l}", b_block(l, xl))
            to_pair(f"pbL{l}", b_block(l, xr))

    def bx(l):
        got(f"bfR{l}", b_lead(l, xo))
        got(f"bfL{l}", b_tail(l, xo))
        if SHARE_B[l]:
            to_pair(f"pbF{l}", b_block(l, xo))
        local_wait(4 * l + 1, bbuf_w.at[l, x, c])
        view = bbuf_w.at[l, :, c, pl.ds(b_mine, b_half)] if SHARE_B[l] else bbuf_w.at[l, :, c]
        send(f"bT{l}", [(view, view)], twin)

    def bw(l):
        for name, xx in (("pbR", xl), ("pbL", xr), ("pbF", xo)):
            got(f"{name}{l}", bbuf_w.at[l, xx, c, pl.ds(b_other, b_half)])
        view = bbuf_w.at[l, :, c, pl.ds(b_other, b_half)]
        send(f"bT1{l}", [(view, view)], twin)

    def b_ready(l):
        if SHARE_B[l]:
            got(f"bT{l}", bbuf_w.at[l, :, cc, pl.ds(b_mine, b_half)])
            got(f"bT1{l}", bbuf_w.at[l, :, cc, pl.ds(b_other, b_half)])
        else:
            got(f"bT{l}", bbuf_w.at[l, :, cc])

    def by_matrix(l, name, lo, size, dst, dev):
        for value, ref in ((0, wg_ref), (1, wu_ref)):
            @pl.when(h == value)
            def _():
                copy_of(name, ref.at[l, :, pl.ds(lo, size)], dst, dev).start()
        pending[name] = dst

    def cd(l):
        by_matrix(l, f"cR{l}", xr_start, win, gu_w.at[l, h, x, c], right)
        by_matrix(l, f"cL{l}", xl_start, win, gu_w.at[l, h, x, c], left)

    def ct(l):
        by_matrix(l, f"tR{l}", xo_start, win // 2, tr_w.at[l, 0], right)
        by_matrix(l, f"tL{l}", xo_mid, win // 2, tr_w.at[l, 1], left)

    def cf(l):
        got(f"tR{l}", tr_w.at[l, 0])
        send(f"cfR{l}", [(tr_w.at[l, 0], gu_w.at[l, h, xl, c, :, pl.ds(0, win // 2)])], right)
        got(f"tL{l}", tr_w.at[l, 1])
        send(f"cfL{l}", [(tr_w.at[l, 1], gu_w.at[l, h, xr, c, :, pl.ds(win // 2, win // 2)])], left)

    def cn(l):
        for name, xx in (("cR", xl), ("cL", xr)):
            got(f"{name}{l}", gu_w.at[l, h, xx, c])
            to_pair(f"p{name}{l}", gu_w.at[l, h, xx, c])

    def cx(l):
        got(f"cfR{l}", gu_w.at[l, h, xo, c, :, pl.ds(0, win // 2)])
        got(f"cfL{l}", gu_w.at[l, h, xo, c, :, pl.ds(win // 2, win // 2)])
        to_pair(f"pcF{l}", gu_w.at[l, h, xo, c])

    def cw(l):
        local_wait(4 * l + 2, gu_w.at[l, :, x, c])
        view = gu_w.at[l, h, :, c]
        send(f"cT{l}", [(view, view)], twin)
        for name, xx in (("pcR", xl), ("pcL", xr), ("pcF", xo)):
            got(f"{name}{l}", gu_w.at[l, hh, xx, c])
        view = gu_w.at[l, hh, :, c]
        send(f"cT1{l}", [(view, view)], twin)

    def c_ready(l):
        got(f"cT{l}", gu_w.at[l, h, :, cc])
        got(f"cT1{l}", gu_w.at[l, hh, :, cc])

    def dt(l):
        send(f"dT{l}", [(wd_ref.at[l], wd_w.at[l, wd_mine])], twin)

    def d_ready(l):
        local_wait(4 * l + 3, wd_w.at[l, wd_mine])
        got(f"dT{l}", wd_w.at[l, wd_twin])

    for l in range(layers):
        start = pl.multiple_of(jnp.where(lax.rem(x, 2) == 0, chip_cols, 0), 64)
        wd_w[l, pl.ds(start, pad), :] = jnp.zeros((pad, width), BF16)
    gsrc[...] = jnp.zeros_like(gsrc)
    gsrc[0:layers, 0:piece] = an_ref[...]
    gsrc[layers:2 * layers, 0:piece] = mn_ref[...]
    gsrc[...] = pltpu.roll(gsrc[...], lax.rem(w * piece, LANES), 1)
    barrier = pltpu.get_barrier_semaphore()
    for i in range(1, n_dev):
        pl.semaphore_signal(barrier, inc=1, device_id=(dp, lax.rem(w + i, n_dev)), device_id_type=MESH)
    pl.semaphore_signal(barrier, inc=1, device_id=pair, device_id_type=MESH)
    pl.semaphore_wait(barrier, n_dev)

    def entry():
        for i in range(1, n_dev):
            copy_of("gain", gsrc, gbuf.at[w], (dp, lax.rem(w + i, n_dev))).start()
        pending["gain"] = gbuf.at[pl.ds(0, n_dev - 1)]
        gbuf[w] = gsrc[...]
        kv_start(0, 0)
        for l in range(layers):
            local_start(4 * l, a_both(l))
            local_start(4 * l + 1, [(wo_ref.at[l], bbuf_w.at[l, x, c])])
            cols = pl.ds(x_start, win)
            local_start(4 * l + 2, [(wg_ref.at[l, :, cols], gu_w.at[l, 0, x, c]), (wu_ref.at[l, :, cols], gu_w.at[l, 1, x, c])])
            local_start(4 * l + 3, [(wd_ref.at[l], wd_w.at[l, wd_mine])])
        kv_start(1, 1)
        hbuf[...] = hid_ref[...]
        lane_block = lax.div(lax.broadcasted_iota(jnp.int32, (1, LANES), 1), SEQ_GROUP)
        for g in range(groups):
            line = pos_ref[...]
            for j in range(heads):
                moved = pltpu.roll(pos_ref[...], lax.rem(w * 0 + (j - g + heads) * SEQ_GROUP, LANES), 1)
                line = jnp.where(lane_block == j, moved, line)
            pos_buf[g] = line
        angles = jnp.broadcast_to(pos_ref[...].astype(F32), (rows, rows)).T * freq_ref[...]
        cos_buf[...] = jnp.cos(angles)
        sin_buf[...] = jnp.sin(angles)

    def all_gains():
        tiles = []
        for j in range(width // LANES):
            total = None
            for s in range(n_dev):
                lo = (s * piece) // LANES
                for k in range(2):
                    if lo + k == j:
                        block = gbuf[s, :, k * LANES:(k + 1) * LANES]
                        total = block if total is None else total + block
            tiles.append(total)
        return 1.0 + jnp.concatenate(tiles, axis=1)

    def rms(hid, row):
        mean_sq = jnp.sum(hid * hid, axis=-1, keepdims=True) / width
        return (hid * lax.rsqrt(mean_sq + EPS) * all_gains()[row:row + 1, :]).astype(BF16)

    chunk = 4

    def attend(l, group):
        lane_seq = lax.rem(lax.broadcasted_iota(jnp.int32, (cache_len, LANES), 1), SEQ_GROUP)
        row_seq = lax.rem(lax.broadcasted_iota(jnp.int32, (LANES, cache_len), 0), SEQ_GROUP)
        row_t = lax.broadcasted_iota(jnp.int32, (cache_len, LANES), 0)
        lane_new = lax.rem(lax.broadcasted_iota(jnp.int32, (SEQ_GROUP, LANES), 1), SEQ_GROUP)
        row_new = lax.broadcasted_iota(jnp.int32, (SEQ_GROUP, LANES), 0)
        i = l * groups + group
        slot = lax.rem(group, 2)
        for copy in kv_copies(i, slot):
            copy.wait()
        seqs = pl.ds(pl.multiple_of(group * SEQ_GROUP, SEQ_GROUP), SEQ_GROUP)
        query = jnp.concatenate([qbuf[j, seqs, :] for j in range(heads)], axis=0)
        scores = jnp.zeros((cache_len, LANES), F32)
        for b in range(0, SEQ_GROUP, chunk):
            block = kbuf[slot, b:b + chunk].reshape(chunk * cache_len, head_dim)
            prod = dot_t(block, query)
            for j in range(chunk):
                scores = jnp.where(lane_seq == b + j, prod[j * cache_len:(j + 1) * cache_len], scores)
        k_new = knew_ref[l, seqs, :].astype(BF16)
        v_new = vnew_ref[l, seqs, :]
        new_score = jnp.sum(jnp.where(row_new == lane_new, dot_t(k_new, query), 0.0), axis=0, keepdims=True)
        scores = jnp.where(row_t < pos_buf[group], scores, -1e30)
        top = jnp.maximum(jnp.max(scores, axis=0, keepdims=True), new_score)
        prob = jnp.exp(scores - top)
        prob_new = jnp.exp(new_score - top)
        total = jnp.sum(prob, axis=0, keepdims=True) + prob_new
        prob_t = prob.T
        total_t = jnp.broadcast_to(total, (LANES, LANES)).T
        new_t = jnp.broadcast_to(prob_new, (LANES, LANES)).T.astype(BF16).astype(F32)
        v_rep = jnp.concatenate([v_new] * heads, axis=0)
        acc = jnp.concatenate([new_t] * (head_dim // LANES), axis=1) * v_rep
        for b in range(0, SEQ_GROUP, chunk):
            spread = jnp.concatenate([jnp.where(row_seq == b + j, prob_t, 0.0).astype(BF16) for j in range(chunk)], axis=1)
            acc = acc + dot(spread, vbuf[slot, b:b + chunk].reshape(chunk * cache_len, head_dim))
        attn = (acc / jnp.concatenate([total_t] * (head_dim // LANES), axis=1)).astype(BF16)
        for j in range(heads):
            abuf[seqs, j * head_dim:(j + 1) * head_dim] = attn[j * SEQ_GROUP:(j + 1) * SEQ_GROUP, :]

        @pl.when(i + 2 < layers * groups)
        def _():
            kv_start(i + 2, slot)

    def qkv(l):
        a_ready(l)
        if l == 0:
            got("gain", gbuf.at[pl.ds(0, n_dev - 1)])
        cos_tab, sin_tab = cos_buf[...], sin_buf[...]
        normed = rms(hbuf[...].astype(F32), l)
        halves = [dot(normed, abuf_w[l, hf].reshape(width, a_cols)) for hf in range(2)]

        def rope(lead, tail):
            return jnp.concatenate([lead * cos_tab - tail * sin_tab, tail * cos_tab + lead * sin_tab], axis=1)

        for j in range(heads):
            out, lo = halves[j // (heads // 2)], (j % (heads // 2)) * head_dim
            qbuf[j] = (rope(out[:, lo:lo + half], out[:, lo + half:lo + head_dim]) * head_dim ** -0.5).astype(BF16)
        knew_ref[l] = rope(halves[0][:, q_half:q_half + half], halves[1][:, q_half:q_half + half]).astype(BF16).astype(F32)
        vnew_ref[l] = jnp.concatenate([hv[:, q_half + half:q_half + 2 * half] for hv in halves], axis=1).astype(BF16).astype(F32)

    r2 = rows // 2
    upper, lower = pl.ds(0, r2), pl.ds(r2, r2)

    def mix(l):
        b_ready(l)
        mixed = dot(abuf[...], bbuf_w[l].reshape(heads * head_dim, width))
        hid_mid = (hbuf[...].astype(F32) + mixed).astype(BF16)
        hbuf[...] = hid_mid
        y_all[l, x] = rms(hid_mid.astype(F32), layers + l)
        top, bottom = y_all.at[l, x, upper], y_all.at[l, x, lower]
        send(f"yR1{l}", [(top, top)], right)
        send(f"yL1{l}", [(bottom, bottom)], left)
        send(f"yR2{l}", [(bottom, bottom)], right)
        send(f"yL2{l}", [(top, top)], left)

    def yf(l):
        view = y_all.at[l, xl, upper]
        got(f"yR1{l}", view)
        send(f"yfR{l}", [(view, view)], right)
        view = y_all.at[l, xr, lower]
        got(f"yL1{l}", view)
        send(f"yfL{l}", [(view, view)], left)

    n_tile = 2 * LANES

    def gate_up(l, blocks):
        span = slice(0, len(blocks) * rows)

        def at_tile(n):
            return pl.ds(pl.multiple_of(n * n_tile, n_tile), n_tile)

        def multiply(n, slot):
            act = jnp.concatenate([y_all[l, b] for b in blocks], axis=0)
            for k in range(2):
                act_buf[slot, k, span] = dot(act, gu_w[l, k, :, :, :, at_tile(n)].reshape(width, n_tile))

        def activate(n, slot):
            mid = (jax.nn.gelu(act_buf[slot, 0, span], approximate=True) * act_buf[slot, 1, span]).astype(BF16)
            for k, b in enumerate(blocks):
                m_buf[b, :, at_tile(n)] = mid[k * rows:(k + 1) * rows]

        tiles = win // n_tile
        assert tiles % 2 == 1
        multiply(0, 0)

        @pl.loop(0, tiles // 2)
        def _(k):
            multiply(2 * k + 1, 1)
            activate(2 * k, 0)
            multiply(2 * k + 2, 0)
            activate(2 * k + 1, 1)

        activate(tiles - 1, 0)

    def guo(l):
        if l:
            c_ready(l)
        gate_up(l, (x,))

    def gua(l):
        got(f"yR2{l}", y_all.at[l, xl, lower])
        got(f"yL2{l}", y_all.at[l, xr, upper])
        if not l:
            c_ready(l)
        gate_up(l, (xl, xr))

    def gub(l):
        got(f"yfR{l}", y_all.at[l, xo, upper])
        got(f"yfL{l}", y_all.at[l, xo, lower])
        gate_up(l, (xo,))

    def down(l, xx):
        part[xx] = dot(m_buf[xx], wd_w[l])

    last = layers - 1

    def export(src, dst):
        pltpu.make_async_copy(src, dst, out_sem.at[len(exports)]).start()
        exports.append((src, dst))

    exports = []

    def near(l):
        if l:
            drain([f"{name}{l - 1}" for name in ("eR2", "eL2", "eR3", "eL3")])
        down(l, xr)
        if l == last:
            export(part.at[xr, lower], first_r.at[lower])
            export(part.at[xr, upper], next_r)
        else:
            send(f"eR2{l}", [(part.at[xr, lower], r_f.at[l, 0, lower])], right)
        down(l, xl)
        if l == last:
            export(part.at[xl, upper], first_l.at[upper])
            export(part.at[xl, lower], next_l)
        else:
            send(f"eL2{l}", [(part.at[xl, upper], r_f.at[l, 1, upper])], left)

    def far(l):
        if l:
            drain([f"{name}{l - 1}" for name in ("eR1", "eL1")])
        down(l, xo)
        if l == last:
            export(part.at[xo, upper], first_r.at[upper])
            export(part.at[xo, lower], first_l.at[lower])
        else:
            send(f"eR1{l}", [(part.at[xo, upper], r_t.at[l, 0])], right)
            send(f"eL1{l}", [(part.at[xo, lower], r_t.at[l, 1])], left)

    def er(l):
        got(f"eR1{l}", r_t.at[l, 0])
        part[xr, 0:r2] = part[xr, 0:r2] + r_t[l, 0]
        send(f"eR3{l}", [(part.at[xr, upper], r_f.at[l, 0, upper])], right)
        got(f"eL1{l}", r_t.at[l, 1])
        part[xl, r2:rows] = part[xl, r2:rows] + r_t[l, 1]
        send(f"eL3{l}", [(part.at[xl, lower], r_f.at[l, 1, lower])], left)

    def own(l):
        down(l, x)
        if l == last:
            export(part.at[x], own_out)
            hid_out[...] = hbuf[...]

    def done(l):
        got(f"eR2{l}", r_f.at[l, 0, lower])
        got(f"eL2{l}", r_f.at[l, 1, upper])
        got(f"eR3{l}", r_f.at[l, 0, upper])
        got(f"eL3{l}", r_f.at[l, 1, lower])
        hbuf[...] = (hbuf[...].astype(F32) + (part[x] + r_f[l, 0] + r_f[l, 1])).astype(BF16)

    table = dict(
        ao=ao, af=af, ax=ax, aw=aw, bo=bo, bf=bf, bx=bx, bw=bw, cd=cd, ct=ct, cf=cf, cn=cn, cx=cx, cw=cw, dt=dt,
        qkv=qkv, mix=mix, yf=yf, guo=guo, gua=gua, gub=gub, dr=d_ready, near=near, far=far, er=er, own=own, done=done,
    )

    def run(step):
        table[step[:-1]](int(step[-1]))

    entry()
    at = 0
    reached = [0] * layers
    while at < len(ORDER):
        step = ORDER[at]
        if not step.startswith("att"):
            run(step)
            at += 1
            continue
        l, count = int(step[-1]), 0
        while ORDER[at] == step:
            count += 1
            at += 1
        first = reached[l]
        reached[l] += count

        @pl.loop(first, first + count)
        def _(group):
            attend(l, group)

    drain(list(pending))
    for i, (src, dst) in enumerate(exports):
        pltpu.make_async_copy(src, dst, out_sem.at[i]).wait()
    assert len(msg_ids) <= send_sem.shape[0]


def decode(hidden, positions, k_cache, v_cache, attn_norm, w_query, w_key, w_value, w_out, mlp_norm, w_gate, w_up, w_down):
    layers, rows, _, cache_len, head_dim = k_cache.shape
    width = hidden.shape[1]
    n_dev = lax.axis_size("w")
    ff = w_gate.shape[-1]
    heads = w_query.shape[-1] // head_dim
    chip_cols = ff // CHIPS
    win = -(-(chip_cols + LANES // 2) // LANES) * LANES
    piece = width // n_dev
    groups = rows // SEQ_GROUP
    assert n_dev == CHIPS * CORES and heads * SEQ_GROUP == LANES and cache_len == LANES and rows == LANES
    assert lax.axis_size("dp") % 2 == 0
    inv_freq = ROPE_BASE ** (-2.0 * jnp.arange(head_dim // 2, dtype=F32) / head_dim)
    dims = (layers, rows, width, heads, head_dim, cache_len, n_dev, ff)
    vmem, anym = pl.BlockSpec(memory_space=pltpu.VMEM), pl.BlockSpec(memory_space=pl.ANY)
    new_shape = jax.ShapeDtypeStruct((layers, rows, head_dim), F32)
    whole_sum = jax.ShapeDtypeStruct(hidden.shape, F32)
    half_sum = jax.ShapeDtypeStruct((rows // 2, width), F32)
    n_msg = 96
    return pl.pallas_call(
        functools.partial(decode_kernel, dims),
        out_shape=(jax.ShapeDtypeStruct(hidden.shape, BF16), new_shape, new_shape) + (whole_sum, whole_sum, half_sum, half_sum, whole_sum),
        in_specs=[vmem] * 5 + [anym] * 9,
        out_specs=(vmem,) * 3 + (anym,) * 5,
        scratch_shapes=[
            pltpu.VMEM((rows, head_dim // 2), F32),
            pltpu.VMEM((rows, head_dim // 2), F32),
            pltpu.VMEM((2, 2, 2 * rows, 2 * LANES), F32),
            pltpu.VMEM((8, 2 * LANES), F32),
            pltpu.VMEM((n_dev, 8, 2 * LANES), F32),
            pltpu.VMEM((groups, 1, LANES), jnp.int32),
            pltpu.VMEM((layers, 2, CHIPS, CORES, piece, w_query.shape[-1] // 2 + head_dim), BF16),
            pltpu.VMEM((layers, CHIPS, CORES, w_out.shape[1], width), BF16),
            pltpu.VMEM((layers, 2, CHIPS, CORES, piece, win), BF16),
            pltpu.VMEM((layers, win, width), BF16),
            pltpu.VMEM((layers, 2, piece, win // 2), BF16),
            pltpu.VMEM((layers, CHIPS, rows, width), BF16),
            pltpu.VMEM((CHIPS, rows, win), BF16),
            pltpu.VMEM((CHIPS, rows, width), F32),
            pltpu.VMEM((layers - 1, 2, rows // 2, width), F32),
            pltpu.VMEM((layers - 1, 2, rows, width), F32),
            pltpu.VMEM((2, SEQ_GROUP, cache_len, head_dim), BF16),
            pltpu.VMEM((2, SEQ_GROUP, cache_len, head_dim), BF16),
            pltpu.VMEM((heads, rows, head_dim), BF16),
            pltpu.VMEM((rows, heads * head_dim), BF16),
            pltpu.VMEM((rows, width), BF16),
            pltpu.SemaphoreType.DMA((n_msg,)),
            pltpu.SemaphoreType.DMA((n_msg,)),
            pltpu.SemaphoreType.DMA((4 * layers,)),
            pltpu.SemaphoreType.DMA((2, 2)),
            pltpu.SemaphoreType.DMA((8,)),
        ],
        compiler_params=pltpu.CompilerParams(collective_id=0, has_side_effects=True, vmem_limit_bytes=67043328),
        name="decode",
    )(hidden, inv_freq.reshape(1, head_dim // 2), attn_norm, mlp_norm, positions.reshape(1, rows), k_cache, v_cache, w_query, w_key, w_value, w_out, w_gate, w_up, w_down)


TILE_ROWS = 16
CACHE_BLOCK = 8
CACHE_SLOTS = 24


def cache_kernel(pos_ref, old_ref, new_ref, out_ref, buf, in_sem, out_sem):
    layers, rows = old_ref.shape[:2]
    blocks = rows // CACHE_BLOCK
    steps = [(l, b) for l in range(layers) for b in range(blocks)]

    def load(i):
        l, b = steps[i]
        slot = i % CACHE_SLOTS
        return pltpu.make_async_copy(old_ref.at[l, pl.ds(b * CACHE_BLOCK, CACHE_BLOCK), 0], buf.at[slot], in_sem.at[slot])

    def store(i):
        l, b = steps[i]
        slot = i % CACHE_SLOTS
        return pltpu.make_async_copy(buf.at[slot], out_ref.at[l, pl.ds(b * CACHE_BLOCK, CACHE_BLOCK), 0], out_sem.at[slot])

    ahead = CACHE_SLOTS // 2
    for i in range(ahead):
        load(i).start()
    row = lax.broadcasted_iota(jnp.int32, (TILE_ROWS, buf.shape[-1]), 0)
    for i in range(len(steps)):
        load(i).wait()
        l, b = steps[i]
        slot = i % CACHE_SLOTS

        @pl.loop(0, CACHE_BLOCK)
        def _(s):
            pos = pos_ref[b * CACHE_BLOCK + s]
            base = pl.multiple_of(pos // TILE_ROWS * TILE_ROWS, TILE_ROWS)
            tile = buf[slot, s, pl.ds(base, TILE_ROWS), :].astype(F32)
            fresh = new_ref[l, pl.ds(b * CACHE_BLOCK + s, 1), :]
            buf[slot, s, pl.ds(base, TILE_ROWS), :] = jnp.where(row == pos - base, fresh, tile).astype(BF16)

        store(i).start()
        nxt = i + ahead
        if nxt < len(steps):
            if nxt >= CACHE_SLOTS:
                store(nxt - CACHE_SLOTS).wait()
            load(nxt).start()
    for i in range(max(0, len(steps) - CACHE_SLOTS), len(steps)):
        store(i).wait()


def write_cache(positions, cache, new_rows):
    cache_len, head_dim = cache.shape[-2:]
    vmem, anym = pl.BlockSpec(memory_space=pltpu.VMEM), pl.BlockSpec(memory_space=pl.ANY)
    return pl.pallas_call(
        cache_kernel,
        out_shape=jax.ShapeDtypeStruct(cache.shape, BF16),
        in_specs=[pl.BlockSpec(memory_space=pltpu.SMEM), anym, vmem],
        out_specs=anym,
        scratch_shapes=[
            pltpu.VMEM((CACHE_SLOTS, CACHE_BLOCK, cache_len, head_dim), BF16),
            pltpu.SemaphoreType.DMA((CACHE_SLOTS,)),
            pltpu.SemaphoreType.DMA((CACHE_SLOTS,)),
        ],
        cost_estimate=pl.CostEstimate(flops=10**11, bytes_accessed=4 * cache.size, transcendentals=0),
        compiler_params=pltpu.CompilerParams(vmem_limit_bytes=60 * 2**20),
        name="cache",
    )(positions, cache, new_rows)


def solution(mesh):
    batch_spec = P(("dp", "w"))
    cache_spec = P(None, ("dp", "w"))
    gain_spec = P(None, "w")
    weight_spec = P(None, "w", None)

    def per_device(hidden, positions, k_cache, v_cache, *weights):
        hid_mid, k_new, v_new, first_r, first_l, next_r, next_l, own = decode(hidden, positions, k_cache, v_cache, *weights)
        n_dev, half = mesh.shape["w"], hidden.shape[0] // 2
        ahead = [(i, (i + CORES) % n_dev) for i in range(n_dev)]
        back = [(i, (i - CORES) % n_dev) for i in range(n_dev)]
        got_r = lax.ppermute(first_r, "w", ahead)
        got_l = lax.ppermute(first_l, "w", back)
        k_out = write_cache(positions, k_cache, k_new)
        upper = lax.ppermute(next_r + got_r[:half], "w", ahead)
        lower = lax.ppermute(next_l + got_l[half:], "w", back)
        v_out = write_cache(positions, v_cache, v_new)
        is_upper = lax.broadcasted_iota(jnp.int32, own.shape, 0) < half
        total = own + jnp.where(is_upper, got_l, got_r) + jnp.concatenate([upper, lower], axis=0)
        hidden_out = (hid_mid.astype(F32) + total).astype(BF16)
        return hidden_out, k_out, v_out

    in_specs = (batch_spec, batch_spec, cache_spec, cache_spec, gain_spec, weight_spec, weight_spec, weight_spec, weight_spec, gain_spec, weight_spec, weight_spec, weight_spec)
    out_specs = (batch_spec, cache_spec, cache_spec)
    return jax.shard_map(per_device, mesh=mesh, in_specs=in_specs, out_specs=out_specs, check_vma=False)
```

```python
import functools

import jax
import jax.numpy as jnp
from jax import lax
from jax.experimental import pallas as pl
from jax.experimental.pallas import tpu as pltpu
from jax.sharding import PartitionSpec as P

EPS = 1e-6
ROPE_BASE = 10000.0
LANES = 128
CORES = 2
CHIPS = 4
SEQ_GROUP = 32
KV_SLOTS = 3
MESH = pl.DeviceIdType.MESH
F32 = jnp.float32
BF16 = jnp.bfloat16


def dot(a, b):
    return jnp.dot(a, b, preferred_element_type=F32)


def dot_t(a, b):
    return lax.dot_general(a, b, (((1,), (1,)), ((), ())), preferred_element_type=F32)


ORDER = (
    "bo0", "ao0", "ce0", "in0", "bp0", "af0", "ct0", "bf0", "cd0", "dt1", "ap0", "ao1", "ce1", "cm0", "at0", "ax0",
    "cf0", "cn0", "bx0", "aw0", "dt0", "af1", "qkv0", "att0", "bo1", "att0", "cx0", "ct1", "att0", "bt0", "bw0", "att0",
    "mix0", "cm1", "cf1", "yf0", "cw0", "cu0", "ap1", "cd1", "gua0", "dr0", "near0", "ax1", "gub0", "far0", "cn1", "cu1",
    "aw1", "er0", "bf1", "guo0", "at1", "own0", "cx1", "done0", "qkv1", "att1", "att1", "bx1", "bt1", "att1", "att1", "mix1",
    "cw1", "yf1", "guo1", "dr1", "own1", "gua1", "near1", "gub1", "far1",
)
SHARE_A = (True, True)
SHARE_B = (True, False)


def decode_kernel(
    dims,
    hid_ref, freq_ref, an_ref, mn_ref, pos_ref, kc_ref, vc_ref,
    wq_ref, wk_ref, wv_ref, wo_ref, wg_ref, wu_ref, wd_ref,
    hid_out, knew_ref, vnew_ref, first_r, first_l, next_r, next_l, own_out,
    cos_buf, sin_buf, act_buf, an_buf, mn_buf, freq_buf, pos_in, know, vnow, gsrc, gbuf, pos_buf, abuf_w, bbuf_w, gu_w, wd_w, tr_w, y_all, m_buf, part, r_t, r_f,
    kbuf, vbuf, qbuf, abuf, hbuf,
    send_sem, recv_sem, loc_sem, kv_sem, out_sem, in_sem,
):
    layers, rows, width, heads, head_dim, cache_len, n_dev, ff = dims
    half = head_dim // 2
    piece = width // n_dev
    chip_cols = ff // CHIPS
    win = gu_w.shape[-1]
    pad = win - chip_cols
    wd_rows = wd_ref.shape[1]
    wo_rows = wo_ref.shape[1]
    q_half = wq_ref.shape[-1] // 2
    kv_half = half
    a_cols = abuf_w.shape[-1]
    groups = rows // SEQ_GROUP
    w = lax.axis_index("w")
    dp = lax.axis_index("dp")
    x, c = lax.div(w, CORES), lax.rem(w, CORES)
    h = lax.rem(dp, 2)
    xr, xo, xl = lax.rem(x + 1, CHIPS), lax.rem(x + 2, CHIPS), lax.rem(x + 3, CHIPS)
    cc = 1 - c
    hh = 1 - h
    right, left = (dp, xr * CORES + c), (dp, xl * CORES + c)
    twin = (dp, x * CORES + cc)
    pair = (dp + 1 - 2 * h, w)
    b_half, b_quarter = wo_rows // 2, wo_rows // 4
    b_mine = pl.multiple_of(h * b_half, b_quarter)
    b_mid = pl.multiple_of(h * b_half + b_quarter, b_quarter)
    b_other = pl.multiple_of(hh * b_half, b_quarter)
    q_mine = pl.multiple_of(h * q_half, LANES)
    kv_mine = pl.multiple_of(h * kv_half, LANES)
    starts = [pl.multiple_of(lax.div(chip_cols * xx, LANES) * LANES, LANES) for xx in (x, xr, xo, xl)]
    x_start, xr_start, xo_start, xl_start = starts
    xr_mid, xo_mid, xl_mid = [pl.multiple_of(xx + win // 2, LANES) for xx in starts[1:]]
    shift = lax.rem(chip_cols * x, LANES)
    wd_mine = pl.ds(pl.multiple_of(shift + wd_rows * c, 32), wd_rows)
    wd_twin = pl.ds(pl.multiple_of(shift + wd_rows * cc, 32), wd_rows)

    msg_ids = {}
    pending = {}

    def copy_of(name, src, dst, dev):
        i = msg_ids.setdefault(name, len(msg_ids))
        return pltpu.make_async_remote_copy(src, dst, send_sem.at[i], recv_sem.at[i], device_id=dev, device_id_type=MESH)

    def send(name, pairs, dev, view=None):
        for src, dst in pairs:
            copy_of(name, src, dst, dev).start()
        pending[name] = pairs[0][0] if view is None else view

    arrived = set()

    def got(name, view):
        if name not in arrived:
            arrived.add(name)
            copy_of(name, view, view, right).wait_recv()

    def drain(names):
        for name in names:
            view = pending.pop(name)
            copy_of(name, view, view, right).wait_send()

    def local_start(sem, pairs):
        for src, dst in pairs:
            pltpu.make_async_copy(src, dst, loc_sem.at[sem]).start()

    def local_wait(sem, view):
        if sem not in arrived:
            arrived.add(sem)
            pltpu.make_async_copy(view, view, loc_sem.at[sem]).wait()

    def kv_copies(i, slot):
        layer, group = lax.div(i, groups), lax.rem(i, groups)
        seqs = pl.ds(group * SEQ_GROUP, SEQ_GROUP)
        return (
            pltpu.make_async_copy(kc_ref.at[layer, seqs, 0], kbuf.at[slot], kv_sem.at[slot, 0]),
            pltpu.make_async_copy(vc_ref.at[layer, seqs, 0], vbuf.at[slot], kv_sem.at[slot, 1]),
        )

    def kv_start(i, slot):
        for copy in kv_copies(i, slot):
            copy.start()

    def a_pairs(l, hf, q_lo, kv_lo):
        dst = abuf_w.at[l, hf, x, c]
        return [
            (wq_ref.at[l, :, pl.ds(q_lo, q_half)], dst.at[:, pl.ds(0, q_half)]),
            (wk_ref.at[l, :, pl.ds(kv_lo, kv_half)], dst.at[:, pl.ds(q_half, kv_half)]),
            (wv_ref.at[l, :, pl.ds(kv_lo, kv_half)], dst.at[:, pl.ds(q_half + kv_half, kv_half)]),
        ]

    def a_both(l):
        return a_pairs(l, 0, 0, 0) + a_pairs(l, 1, q_half, kv_half)

    def a_block(l, xx):
        return abuf_w.at[l, h, xx, c] if SHARE_A[l] else abuf_w.at[l, :, xx, c]

    def a_lead(l, xx):
        return abuf_w.at[l, h, xx, c, :, pl.ds(0, a_cols // 2)] if SHARE_A[l] else abuf_w.at[l, 0, xx, c]

    def a_tail(l, xx):
        return abuf_w.at[l, h, xx, c, :, pl.ds(a_cols // 2, a_cols // 2)] if SHARE_A[l] else abuf_w.at[l, 1, xx, c]

    def ao(l):
        pairs = a_pairs(l, h, q_mine, kv_mine) if SHARE_A[l] else a_both(l)
        send(f"aR{l}", pairs, right, a_block(l, x))
        send(f"aL{l}", pairs, left, a_block(l, x))

    def to_pair(name, view):
        send(name, [(view, view)], pair)

    def a_near(l):
        got(f"aR{l}", a_block(l, xl))
        got(f"aL{l}", a_block(l, xr))

    def a_far(l):
        got(f"afR{l}", a_lead(l, xo))
        got(f"afL{l}", a_tail(l, xo))

    def af(l):
        a_near(l)
        send(f"afR{l}", [(a_lead(l, xl), a_lead(l, xl))], right)
        send(f"afL{l}", [(a_tail(l, xr), a_tail(l, xr))], left)

    def ap(l):
        a_near(l)
        to_pair(f"paR{l}", a_block(l, xl))
        to_pair(f"paL{l}", a_block(l, xr))

    def ax(l):
        a_far(l)
        if SHARE_A[l]:
            to_pair(f"paF{l}", a_block(l, xo))

    def at(l):
        a_near(l)
        a_far(l)
        local_wait(4 * l, abuf_w.at[l, :, x, c])
        view = abuf_w.at[l, h, :, c] if SHARE_A[l] else abuf_w.at[l, :, :, c]
        send(f"aT{l}", [(view, view)], twin)

    def aw(l):
        for name, xx in (("paR", xl), ("paL", xr), ("paF", xo)):
            got(f"{name}{l}", abuf_w.at[l, hh, xx, c])
        local_wait(4 * l, abuf_w.at[l, :, x, c])
        view = abuf_w.at[l, hh, :, c]
        send(f"aT1{l}", [(view, view)], twin)

    def a_ready(l):
        if SHARE_A[l]:
            got(f"aT{l}", abuf_w.at[l, h, :, cc])
            got(f"aT1{l}", abuf_w.at[l, hh, :, cc])
        else:
            got(f"aT{l}", abuf_w.at[l, :, :, cc])

    def b_block(l, xx):
        return bbuf_w.at[l, xx, c, pl.ds(b_mine, b_half)] if SHARE_B[l] else bbuf_w.at[l, xx, c]

    def b_lead(l, xx):
        return bbuf_w.at[l, xx, c, pl.ds(b_mine, b_quarter)] if SHARE_B[l] else bbuf_w.at[l, xx, c, pl.ds(0, b_half)]

    def b_tail(l, xx):
        return bbuf_w.at[l, xx, c, pl.ds(b_mid, b_quarter)] if SHARE_B[l] else bbuf_w.at[l, xx, c, pl.ds(b_half, b_half)]

    def bo(l):
        src = wo_ref.at[l, pl.ds(b_mine, b_half)] if SHARE_B[l] else wo_ref.at[l]
        send(f"bR{l}", [(src, b_block(l, x))], right)
        send(f"bL{l}", [(src, b_block(l, x))], left)

    def b_near(l):
        got(f"bR{l}", b_block(l, xl))
        got(f"bL{l}", b_block(l, xr))

    def b_far(l):
        got(f"bfR{l}", b_lead(l, xo))
        got(f"bfL{l}", b_tail(l, xo))

    def bf(l):
        b_near(l)
        send(f"bfR{l}", [(b_lead(l, xl), b_lead(l, xl))], right)
        send(f"bfL{l}", [(b_tail(l, xr), b_tail(l, xr))], left)

    def bp(l):
        b_near(l)
        to_pair(f"pbR{l}", b_block(l, xl))
        to_pair(f"pbL{l}", b_block(l, xr))

    def bx(l):
        b_far(l)
        if SHARE_B[l]:
            to_pair(f"pbF{l}", b_block(l, xo))

    def bt(l):
        b_near(l)
        b_far(l)
        local_wait(4 * l + 1, bbuf_w.at[l, x, c])
        view = bbuf_w.at[l, :, c, pl.ds(b_mine, b_half)] if SHARE_B[l] else bbuf_w.at[l, :, c]
        send(f"bT{l}", [(view, view)], twin)

    def bw(l):
        for name, xx in (("pbR", xl), ("pbL", xr), ("pbF", xo)):
            got(f"{name}{l}", bbuf_w.at[l, xx, c, pl.ds(b_other, b_half)])
        local_wait(4 * l + 1, bbuf_w.at[l, x, c])
        view = bbuf_w.at[l, :, c, pl.ds(b_other, b_half)]
        send(f"bT1{l}", [(view, view)], twin)

    def b_ready(l):
        if SHARE_B[l]:
            got(f"bT{l}", bbuf_w.at[l, :, cc, pl.ds(b_mine, b_half)])
            got(f"bT1{l}", bbuf_w.at[l, :, cc, pl.ds(b_other, b_half)])
        else:
            got(f"bT{l}", bbuf_w.at[l, :, cc])

    def by_matrix(l, name, lo, size, dst, dev):
        for value, ref in ((0, wg_ref), (1, wu_ref)):
            @pl.when(h == value)
            def _():
                copy_of(name, ref.at[l, :, pl.ds(lo, size)], dst, dev).start()
        pending[name] = dst

    fore, aft = pl.ds(0, win // 2), pl.ds(win // 2, win // 2)

    def cd(l):
        by_matrix(l, f"cR{l}", xr_start, win // 2, gu_w.at[l, h, x, c, :, fore], right)
        by_matrix(l, f"cL{l}", xl_start, win // 2, gu_w.at[l, h, x, c, :, fore], left)

    def ce(l):
        by_matrix(l, f"dR{l}", xr_mid, win // 2, gu_w.at[l, h, x, c, :, aft], right)
        by_matrix(l, f"dL{l}", xl_mid, win // 2, gu_w.at[l, h, x, c, :, aft], left)

    def ct(l):
        by_matrix(l, f"tR{l}", xo_start, win // 2, tr_w.at[l, 0], right)
        by_matrix(l, f"tL{l}", xo_mid, win // 2, tr_w.at[l, 1], left)

    def cf(l):
        got(f"tR{l}", tr_w.at[l, 0])
        send(f"cfR{l}", [(tr_w.at[l, 0], gu_w.at[l, h, xl, c, :, fore])], right)
        got(f"tL{l}", tr_w.at[l, 1])
        send(f"cfL{l}", [(tr_w.at[l, 1], gu_w.at[l, h, xr, c, :, aft])], left)

    def c_near(l, part_name, cols):
        got(f"{part_name}R{l}", gu_w.at[l, h, xl, c, :, cols])
        got(f"{part_name}L{l}", gu_w.at[l, h, xr, c, :, cols])

    def c_far(l):
        got(f"cfR{l}", gu_w.at[l, h, xo, c, :, fore])
        got(f"cfL{l}", gu_w.at[l, h, xo, c, :, aft])

    def cn(l):
        c_near(l, "c", fore)
        to_pair(f"pcR{l}", gu_w.at[l, h, xl, c, :, fore])
        to_pair(f"pcL{l}", gu_w.at[l, h, xr, c, :, fore])

    def cm(l):
        c_near(l, "d", aft)
        to_pair(f"pdR{l}", gu_w.at[l, h, xl, c, :, aft])
        to_pair(f"pdL{l}", gu_w.at[l, h, xr, c, :, aft])

    def cx(l):
        c_far(l)
        to_pair(f"pcF{l}", gu_w.at[l, h, xo, c])

    def cu(l):
        c_near(l, "c", fore)
        c_near(l, "d", aft)
        c_far(l)
        local_wait(4 * l + 2, gu_w.at[l, :, x, c])
        view = gu_w.at[l, h, :, c]
        send(f"cT{l}", [(view, view)], twin)

    def cw(l):
        for name, xx, cols in (("pcR", xl, fore), ("pcL", xr, fore), ("pdR", xl, aft), ("pdL", xr, aft)):
            got(f"{name}{l}", gu_w.at[l, hh, xx, c, :, cols])
        got(f"pcF{l}", gu_w.at[l, hh, xo, c])
        local_wait(4 * l + 2, gu_w.at[l, :, x, c])
        view = gu_w.at[l, hh, :, c]
        send(f"cT1{l}", [(view, view)], twin)

    def c_ready(l):
        got(f"cT{l}", gu_w.at[l, h, :, cc])
        got(f"cT1{l}", gu_w.at[l, hh, :, cc])

    def dt(l):
        send(f"dT{l}", [(wd_ref.at[l], wd_w.at[l, wd_mine])], twin)

    def d_ready(l):
        local_wait(4 * l + 3, wd_w.at[l, wd_mine])
        got(f"dT{l}", wd_w.at[l, wd_twin])

    small = [(an_ref, an_buf), (mn_ref, mn_buf), (freq_ref, freq_buf), (pos_ref, pos_in)]
    for i, (src, dst) in enumerate(small):
        pltpu.make_async_copy(src, dst, in_sem.at[i]).start()
    barrier = pltpu.get_barrier_semaphore()
    for i in range(1, n_dev):
        pl.semaphore_signal(barrier, inc=1, device_id=(dp, lax.rem(w + i, n_dev)), device_id_type=MESH)
    pl.semaphore_signal(barrier, inc=1, device_id=pair, device_id_type=MESH)
    pl.semaphore_wait(barrier, n_dev)

    def entry(_):
        hid_copy = pltpu.make_async_copy(hid_ref, hbuf, in_sem.at[len(small)])
        hid_copy.start()
        for i in range(KV_SLOTS):
            kv_start(i, i)
        for l in range(layers):
            local_start(4 * l, a_both(l))
            local_start(4 * l + 1, [(wo_ref.at[l], bbuf_w.at[l, x, c])])
            cols = pl.ds(x_start, win)
            local_start(4 * l + 2, [(wg_ref.at[l, :, cols], gu_w.at[l, 0, x, c]), (wu_ref.at[l, :, cols], gu_w.at[l, 1, x, c])])
            local_start(4 * l + 3, [(wd_ref.at[l], wd_w.at[l, wd_mine])])
        for i, (src, dst) in enumerate(small):
            pltpu.make_async_copy(src, dst, in_sem.at[i]).wait()
        gsrc[...] = jnp.zeros_like(gsrc)
        gsrc[0:layers, 0:piece] = an_buf[...]
        gsrc[layers:2 * layers, 0:piece] = mn_buf[...]
        own_gain = pltpu.roll(gsrc[...], lax.rem(w * piece, LANES), 1)
        gsrc[...] = own_gain
        gbuf[w] = own_gain
        for l in range(layers):
            start = pl.multiple_of(jnp.where(lax.rem(x, 2) == 0, chip_cols, 0), 64)
            wd_w[l, pl.ds(start, pad), :] = jnp.zeros((pad, width), BF16)
        lane_block = lax.div(lax.broadcasted_iota(jnp.int32, (1, LANES), 1), SEQ_GROUP)
        for g in range(groups):
            line = pos_in[...]
            for j in range(heads):
                moved = pltpu.roll(pos_in[...], ((j - g) * SEQ_GROUP) % LANES, 1)
                line = jnp.where(lane_block == j, moved, line)
            pos_buf[g] = line
        angles = jnp.broadcast_to(pos_in[...].astype(F32), (rows, rows)).T * freq_buf[...]
        cos_buf[...] = jnp.cos(angles)
        sin_buf[...] = jnp.sin(angles)
        for i in range(1, n_dev):
            copy_of("gain", gsrc, gbuf.at[w], (dp, lax.rem(w + i, n_dev))).start()
        pending["gain"] = gbuf.at[pl.ds(0, n_dev - 1)]
        hid_copy.wait()

    def all_gains():
        tiles = []
        for j in range(width // LANES):
            total = None
            for s in range(n_dev):
                lo = (s * piece) // LANES
                for k in range(2):
                    if lo + k == j:
                        block = gbuf[s, :, k * LANES:(k + 1) * LANES]
                        total = block if total is None else total + block
            tiles.append(total)
        return 1.0 + jnp.concatenate(tiles, axis=1)

    def rms(hid, row):
        mean_sq = jnp.sum(hid * hid, axis=-1, keepdims=True) / width
        return (hid * lax.rsqrt(mean_sq + EPS) * all_gains()[row:row + 1, :]).astype(BF16)

    chunk = 4

    def attend(l, group):
        lane_seq = lax.rem(lax.broadcasted_iota(jnp.int32, (cache_len, LANES), 1), SEQ_GROUP)
        row_seq = lax.rem(lax.broadcasted_iota(jnp.int32, (LANES, cache_len), 0), SEQ_GROUP)
        row_t = lax.broadcasted_iota(jnp.int32, (cache_len, LANES), 0)
        lane_new = lax.rem(lax.broadcasted_iota(jnp.int32, (SEQ_GROUP, LANES), 1), SEQ_GROUP)
        row_new = lax.broadcasted_iota(jnp.int32, (SEQ_GROUP, LANES), 0)
        i = l * groups + group
        slot = lax.rem(i, KV_SLOTS)
        for copy in kv_copies(i, slot):
            copy.wait()
        seqs = pl.ds(pl.multiple_of(group * SEQ_GROUP, SEQ_GROUP), SEQ_GROUP)
        query = jnp.concatenate([qbuf[j, seqs, :] for j in range(heads)], axis=0)
        scores = jnp.zeros((cache_len, LANES), F32)
        for b in range(0, SEQ_GROUP, chunk):
            block = kbuf[slot, b:b + chunk].reshape(chunk * cache_len, head_dim)
            prod = dot_t(block, query)
            for j in range(chunk):
                scores = jnp.where(lane_seq == b + j, prod[j * cache_len:(j + 1) * cache_len], scores)
        k_new = know[l, seqs, :].astype(BF16)
        v_new = vnow[l, seqs, :]
        new_score = jnp.sum(jnp.where(row_new == lane_new, dot_t(k_new, query), 0.0), axis=0, keepdims=True)
        scores = jnp.where(row_t < pos_buf[group], scores, -1e30)
        top = jnp.maximum(jnp.max(scores, axis=0, keepdims=True), new_score)
        prob = jnp.exp(scores - top)
        prob_new = jnp.exp(new_score - top)
        total = jnp.sum(prob, axis=0, keepdims=True) + prob_new
        prob_t = prob.T
        total_t = jnp.broadcast_to(total, (LANES, LANES)).T
        new_t = jnp.broadcast_to(prob_new, (LANES, LANES)).T.astype(BF16).astype(F32)
        v_rep = jnp.concatenate([v_new] * heads, axis=0)
        acc = jnp.concatenate([new_t] * (head_dim // LANES), axis=1) * v_rep
        for b in range(0, SEQ_GROUP, chunk):
            spread = jnp.concatenate([jnp.where(row_seq == b + j, prob_t, 0.0).astype(BF16) for j in range(chunk)], axis=1)
            acc = acc + dot(spread, vbuf[slot, b:b + chunk].reshape(chunk * cache_len, head_dim))
        attn = (acc / jnp.concatenate([total_t] * (head_dim // LANES), axis=1)).astype(BF16)
        for j in range(heads):
            abuf[seqs, j * head_dim:(j + 1) * head_dim] = attn[j * SEQ_GROUP:(j + 1) * SEQ_GROUP, :]

        @pl.when(i + KV_SLOTS < layers * groups)
        def _():
            kv_start(i + KV_SLOTS, slot)

    last = layers - 1
    exports = []

    def export(src, dst):
        pltpu.make_async_copy(src, dst, out_sem.at[len(exports)]).start()
        exports.append((src, dst))

    def qkv(l):
        a_ready(l)
        if l == 0:
            got("gain", gbuf.at[pl.ds(0, n_dev - 1)])
        cos_tab, sin_tab = cos_buf[...], sin_buf[...]
        normed = rms(hbuf[...].astype(F32), l)
        halves = [dot(normed, abuf_w[l, hf].reshape(width, a_cols)) for hf in range(2)]

        def rope(lead, tail):
            return jnp.concatenate([lead * cos_tab - tail * sin_tab, tail * cos_tab + lead * sin_tab], axis=1)

        for j in range(heads):
            out, lo = halves[j // (heads // 2)], (j % (heads // 2)) * head_dim
            qbuf[j] = (rope(out[:, lo:lo + half], out[:, lo + half:lo + head_dim]) * head_dim ** -0.5).astype(BF16)
        know[l] = rope(halves[0][:, q_half:q_half + half], halves[1][:, q_half:q_half + half]).astype(BF16).astype(F32)
        vnow[l] = jnp.concatenate([hv[:, q_half + half:q_half + 2 * half] for hv in halves], axis=1).astype(BF16).astype(F32)
        export(know.at[l], knew_ref.at[l])
        export(vnow.at[l], vnew_ref.at[l])

    r2 = rows // 2
    upper, lower = pl.ds(0, r2), pl.ds(r2, r2)

    def mix(l):
        b_ready(l)
        mixed = dot(abuf[...], bbuf_w[l].reshape(heads * head_dim, width))
        hid_mid = (hbuf[...].astype(F32) + mixed).astype(BF16)
        hbuf[...] = hid_mid
        y_all[l, x] = rms(hid_mid.astype(F32), layers + l)
        top, bottom = y_all.at[l, x, upper], y_all.at[l, x, lower]
        send(f"yR1{l}", [(top, top)], right)
        send(f"yL1{l}", [(bottom, bottom)], left)
        send(f"yR2{l}", [(bottom, bottom)], right)
        send(f"yL2{l}", [(top, top)], left)

    def yf(l):
        view = y_all.at[l, xl, upper]
        got(f"yR1{l}", view)
        send(f"yfR{l}", [(view, view)], right)
        view = y_all.at[l, xr, lower]
        got(f"yL1{l}", view)
        send(f"yfL{l}", [(view, view)], left)

    n_tile = 2 * LANES

    def gate_up(l, blocks):
        span = slice(0, len(blocks) * rows)

        def at_tile(n):
            return pl.ds(pl.multiple_of(n * n_tile, n_tile), n_tile)

        def multiply(n, slot):
            act = jnp.concatenate([y_all[l, b] for b in blocks], axis=0)
            for k in range(2):
                act_buf[slot, k, span] = dot(act, gu_w[l, k, :, :, :, at_tile(n)].reshape(width, n_tile))

        def activate(n, slot):
            mid = (jax.nn.gelu(act_buf[slot, 0, span], approximate=True) * act_buf[slot, 1, span]).astype(BF16)
            for k, b in enumerate(blocks):
                m_buf[b, :, at_tile(n)] = mid[k * rows:(k + 1) * rows]

        tiles = win // n_tile
        assert tiles % 2 == 1
        multiply(0, 0)

        @pl.loop(0, tiles // 2)
        def _(k):
            multiply(2 * k + 1, 1)
            activate(2 * k, 0)
            multiply(2 * k + 2, 0)
            activate(2 * k + 1, 1)

        activate(tiles - 1, 0)

    def guo(l):
        if l:
            c_ready(l)
        gate_up(l, (x,))

    def gua(l):
        got(f"yR2{l}", y_all.at[l, xl, lower])
        got(f"yL2{l}", y_all.at[l, xr, upper])
        if not l:
            c_ready(l)
        gate_up(l, (xl, xr))

    def gub(l):
        got(f"yfR{l}", y_all.at[l, xo, upper])
        got(f"yfL{l}", y_all.at[l, xo, lower])
        gate_up(l, (xo,))

    def down(l, xx):
        part[xx] = dot(m_buf[xx], wd_w[l])

    def near(l):
        if l:
            drain([f"{name}{l - 1}" for name in ("eR2", "eL2", "eR3", "eL3")])
        down(l, xr)
        if l == last:
            export(part.at[xr, lower], first_r.at[lower])
            export(part.at[xr, upper], next_r)
        else:
            send(f"eR2{l}", [(part.at[xr, lower], r_f.at[l, 0, lower])], right)
        down(l, xl)
        if l == last:
            export(part.at[xl, upper], first_l.at[upper])
            export(part.at[xl, lower], next_l)
        else:
            send(f"eL2{l}", [(part.at[xl, upper], r_f.at[l, 1, upper])], left)

    def far(l):
        if l:
            drain([f"{name}{l - 1}" for name in ("eR1", "eL1")])
        down(l, xo)
        if l == last:
            export(part.at[xo, upper], first_r.at[upper])
            export(part.at[xo, lower], first_l.at[lower])
        else:
            send(f"eR1{l}", [(part.at[xo, upper], r_t.at[l, 0])], right)
            send(f"eL1{l}", [(part.at[xo, lower], r_t.at[l, 1])], left)

    def er(l):
        got(f"eR1{l}", r_t.at[l, 0])
        part[xr, 0:r2] = part[xr, 0:r2] + r_t[l, 0]
        send(f"eR3{l}", [(part.at[xr, upper], r_f.at[l, 0, upper])], right)
        got(f"eL1{l}", r_t.at[l, 1])
        part[xl, r2:rows] = part[xl, r2:rows] + r_t[l, 1]
        send(f"eL3{l}", [(part.at[xl, lower], r_f.at[l, 1, lower])], left)

    def own(l):
        down(l, x)
        if l == last:
            export(part.at[x], own_out)
            export(hbuf, hid_out)

    def done(l):
        got(f"eR2{l}", r_f.at[l, 0, lower])
        got(f"eL2{l}", r_f.at[l, 1, upper])
        got(f"eR3{l}", r_f.at[l, 0, upper])
        got(f"eL3{l}", r_f.at[l, 1, lower])
        hbuf[...] = (hbuf[...].astype(F32) + (part[x] + r_f[l, 0] + r_f[l, 1])).astype(BF16)

    table = dict(
        ao=ao, af=af, ap=ap, ax=ax, at=at, aw=aw, bo=bo, bf=bf, bp=bp, bx=bx, bt=bt, bw=bw, cd=cd, ce=ce, ct=ct, cf=cf,
        cn=cn, cm=cm, cx=cx, cu=cu, cw=cw, dt=dt, **{"in": entry},
        qkv=qkv, mix=mix, yf=yf, guo=guo, gua=gua, gub=gub, dr=d_ready, near=near, far=far, er=er, own=own, done=done,
    )

    def run(step):
        table[step[:-1]](int(step[-1]))

    here = 0
    reached = [0] * layers
    while here < len(ORDER):
        step = ORDER[here]
        if not step.startswith("att"):
            run(step)
            here += 1
            continue
        l, count = int(step[-1]), 0
        while ORDER[here] == step:
            count += 1
            here += 1
        first = reached[l]
        reached[l] += count

        @pl.loop(first, first + count)
        def _(group):
            attend(l, group)

    drain(list(pending))
    for i, (src, dst) in enumerate(exports):
        pltpu.make_async_copy(src, dst, out_sem.at[i]).wait()
    assert len(msg_ids) <= send_sem.shape[0]


def decode(hidden, positions, k_cache, v_cache, attn_norm, w_query, w_key, w_value, w_out, mlp_norm, w_gate, w_up, w_down):
    layers, rows, _, cache_len, head_dim = k_cache.shape
    width = hidden.shape[1]
    n_dev = lax.axis_size("w")
    ff = w_gate.shape[-1]
    heads = w_query.shape[-1] // head_dim
    chip_cols = ff // CHIPS
    win = -(-(chip_cols + LANES // 2) // LANES) * LANES
    piece = width // n_dev
    groups = rows // SEQ_GROUP
    assert n_dev == CHIPS * CORES and heads * SEQ_GROUP == LANES and cache_len == LANES and rows == LANES
    assert lax.axis_size("dp") % 2 == 0
    inv_freq = ROPE_BASE ** (-2.0 * jnp.arange(head_dim // 2, dtype=F32) / head_dim)
    dims = (layers, rows, width, heads, head_dim, cache_len, n_dev, ff)
    anym = pl.BlockSpec(memory_space=pl.ANY)
    new_shape = jax.ShapeDtypeStruct((layers, rows, head_dim), F32)
    whole_sum = jax.ShapeDtypeStruct(hidden.shape, F32)
    half_sum = jax.ShapeDtypeStruct((rows // 2, width), F32)
    n_msg = 96
    return pl.pallas_call(
        functools.partial(decode_kernel, dims),
        out_shape=(jax.ShapeDtypeStruct(hidden.shape, BF16), new_shape, new_shape) + (whole_sum, whole_sum, half_sum, half_sum, whole_sum),
        in_specs=[anym] * 14,
        out_specs=(anym,) * 8,
        scratch_shapes=[
            pltpu.VMEM((rows, head_dim // 2), F32),
            pltpu.VMEM((rows, head_dim // 2), F32),
            pltpu.VMEM((2, 2, 2 * rows, 2 * LANES), F32),
            pltpu.VMEM(attn_norm.shape, F32),
            pltpu.VMEM(mlp_norm.shape, F32),
            pltpu.VMEM((1, head_dim // 2), F32),
            pltpu.VMEM((1, rows), jnp.int32),
            pltpu.VMEM((layers, rows, head_dim), F32),
            pltpu.VMEM((layers, rows, head_dim), F32),
            pltpu.VMEM((8, 2 * LANES), F32),
            pltpu.VMEM((n_dev, 8, 2 * LANES), F32),
            pltpu.VMEM((groups, 1, LANES), jnp.int32),
            pltpu.VMEM((layers, 2, CHIPS, CORES, piece, w_query.shape[-1] // 2 + head_dim), BF16),
            pltpu.VMEM((layers, CHIPS, CORES, w_out.shape[1], width), BF16),
            pltpu.VMEM((layers, 2, CHIPS, CORES, piece, win), BF16),
            pltpu.VMEM((layers, win, width), BF16),
            pltpu.VMEM((layers, 2, piece, win // 2), BF16),
            pltpu.VMEM((layers, CHIPS, rows, width), BF16),
            pltpu.VMEM((CHIPS, rows, win), BF16),
            pltpu.VMEM((CHIPS, rows, width), F32),
            pltpu.VMEM((layers - 1, 2, rows // 2, width), F32),
            pltpu.VMEM((layers - 1, 2, rows, width), F32),
            pltpu.VMEM((KV_SLOTS, SEQ_GROUP, cache_len, head_dim), BF16),
            pltpu.VMEM((KV_SLOTS, SEQ_GROUP, cache_len, head_dim), BF16),
            pltpu.VMEM((heads, rows, head_dim), BF16),
            pltpu.VMEM((rows, heads * head_dim), BF16),
            pltpu.VMEM((rows, width), BF16),
            pltpu.SemaphoreType.DMA((n_msg,)),
            pltpu.SemaphoreType.DMA((n_msg,)),
            pltpu.SemaphoreType.DMA((4 * layers,)),
            pltpu.SemaphoreType.DMA((KV_SLOTS, 2)),
            pltpu.SemaphoreType.DMA((16,)),
            pltpu.SemaphoreType.DMA((8,)),
        ],
        compiler_params=pltpu.CompilerParams(collective_id=0, has_side_effects=True, vmem_limit_bytes=67043328),
        name="decode",
    )(hidden, inv_freq.reshape(1, head_dim // 2), attn_norm, mlp_norm, positions.reshape(1, rows), k_cache, v_cache, w_query, w_key, w_value, w_out, w_gate, w_up, w_down)


TILE_ROWS = 16
CACHE_BLOCK = 16
CACHE_SLOTS = 12


def cache_kernel(pos_ref, old_ref, new_ref, out_ref, buf, in_sem, out_sem):
    layers, rows = old_ref.shape[:2]
    blocks = rows // CACHE_BLOCK
    steps = layers * blocks

    def split(i):
        return i // blocks, i % blocks, i % CACHE_SLOTS

    def load(i):
        l, b, slot = split(i)
        return pltpu.make_async_copy(old_ref.at[l, pl.ds(b * CACHE_BLOCK, CACHE_BLOCK), 0], buf.at[slot], in_sem.at[slot])

    def store(i):
        l, b, slot = split(i)
        return pltpu.make_async_copy(buf.at[slot], out_ref.at[l, pl.ds(b * CACHE_BLOCK, CACHE_BLOCK), 0], out_sem.at[slot])

    ahead = CACHE_SLOTS // 2
    for i in range(ahead):
        load(i).start()
    row = lax.broadcasted_iota(jnp.int32, (TILE_ROWS, buf.shape[-1]), 0)

    @pl.loop(0, steps)
    def _(i):
        load(i).wait()
        l, b, slot = split(i)
        fresh = new_ref[l, pl.ds(pl.multiple_of(b * CACHE_BLOCK, CACHE_BLOCK), CACHE_BLOCK), :]
        tiles = []
        for s in range(CACHE_BLOCK):
            pos = pos_ref[b * CACHE_BLOCK + s]
            base = pl.multiple_of(pos // TILE_ROWS * TILE_ROWS, TILE_ROWS)
            tile = buf[slot, s, pl.ds(base, TILE_ROWS), :].astype(F32)
            tiles.append((s, base, jnp.where(row == pos - base, fresh[s:s + 1, :], tile).astype(BF16)))
        for s, base, tile in tiles:
            buf[slot, s, pl.ds(base, TILE_ROWS), :] = tile
        store(i).start()

        @pl.when(i + ahead < steps)
        def _():
            @pl.when(i + ahead >= CACHE_SLOTS)
            def _():
                store(i + ahead - CACHE_SLOTS).wait()
            load(i + ahead).start()

    @pl.loop(steps - CACHE_SLOTS, steps)
    def _(i):
        store(i).wait()


def write_cache(positions, cache, new_rows):
    cache_len, head_dim = cache.shape[-2:]
    vmem, anym = pl.BlockSpec(memory_space=pltpu.VMEM), pl.BlockSpec(memory_space=pl.ANY)
    return pl.pallas_call(
        cache_kernel,
        out_shape=jax.ShapeDtypeStruct(cache.shape, BF16),
        in_specs=[pl.BlockSpec(memory_space=pltpu.SMEM), anym, vmem],
        out_specs=anym,
        scratch_shapes=[
            pltpu.VMEM((CACHE_SLOTS, CACHE_BLOCK, cache_len, head_dim), BF16),
            pltpu.SemaphoreType.DMA((CACHE_SLOTS,)),
            pltpu.SemaphoreType.DMA((CACHE_SLOTS,)),
        ],
        cost_estimate=pl.CostEstimate(flops=10**11, bytes_accessed=4 * cache.size, transcendentals=0),
        compiler_params=pltpu.CompilerParams(vmem_limit_bytes=60 * 2**20),
        name="cache",
    )(positions, cache, new_rows)


def solution(mesh):
    batch_spec = P(("dp", "w"))
    cache_spec = P(None, ("dp", "w"))
    gain_spec = P(None, "w")
    weight_spec = P(None, "w", None)

    def per_device(hidden, positions, k_cache, v_cache, *weights):
        hid_mid, k_new, v_new, first_r, first_l, next_r, next_l, own = decode(hidden, positions, k_cache, v_cache, *weights)
        n_dev, half = mesh.shape["w"], hidden.shape[0] // 2
        ahead = [(i, (i + CORES) % n_dev) for i in range(n_dev)]
        back = [(i, (i - CORES) % n_dev) for i in range(n_dev)]
        got_r = lax.ppermute(first_r, "w", ahead)
        got_l = lax.ppermute(first_l, "w", back)
        k_out = write_cache(positions, k_cache, k_new)
        upper = lax.ppermute(next_r + got_r[:half], "w", ahead)
        lower = lax.ppermute(next_l + got_l[half:], "w", back)
        v_out = write_cache(positions, v_cache, v_new)
        is_upper = lax.broadcasted_iota(jnp.int32, own.shape, 0) < half
        total = own + jnp.where(is_upper, got_l, got_r) + jnp.concatenate([upper, lower], axis=0)
        hidden_out = (hid_mid.astype(F32) + total).astype(BF16)
        return hidden_out, k_out, v_out

    in_specs = (batch_spec, batch_spec, cache_spec, cache_spec, gain_spec, weight_spec, weight_spec, weight_spec, weight_spec, gain_spec, weight_spec, weight_spec, weight_spec)
    out_specs = (batch_spec, cache_spec, cache_spec)
    return jax.shard_map(per_device, mesh=mesh, in_specs=in_specs, out_specs=out_specs, check_vma=False)
```

```python
import functools

import jax
import jax.numpy as jnp
import numpy as np
from jax import lax
from jax.experimental import pallas as pl
from jax.experimental.pallas import tpu as pltpu
from jax.sharding import PartitionSpec as P

EPS = 1e-6
ROPE_BASE = 10000.0
LANES = 128
CORES = 2
CHIPS = 4
SEQ_GROUP = 32
KV_SLOTS = 3
MESH = pl.DeviceIdType.MESH
F32 = jnp.float32
BF16 = jnp.bfloat16


def dot(a, b):
    return jnp.dot(a, b, preferred_element_type=F32)


def dot_t(a, b):
    return lax.dot_general(a, b, (((1,), (1,)), ((), ())), preferred_element_type=F32)


ORDER = (
    "bo0", "ao0", "ce0", "in0", "bp0", "af0", "ct0", "bf0", "cd0", "dt1", "ap0", "ao1", "ce1", "cm0", "at0", "ax0",
    "cf0", "cn0", "bx0", "aw0", "dt0", "af1", "qkv0", "att0", "bo1", "att0", "cx0", "ct1", "att0", "bt0", "bw0", "att0",
    "mix0", "cm1", "cf1", "yf0", "cw0", "cu0", "ap1", "cd1", "gua0", "dr0", "near0", "ax1", "gub0", "far0", "cn1", "cu1",
    "aw1", "er0", "bf1", "guo0", "at1", "own0", "cx1", "done0", "qkv1", "att1", "att1", "bx1", "bt1", "att1", "att1", "mix1",
    "cw1", "yf1", "guo1", "dr1", "own1", "gua1", "near1", "gub1", "far1",
)
SHARE_A = (True, True)
SHARE_B = (True, False)


def decode_kernel(
    dims,
    hid_ref, freq_ref, an_ref, mn_ref, pos_ref, kc_ref, vc_ref,
    wq_ref, wk_ref, wv_ref, wo_ref, wg_ref, wu_ref, wd_ref,
    hid_out, knew_ref, vnew_ref, first_r, first_l, next_r, next_l, own_out,
    cos_buf, sin_buf, act_buf, an_buf, mn_buf, freq_buf, pos_in, know, vnow, gsrc, gbuf, pos_rows, abuf_w, bbuf_w, gu_w, wd_w, tr_w, y_all, m_buf, part, r_t, r_f,
    kbuf, vbuf, qbuf, abuf, hbuf,
    send_sem, recv_sem, loc_sem, kv_sem, out_sem, in_sem,
):
    layers, rows, width, heads, head_dim, cache_len, n_dev, ff = dims
    half = head_dim // 2
    piece = width // n_dev
    chip_cols = ff // CHIPS
    win = gu_w.shape[-1]
    pad = win - chip_cols
    wd_rows = wd_ref.shape[1]
    wo_rows = wo_ref.shape[1]
    q_half = wq_ref.shape[-1] // 2
    kv_half = half
    a_cols = abuf_w.shape[-1]
    groups = rows // SEQ_GROUP
    w = lax.axis_index("w")
    dp = lax.axis_index("dp")
    x, c = lax.div(w, CORES), lax.rem(w, CORES)
    h = lax.rem(dp, 2)
    xr, xo, xl = lax.rem(x + 1, CHIPS), lax.rem(x + 2, CHIPS), lax.rem(x + 3, CHIPS)
    cc = 1 - c
    hh = 1 - h
    right, left = (dp, xr * CORES + c), (dp, xl * CORES + c)
    twin = (dp, x * CORES + cc)
    pair = (dp + 1 - 2 * h, w)
    b_half, b_quarter = wo_rows // 2, wo_rows // 4
    b_mine = pl.multiple_of(h * b_half, b_quarter)
    b_mid = pl.multiple_of(h * b_half + b_quarter, b_quarter)
    b_other = pl.multiple_of(hh * b_half, b_quarter)
    q_mine = pl.multiple_of(h * q_half, LANES)
    kv_mine = pl.multiple_of(h * kv_half, LANES)
    starts = [pl.multiple_of(lax.div(chip_cols * xx, LANES) * LANES, LANES) for xx in (x, xr, xo, xl)]
    x_start, xr_start, xo_start, xl_start = starts
    xr_mid, xo_mid, xl_mid = [pl.multiple_of(xx + win // 2, LANES) for xx in starts[1:]]
    shift = lax.rem(chip_cols * x, LANES)
    wd_mine = pl.ds(pl.multiple_of(shift + wd_rows * c, 32), wd_rows)
    wd_twin = pl.ds(pl.multiple_of(shift + wd_rows * cc, 32), wd_rows)

    msg_ids = {}
    pending = {}

    def copy_of(name, src, dst, dev):
        i = msg_ids.setdefault(name, len(msg_ids))
        return pltpu.make_async_remote_copy(src, dst, send_sem.at[i], recv_sem.at[i], device_id=dev, device_id_type=MESH)

    def send(name, pairs, dev, view=None):
        for src, dst in pairs:
            copy_of(name, src, dst, dev).start()
        pending[name] = pairs[0][0] if view is None else view

    arrived = set()

    def got(name, view):
        if name not in arrived:
            arrived.add(name)
            copy_of(name, view, view, right).wait_recv()

    def drain(names):
        for name in names:
            view = pending.pop(name)
            copy_of(name, view, view, right).wait_send()

    def local_start(sem, pairs):
        for src, dst in pairs:
            pltpu.make_async_copy(src, dst, loc_sem.at[sem]).start()

    def local_wait(sem, view):
        if sem not in arrived:
            arrived.add(sem)
            pltpu.make_async_copy(view, view, loc_sem.at[sem]).wait()

    def kv_copies(i, slot):
        layer, group = lax.div(i, groups), lax.rem(i, groups)
        seqs = pl.ds(group * SEQ_GROUP, SEQ_GROUP)
        return (
            pltpu.make_async_copy(kc_ref.at[layer, seqs, 0], kbuf.at[slot], kv_sem.at[slot, 0]),
            pltpu.make_async_copy(vc_ref.at[layer, seqs, 0], vbuf.at[slot], kv_sem.at[slot, 1]),
        )

    def kv_start(i, slot):
        for copy in kv_copies(i, slot):
            copy.start()

    def a_pairs(l, hf, q_lo, kv_lo):
        dst = abuf_w.at[l, hf, x, c]
        return [
            (wq_ref.at[l, :, pl.ds(q_lo, q_half)], dst.at[:, pl.ds(0, q_half)]),
            (wk_ref.at[l, :, pl.ds(kv_lo, kv_half)], dst.at[:, pl.ds(q_half, kv_half)]),
            (wv_ref.at[l, :, pl.ds(kv_lo, kv_half)], dst.at[:, pl.ds(q_half + kv_half, kv_half)]),
        ]

    def a_both(l):
        return a_pairs(l, 0, 0, 0) + a_pairs(l, 1, q_half, kv_half)

    def a_block(l, xx):
        return abuf_w.at[l, h, xx, c] if SHARE_A[l] else abuf_w.at[l, :, xx, c]

    def a_lead(l, xx):
        return abuf_w.at[l, h, xx, c, :, pl.ds(0, a_cols // 2)] if SHARE_A[l] else abuf_w.at[l, 0, xx, c]

    def a_tail(l, xx):
        return abuf_w.at[l, h, xx, c, :, pl.ds(a_cols // 2, a_cols // 2)] if SHARE_A[l] else abuf_w.at[l, 1, xx, c]

    def ao(l):
        pairs = a_pairs(l, h, q_mine, kv_mine) if SHARE_A[l] else a_both(l)
        send(f"aR{l}", pairs, right, a_block(l, x))
        send(f"aL{l}", pairs, left, a_block(l, x))

    def to_pair(name, view):
        send(name, [(view, view)], pair)

    def a_near(l):
        got(f"aR{l}", a_block(l, xl))
        got(f"aL{l}", a_block(l, xr))

    def a_far(l):
        got(f"afR{l}", a_lead(l, xo))
        got(f"afL{l}", a_tail(l, xo))

    def af(l):
        a_near(l)
        send(f"afR{l}", [(a_lead(l, xl), a_lead(l, xl))], right)
        send(f"afL{l}", [(a_tail(l, xr), a_tail(l, xr))], left)

    def ap(l):
        a_near(l)
        to_pair(f"paR{l}", a_block(l, xl))
        to_pair(f"paL{l}", a_block(l, xr))

    def ax(l):
        a_far(l)
        if SHARE_A[l]:
            to_pair(f"paF{l}", a_block(l, xo))

    def at(l):
        a_near(l)
        a_far(l)
        local_wait(4 * l, abuf_w.at[l, :, x, c])
        view = abuf_w.at[l, h, :, c] if SHARE_A[l] else abuf_w.at[l, :, :, c]
        send(f"aT{l}", [(view, view)], twin)

    def aw(l):
        for name, xx in (("paR", xl), ("paL", xr), ("paF", xo)):
            got(f"{name}{l}", abuf_w.at[l, hh, xx, c])
        local_wait(4 * l, abuf_w.at[l, :, x, c])
        view = abuf_w.at[l, hh, :, c]
        send(f"aT1{l}", [(view, view)], twin)

    def a_ready(l):
        if SHARE_A[l]:
            got(f"aT{l}", abuf_w.at[l, h, :, cc])
            got(f"aT1{l}", abuf_w.at[l, hh, :, cc])
        else:
            got(f"aT{l}", abuf_w.at[l, :, :, cc])

    def b_block(l, xx):
        return bbuf_w.at[l, xx, c, pl.ds(b_mine, b_half)] if SHARE_B[l] else bbuf_w.at[l, xx, c]

    def b_lead(l, xx):
        return bbuf_w.at[l, xx, c, pl.ds(b_mine, b_quarter)] if SHARE_B[l] else bbuf_w.at[l, xx, c, pl.ds(0, b_half)]

    def b_tail(l, xx):
        return bbuf_w.at[l, xx, c, pl.ds(b_mid, b_quarter)] if SHARE_B[l] else bbuf_w.at[l, xx, c, pl.ds(b_half, b_half)]

    def bo(l):
        src = wo_ref.at[l, pl.ds(b_mine, b_half)] if SHARE_B[l] else wo_ref.at[l]
        send(f"bR{l}", [(src, b_block(l, x))], right)
        send(f"bL{l}", [(src, b_block(l, x))], left)

    def b_near(l):
        got(f"bR{l}", b_block(l, xl))
        got(f"bL{l}", b_block(l, xr))

    def b_far(l):
        got(f"bfR{l}", b_lead(l, xo))
        got(f"bfL{l}", b_tail(l, xo))

    def bf(l):
        b_near(l)
        send(f"bfR{l}", [(b_lead(l, xl), b_lead(l, xl))], right)
        send(f"bfL{l}", [(b_tail(l, xr), b_tail(l, xr))], left)

    def bp(l):
        b_near(l)
        to_pair(f"pbR{l}", b_block(l, xl))
        to_pair(f"pbL{l}", b_block(l, xr))

    def bx(l):
        b_far(l)
        if SHARE_B[l]:
            to_pair(f"pbF{l}", b_block(l, xo))

    def bt(l):
        b_near(l)
        b_far(l)
        local_wait(4 * l + 1, bbuf_w.at[l, x, c])
        view = bbuf_w.at[l, :, c, pl.ds(b_mine, b_half)] if SHARE_B[l] else bbuf_w.at[l, :, c]
        send(f"bT{l}", [(view, view)], twin)

    def bw(l):
        for name, xx in (("pbR", xl), ("pbL", xr), ("pbF", xo)):
            got(f"{name}{l}", bbuf_w.at[l, xx, c, pl.ds(b_other, b_half)])
        local_wait(4 * l + 1, bbuf_w.at[l, x, c])
        view = bbuf_w.at[l, :, c, pl.ds(b_other, b_half)]
        send(f"bT1{l}", [(view, view)], twin)

    def b_ready(l):
        if SHARE_B[l]:
            got(f"bT{l}", bbuf_w.at[l, :, cc, pl.ds(b_mine, b_half)])
            got(f"bT1{l}", bbuf_w.at[l, :, cc, pl.ds(b_other, b_half)])
        else:
            got(f"bT{l}", bbuf_w.at[l, :, cc])

    def by_matrix(l, name, lo, size, dst, dev):
        for value, ref in ((0, wg_ref), (1, wu_ref)):
            @pl.when(h == value)
            def _():
                copy_of(name, ref.at[l, :, pl.ds(lo, size)], dst, dev).start()
        pending[name] = dst

    fore, aft = pl.ds(0, win // 2), pl.ds(win // 2, win // 2)

    def cd(l):
        by_matrix(l, f"cR{l}", xr_start, win // 2, gu_w.at[l, h, x, c, :, fore], right)
        by_matrix(l, f"cL{l}", xl_start, win // 2, gu_w.at[l, h, x, c, :, fore], left)

    def ce(l):
        by_matrix(l, f"dR{l}", xr_mid, win // 2, gu_w.at[l, h, x, c, :, aft], right)
        by_matrix(l, f"dL{l}", xl_mid, win // 2, gu_w.at[l, h, x, c, :, aft], left)

    def ct(l):
        by_matrix(l, f"tR{l}", xo_start, win // 2, tr_w.at[l, 0], right)
        by_matrix(l, f"tL{l}", xo_mid, win // 2, tr_w.at[l, 1], left)

    def cf(l):
        got(f"tR{l}", tr_w.at[l, 0])
        send(f"cfR{l}", [(tr_w.at[l, 0], gu_w.at[l, h, xl, c, :, fore])], right)
        got(f"tL{l}", tr_w.at[l, 1])
        send(f"cfL{l}", [(tr_w.at[l, 1], gu_w.at[l, h, xr, c, :, aft])], left)

    def c_near(l, part_name, cols):
        got(f"{part_name}R{l}", gu_w.at[l, h, xl, c, :, cols])
        got(f"{part_name}L{l}", gu_w.at[l, h, xr, c, :, cols])

    def c_far(l):
        got(f"cfR{l}", gu_w.at[l, h, xo, c, :, fore])
        got(f"cfL{l}", gu_w.at[l, h, xo, c, :, aft])

    def cn(l):
        c_near(l, "c", fore)
        to_pair(f"pcR{l}", gu_w.at[l, h, xl, c, :, fore])
        to_pair(f"pcL{l}", gu_w.at[l, h, xr, c, :, fore])

    def cm(l):
        c_near(l, "d", aft)
        to_pair(f"pdR{l}", gu_w.at[l, h, xl, c, :, aft])
        to_pair(f"pdL{l}", gu_w.at[l, h, xr, c, :, aft])

    def cx(l):
        c_far(l)
        to_pair(f"pcF{l}", gu_w.at[l, h, xo, c])

    def cu(l):
        c_near(l, "c", fore)
        c_near(l, "d", aft)
        c_far(l)
        local_wait(4 * l + 2, gu_w.at[l, :, x, c])
        view = gu_w.at[l, h, :, c]
        send(f"cT{l}", [(view, view)], twin)

    def cw(l):
        for name, xx, cols in (("pcR", xl, fore), ("pcL", xr, fore), ("pdR", xl, aft), ("pdL", xr, aft)):
            got(f"{name}{l}", gu_w.at[l, hh, xx, c, :, cols])
        got(f"pcF{l}", gu_w.at[l, hh, xo, c])
        local_wait(4 * l + 2, gu_w.at[l, :, x, c])
        view = gu_w.at[l, hh, :, c]
        send(f"cT1{l}", [(view, view)], twin)

    def c_ready(l):
        got(f"cT{l}", gu_w.at[l, h, :, cc])
        got(f"cT1{l}", gu_w.at[l, hh, :, cc])

    def dt(l):
        send(f"dT{l}", [(wd_ref.at[l], wd_w.at[l, wd_mine])], twin)

    def d_ready(l):
        local_wait(4 * l + 3, wd_w.at[l, wd_mine])
        got(f"dT{l}", wd_w.at[l, wd_twin])

    small = [(an_ref, an_buf), (mn_ref, mn_buf), (freq_ref, freq_buf), (pos_ref, pos_in)]
    for i, (src, dst) in enumerate(small):
        pltpu.make_async_copy(src, dst, in_sem.at[i]).start()
    barrier = pltpu.get_barrier_semaphore()
    for i in range(1, n_dev):
        pl.semaphore_signal(barrier, inc=1, device_id=(dp, lax.rem(w + i, n_dev)), device_id_type=MESH)
    pl.semaphore_signal(barrier, inc=1, device_id=pair, device_id_type=MESH)
    pl.semaphore_wait(barrier, n_dev)

    def entry(_):
        hid_copy = pltpu.make_async_copy(hid_ref, hbuf, in_sem.at[len(small)])
        hid_copy.start()
        for i in range(KV_SLOTS):
            kv_start(i, i)
        for l in range(layers):
            local_start(4 * l, a_both(l))
            local_start(4 * l + 1, [(wo_ref.at[l], bbuf_w.at[l, x, c])])
            cols = pl.ds(x_start, win)
            local_start(4 * l + 2, [(wg_ref.at[l, :, cols], gu_w.at[l, 0, x, c]), (wu_ref.at[l, :, cols], gu_w.at[l, 1, x, c])])
            local_start(4 * l + 3, [(wd_ref.at[l], wd_w.at[l, wd_mine])])
        for i, (src, dst) in enumerate(small):
            pltpu.make_async_copy(src, dst, in_sem.at[i]).wait()
        gsrc[...] = jnp.zeros_like(gsrc)
        gsrc[0:layers, 0:piece] = an_buf[...]
        gsrc[layers:2 * layers, 0:piece] = mn_buf[...]
        own_gain = pltpu.roll(gsrc[...], lax.rem(w * piece, LANES), 1)
        gsrc[...] = own_gain
        gbuf[w] = own_gain
        for l in range(layers):
            start = pl.multiple_of(jnp.where(lax.rem(x, 2) == 0, chip_cols, 0), 64)
            wd_w[l, pl.ds(start, pad), :] = jnp.zeros((pad, width), BF16)
        pos_rows[...] = jnp.broadcast_to(pos_in[...].astype(F32), (rows, rows)).T
        angles = pos_rows[...] * freq_buf[...]
        cos_buf[...] = jnp.cos(angles)
        sin_buf[...] = jnp.sin(angles)
        for i in range(1, n_dev):
            copy_of("gain", gsrc, gbuf.at[w], (dp, lax.rem(w + i, n_dev))).start()
        pending["gain"] = gbuf.at[pl.ds(0, n_dev - 1)]
        hid_copy.wait()

    def all_gains():
        tiles = []
        for j in range(width // LANES):
            total = None
            for s in range(n_dev):
                lo = (s * piece) // LANES
                for k in range(2):
                    if lo + k == j:
                        block = gbuf[s, :, k * LANES:(k + 1) * LANES]
                        total = block if total is None else total + block
            tiles.append(total)
        return 1.0 + jnp.concatenate(tiles, axis=1)

    def rms(hid, row):
        mean_sq = jnp.sum(hid * hid, axis=-1, keepdims=True) / width
        return (hid * lax.rsqrt(mean_sq + EPS) * all_gains()[row:row + 1, :]).astype(BF16)

    chunk = 4

    def attend(l, group):
        row_seq = lax.rem(lax.broadcasted_iota(jnp.int32, (LANES, cache_len), 0), SEQ_GROUP)
        place = lax.broadcasted_iota(jnp.int32, (LANES, cache_len), 1).astype(F32)
        i = l * groups + group
        slot = lax.rem(i, KV_SLOTS)
        for copy in kv_copies(i, slot):
            copy.wait()
        seqs = pl.ds(pl.multiple_of(group * SEQ_GROUP, SEQ_GROUP), SEQ_GROUP)
        query = jnp.concatenate([qbuf[j, seqs, :] for j in range(heads)], axis=0)
        scores = jnp.zeros((LANES, cache_len), F32)
        for b in range(0, SEQ_GROUP, chunk):
            prod = dot_t(query, kbuf[slot, b:b + chunk].reshape(chunk * cache_len, head_dim))
            for j in range(chunk):
                scores = jnp.where(row_seq == b + j, prod[:, j * cache_len:(j + 1) * cache_len], scores)
        k_rep = jnp.concatenate([know[l, seqs, :]] * heads, axis=0)
        v_rep = jnp.concatenate([vnow[l, seqs, :]] * heads, axis=0)
        new_score = jnp.sum(query.astype(F32) * k_rep, axis=1, keepdims=True)
        pos = jnp.concatenate([pos_rows[seqs, :]] * heads, axis=0)
        scores = jnp.where(place < pos, scores, -1e30)
        top = jnp.maximum(jnp.max(scores, axis=1, keepdims=True), new_score)
        prob = jnp.exp(scores - top)
        prob_new = jnp.exp(new_score - top)
        total = jnp.sum(prob, axis=1, keepdims=True) + prob_new
        acc = prob_new.astype(BF16).astype(F32) * v_rep
        for b in range(0, SEQ_GROUP, chunk):
            spread = jnp.concatenate([jnp.where(row_seq == b + j, prob, 0.0).astype(BF16) for j in range(chunk)], axis=1)
            acc = acc + dot(spread, vbuf[slot, b:b + chunk].reshape(chunk * cache_len, head_dim))
        attn = (acc / total).astype(BF16)
        for j in range(heads):
            abuf[seqs, j * head_dim:(j + 1) * head_dim] = attn[j * SEQ_GROUP:(j + 1) * SEQ_GROUP, :]

        @pl.when(i + KV_SLOTS < layers * groups)
        def _():
            kv_start(i + KV_SLOTS, slot)

    last = layers - 1
    exports = []

    def export(src, dst):
        pltpu.make_async_copy(src, dst, out_sem.at[len(exports)]).start()
        exports.append((src, dst))

    def qkv(l):
        a_ready(l)
        if l == 0:
            got("gain", gbuf.at[pl.ds(0, n_dev - 1)])
        cos_tab, sin_tab = cos_buf[...], sin_buf[...]
        normed = rms(hbuf[...].astype(F32), l)
        halves = [dot(normed, abuf_w[l, hf].reshape(width, a_cols)) for hf in range(2)]

        def rope(lead, tail):
            return jnp.concatenate([lead * cos_tab - tail * sin_tab, tail * cos_tab + lead * sin_tab], axis=1)

        for j in range(heads):
            out, lo = halves[j // (heads // 2)], (j % (heads // 2)) * head_dim
            qbuf[j] = (rope(out[:, lo:lo + half], out[:, lo + half:lo + head_dim]) * head_dim ** -0.5).astype(BF16)
        know[l] = rope(halves[0][:, q_half:q_half + half], halves[1][:, q_half:q_half + half]).astype(BF16).astype(F32)
        vnow[l] = jnp.concatenate([hv[:, q_half + half:q_half + 2 * half] for hv in halves], axis=1).astype(BF16).astype(F32)
        export(know.at[l], knew_ref.at[l])
        export(vnow.at[l], vnew_ref.at[l])

    r2 = rows // 2
    upper, lower = pl.ds(0, r2), pl.ds(r2, r2)

    def mix(l):
        b_ready(l)
        mixed = dot(abuf[...], bbuf_w[l].reshape(heads * head_dim, width))
        hid_mid = (hbuf[...].astype(F32) + mixed).astype(BF16)
        hbuf[...] = hid_mid
        y_all[l, x] = rms(hid_mid.astype(F32), layers + l)
        top, bottom = y_all.at[l, x, upper], y_all.at[l, x, lower]
        send(f"yR1{l}", [(top, top)], right)
        send(f"yL1{l}", [(bottom, bottom)], left)
        send(f"yR2{l}", [(bottom, bottom)], right)
        send(f"yL2{l}", [(top, top)], left)

    def yf(l):
        view = y_all.at[l, xl, upper]
        got(f"yR1{l}", view)
        send(f"yfR{l}", [(view, view)], right)
        view = y_all.at[l, xr, lower]
        got(f"yL1{l}", view)
        send(f"yfL{l}", [(view, view)], left)

    n_tile = 2 * LANES

    def gate_up(l, blocks):
        span = slice(0, len(blocks) * rows)

        def at_tile(n):
            return pl.ds(pl.multiple_of(n * n_tile, n_tile), n_tile)

        def multiply(n, slot):
            act = jnp.concatenate([y_all[l, b] for b in blocks], axis=0)
            for k in range(2):
                act_buf[slot, k, span] = dot(act, gu_w[l, k, :, :, :, at_tile(n)].reshape(width, n_tile))

        def activate(n, slot):
            mid = (jax.nn.gelu(act_buf[slot, 0, span], approximate=True) * act_buf[slot, 1, span]).astype(BF16)
            for k, b in enumerate(blocks):
                m_buf[b, :, at_tile(n)] = mid[k * rows:(k + 1) * rows]

        tiles = win // n_tile
        assert tiles % 2 == 1
        multiply(0, 0)

        @pl.loop(0, tiles // 2)
        def _(k):
            multiply(2 * k + 1, 1)
            activate(2 * k, 0)
            multiply(2 * k + 2, 0)
            activate(2 * k + 1, 1)

        activate(tiles - 1, 0)

    def guo(l):
        if l:
            c_ready(l)
        gate_up(l, (x,))

    def gua(l):
        got(f"yR2{l}", y_all.at[l, xl, lower])
        got(f"yL2{l}", y_all.at[l, xr, upper])
        if not l:
            c_ready(l)
        gate_up(l, (xl, xr))

    def gub(l):
        got(f"yfR{l}", y_all.at[l, xo, upper])
        got(f"yfL{l}", y_all.at[l, xo, lower])
        gate_up(l, (xo,))

    def down(l, xx):
        part[xx] = dot(m_buf[xx], wd_w[l])

    def near(l):
        if l:
            drain([f"{name}{l - 1}" for name in ("eR2", "eL2", "eR3", "eL3")])
        both = dot(jnp.concatenate([m_buf[xr], m_buf[xl]], axis=0), wd_w[l])
        part[xr] = both[:rows]
        part[xl] = both[rows:]
        if l == last:
            export(part.at[xr, lower], first_r.at[lower])
            export(part.at[xl, upper], first_l.at[upper])
            export(part.at[xr, upper], next_r)
            export(part.at[xl, lower], next_l)
        else:
            send(f"eR2{l}", [(part.at[xr, lower], r_f.at[l, 0, lower])], right)
            send(f"eL2{l}", [(part.at[xl, upper], r_f.at[l, 1, upper])], left)

    def far(l):
        if l:
            drain([f"{name}{l - 1}" for name in ("eR1", "eL1")])
        down(l, xo)
        if l == last:
            export(part.at[xo, upper], first_r.at[upper])
            export(part.at[xo, lower], first_l.at[lower])
        else:
            send(f"eR1{l}", [(part.at[xo, upper], r_t.at[l, 0])], right)
            send(f"eL1{l}", [(part.at[xo, lower], r_t.at[l, 1])], left)

    def er(l):
        got(f"eR1{l}", r_t.at[l, 0])
        part[xr, 0:r2] = part[xr, 0:r2] + r_t[l, 0]
        send(f"eR3{l}", [(part.at[xr, upper], r_f.at[l, 0, upper])], right)
        got(f"eL1{l}", r_t.at[l, 1])
        part[xl, r2:rows] = part[xl, r2:rows] + r_t[l, 1]
        send(f"eL3{l}", [(part.at[xl, lower], r_f.at[l, 1, lower])], left)

    def own(l):
        down(l, x)
        if l == last:
            export(part.at[x], own_out)
            export(hbuf, hid_out)

    def done(l):
        got(f"eR2{l}", r_f.at[l, 0, lower])
        got(f"eL2{l}", r_f.at[l, 1, upper])
        got(f"eR3{l}", r_f.at[l, 0, upper])
        got(f"eL3{l}", r_f.at[l, 1, lower])
        hbuf[...] = (hbuf[...].astype(F32) + (part[x] + r_f[l, 0] + r_f[l, 1])).astype(BF16)

    table = dict(
        ao=ao, af=af, ap=ap, ax=ax, at=at, aw=aw, bo=bo, bf=bf, bp=bp, bx=bx, bt=bt, bw=bw, cd=cd, ce=ce, ct=ct, cf=cf,
        cn=cn, cm=cm, cx=cx, cu=cu, cw=cw, dt=dt, **{"in": entry},
        qkv=qkv, mix=mix, yf=yf, guo=guo, gua=gua, gub=gub, dr=d_ready, near=near, far=far, er=er, own=own, done=done,
    )

    def run(step):
        table[step[:-1]](int(step[-1]))

    here = 0
    reached = [0] * layers
    while here < len(ORDER):
        step = ORDER[here]
        if not step.startswith("att"):
            run(step)
            here += 1
            continue
        l, count = int(step[-1]), 0
        while ORDER[here] == step:
            count += 1
            here += 1
        first = reached[l]
        reached[l] += count

        @pl.loop(first, first + count)
        def _(group):
            attend(l, group)

    drain(list(pending))
    for i, (src, dst) in enumerate(exports):
        pltpu.make_async_copy(src, dst, out_sem.at[i]).wait()
    assert len(msg_ids) <= send_sem.shape[0]


def decode(hidden, positions, k_cache, v_cache, attn_norm, w_query, w_key, w_value, w_out, mlp_norm, w_gate, w_up, w_down):
    layers, rows, _, cache_len, head_dim = k_cache.shape
    width = hidden.shape[1]
    n_dev = lax.axis_size("w")
    ff = w_gate.shape[-1]
    heads = w_query.shape[-1] // head_dim
    chip_cols = ff // CHIPS
    win = -(-(chip_cols + LANES // 2) // LANES) * LANES
    piece = width // n_dev
    groups = rows // SEQ_GROUP
    assert n_dev == CHIPS * CORES and heads * SEQ_GROUP == LANES and cache_len == LANES and rows == LANES
    assert lax.axis_size("dp") % 2 == 0
    inv_freq = np.float32(ROPE_BASE) ** (np.float32(-2.0) * np.arange(head_dim // 2, dtype=np.float32) / np.float32(head_dim))
    dims = (layers, rows, width, heads, head_dim, cache_len, n_dev, ff)
    anym = pl.BlockSpec(memory_space=pl.ANY)
    new_shape = jax.ShapeDtypeStruct((layers, rows, head_dim), F32)
    whole_sum = jax.ShapeDtypeStruct(hidden.shape, F32)
    half_sum = jax.ShapeDtypeStruct((rows // 2, width), F32)
    n_msg = 96
    return pl.pallas_call(
        functools.partial(decode_kernel, dims),
        out_shape=(jax.ShapeDtypeStruct(hidden.shape, BF16), new_shape, new_shape) + (whole_sum, whole_sum, half_sum, half_sum, whole_sum),
        in_specs=[anym] * 14,
        out_specs=(anym,) * 8,
        scratch_shapes=[
            pltpu.VMEM((rows, head_dim // 2), F32),
            pltpu.VMEM((rows, head_dim // 2), F32),
            pltpu.VMEM((2, 2, 2 * rows, 2 * LANES), F32),
            pltpu.VMEM(attn_norm.shape, F32),
            pltpu.VMEM(mlp_norm.shape, F32),
            pltpu.VMEM((1, head_dim // 2), F32),
            pltpu.VMEM((1, rows), jnp.int32),
            pltpu.VMEM((layers, rows, head_dim), F32),
            pltpu.VMEM((layers, rows, head_dim), F32),
            pltpu.VMEM((8, 2 * LANES), F32),
            pltpu.VMEM((n_dev, 8, 2 * LANES), F32),
            pltpu.VMEM((rows, LANES), F32),
            pltpu.VMEM((layers, 2, CHIPS, CORES, piece, w_query.shape[-1] // 2 + head_dim), BF16),
            pltpu.VMEM((layers, CHIPS, CORES, w_out.shape[1], width), BF16),
            pltpu.VMEM((layers, 2, CHIPS, CORES, piece, win), BF16),
            pltpu.VMEM((layers, win, width), BF16),
            pltpu.VMEM((layers, 2, piece, win // 2), BF16),
            pltpu.VMEM((layers, CHIPS, rows, width), BF16),
            pltpu.VMEM((CHIPS, rows, win), BF16),
            pltpu.VMEM((CHIPS, rows, width), F32),
            pltpu.VMEM((layers - 1, 2, rows // 2, width), F32),
            pltpu.VMEM((layers - 1, 2, rows, width), F32),
            pltpu.VMEM((KV_SLOTS, SEQ_GROUP, cache_len, head_dim), BF16),
            pltpu.VMEM((KV_SLOTS, SEQ_GROUP, cache_len, head_dim), BF16),
            pltpu.VMEM((heads, rows, head_dim), BF16),
            pltpu.VMEM((rows, heads * head_dim), BF16),
            pltpu.VMEM((rows, width), BF16),
            pltpu.SemaphoreType.DMA((n_msg,)),
            pltpu.SemaphoreType.DMA((n_msg,)),
            pltpu.SemaphoreType.DMA((4 * layers,)),
            pltpu.SemaphoreType.DMA((KV_SLOTS, 2)),
            pltpu.SemaphoreType.DMA((16,)),
            pltpu.SemaphoreType.DMA((8,)),
        ],
        compiler_params=pltpu.CompilerParams(collective_id=0, has_side_effects=True, vmem_limit_bytes=67043328),
        name="decode",
    )(hidden, jnp.asarray(inv_freq).reshape(1, head_dim // 2), attn_norm, mlp_norm, positions.reshape(1, rows), k_cache, v_cache, w_query, w_key, w_value, w_out, w_gate, w_up, w_down)


TILE_ROWS = 16
CACHE_BLOCK = 16


def cache_kernel(pos_ref, old_ref, new_ref, out_ref, buf, in_sem, out_sem):
    layers, rows = old_ref.shape[:2]
    blocks = rows // CACHE_BLOCK
    def load(l, b):
        i = l * blocks + b
        return pltpu.make_async_copy(old_ref.at[l, pl.ds(b * CACHE_BLOCK, CACHE_BLOCK), 0], buf.at[i], in_sem.at[i])

    def store(l, b):
        i = l * blocks + b
        return pltpu.make_async_copy(buf.at[i], out_ref.at[l, pl.ds(b * CACHE_BLOCK, CACHE_BLOCK), 0], out_sem.at[i])

    steps = [(l, b) for l in range(layers) for b in range(blocks)]
    for l, b in steps:
        load(l, b).start()
    row = lax.broadcasted_iota(jnp.int32, (TILE_ROWS, buf.shape[-1]), 0)
    for l in range(layers):
        @pl.loop(0, blocks)
        def _(b):
            load(l, b).wait()
            fresh = new_ref[l, pl.ds(pl.multiple_of(b * CACHE_BLOCK, CACHE_BLOCK), CACHE_BLOCK), :]
            tiles = []
            for s in range(CACHE_BLOCK):
                pos = pos_ref[b * CACHE_BLOCK + s]
                base = pl.multiple_of(pos // TILE_ROWS * TILE_ROWS, TILE_ROWS)
                tile = buf[l * blocks + b, s, pl.ds(base, TILE_ROWS), :].astype(F32)
                tiles.append((s, base, jnp.where(row == pos - base, fresh[s:s + 1, :], tile).astype(BF16)))
            for s, base, tile in tiles:
                buf[l * blocks + b, s, pl.ds(base, TILE_ROWS), :] = tile
            store(l, b).start()
    for l, b in steps:
        store(l, b).wait()


def write_cache(positions, cache, new_rows):
    cache_len, head_dim = cache.shape[-2:]
    slots = cache.shape[0] * cache.shape[1] // CACHE_BLOCK
    vmem, anym = pl.BlockSpec(memory_space=pltpu.VMEM), pl.BlockSpec(memory_space=pl.ANY)
    return pl.pallas_call(
        cache_kernel,
        out_shape=jax.ShapeDtypeStruct(cache.shape, BF16),
        in_specs=[pl.BlockSpec(memory_space=pltpu.SMEM), anym, vmem],
        out_specs=anym,
        scratch_shapes=[
            pltpu.VMEM((slots, CACHE_BLOCK, cache_len, head_dim), BF16),
            pltpu.SemaphoreType.DMA((slots,)),
            pltpu.SemaphoreType.DMA((slots,)),
        ],
        cost_estimate=pl.CostEstimate(flops=10**11, bytes_accessed=4 * cache.size, transcendentals=0),
        compiler_params=pltpu.CompilerParams(vmem_limit_bytes=60 * 2**20),
        name="cache",
    )(positions, cache, new_rows)


def solution(mesh):
    batch_spec = P(("dp", "w"))
    cache_spec = P(None, ("dp", "w"))
    gain_spec = P(None, "w")
    weight_spec = P(None, "w", None)

    def per_device(hidden, positions, k_cache, v_cache, *weights):
        hid_mid, k_new, v_new, first_r, first_l, next_r, next_l, own = decode(hidden, positions, k_cache, v_cache, *weights)
        n_dev, half = mesh.shape["w"], hidden.shape[0] // 2
        ahead = [(i, (i + CORES) % n_dev) for i in range(n_dev)]
        back = [(i, (i - CORES) % n_dev) for i in range(n_dev)]
        got_r = lax.ppermute(first_r, "w", ahead)
        got_l = lax.ppermute(first_l, "w", back)
        k_out = write_cache(positions, k_cache, k_new)
        upper = lax.ppermute(next_r + got_r[:half], "w", ahead)
        lower = lax.ppermute(next_l + got_l[half:], "w", back)
        v_out = write_cache(positions, v_cache, v_new)
        is_upper = lax.broadcasted_iota(jnp.int32, own.shape, 0) < half
        total = own + jnp.where(is_upper, got_l, got_r) + jnp.concatenate([upper, lower], axis=0)
        hidden_out = (hid_mid.astype(F32) + total).astype(BF16)
        return hidden_out, k_out, v_out

    in_specs = (batch_spec, batch_spec, cache_spec, cache_spec, gain_spec, weight_spec, weight_spec, weight_spec, weight_spec, gain_spec, weight_spec, weight_spec, weight_spec)
    out_specs = (batch_spec, cache_spec, cache_spec)
    return jax.shard_map(per_device, mesh=mesh, in_specs=in_specs, out_specs=out_specs, check_vma=False)
```

```python
import functools

import jax
import jax.numpy as jnp
import numpy as np
from jax import lax
from jax.experimental import pallas as pl
from jax.experimental.pallas import tpu as pltpu
from jax.sharding import PartitionSpec as P

EPS = 1e-6
ROPE_BASE = 10000.0
LANES = 128
CORES = 2
CHIPS = 4
SEQ_GROUP = 32
KV_SLOTS = 3
MESH = pl.DeviceIdType.MESH
F32 = jnp.float32
BF16 = jnp.bfloat16


def dot(a, b):
    return jnp.dot(a, b, preferred_element_type=F32)


def dot_t(a, b):
    return lax.dot_general(a, b, (((1,), (1,)), ((), ())), preferred_element_type=F32)


ORDER = (
    "bo0", "ao0", "in0", "bp0", "bq0", "bf0", "ct0", "ap0", "af0", "cd0", "ce0", "cf0", "ax0", "cd1", "bx0", "at0",
    "ao1", "cn0", "aw0", "ce1", "bw0", "bt0", "qkv0", "att0", "ct1", "cx0", "att0", "att0", "af1", "att0", "cm0", "mix0",
    "cu0", "ax1", "ap1", "yf0", "bo1", "dt0", "cw0", "cf1", "at1", "cm1", "gua0", "dr0", "near0", "gub0", "dt1", "cx1",
    "far0", "cn1", "er0", "guo0", "bf1", "own0", "aw1", "cu1", "done0", "qkv1", "att1", "att1", "bx1", "bt1", "att1", "att1",
    "mix1", "cw1", "yf1", "guo1", "dr1", "own1", "gua1", "near1", "gub1", "far1",
)
SHARE_A = (True, True)
SHARE_B = (True, False)


def decode_kernel(
    dims,
    hid_ref, freq_ref, an_ref, mn_ref, pos_ref, kc_ref, vc_ref,
    wq_ref, wk_ref, wv_ref, wo_ref, wg_ref, wu_ref, wd_ref,
    hid_out, knew_ref, vnew_ref, first_r, first_l, next_r, next_l, own_out,
    cos_buf, sin_buf, act_buf, an_buf, mn_buf, freq_buf, pos_in, know, vnow, gsrc, gbuf, pos_rows, abuf_w, bbuf_w, gu_w, wd_w, tr_w, y_all, m_buf, part, r_t, r_f,
    kbuf, vbuf, qbuf, abuf, hbuf,
    send_sem, recv_sem, loc_sem, kv_sem, out_sem, in_sem,
):
    layers, rows, width, heads, head_dim, cache_len, n_dev, ff = dims
    half = head_dim // 2
    piece = width // n_dev
    chip_cols = ff // CHIPS
    win = gu_w.shape[-1]
    pad = win - chip_cols
    wd_rows = wd_ref.shape[1]
    wo_rows = wo_ref.shape[1]
    q_half = wq_ref.shape[-1] // 2
    kv_half = half
    a_cols = abuf_w.shape[-1]
    groups = rows // SEQ_GROUP
    w = lax.axis_index("w")
    dp = lax.axis_index("dp")
    x, c = lax.div(w, CORES), lax.rem(w, CORES)
    h = lax.rem(dp, 2)
    xr, xo, xl = lax.rem(x + 1, CHIPS), lax.rem(x + 2, CHIPS), lax.rem(x + 3, CHIPS)
    cc = 1 - c
    hh = 1 - h
    right, left = (dp, xr * CORES + c), (dp, xl * CORES + c)
    twin = (dp, x * CORES + cc)
    pair = (dp + 1 - 2 * h, w)
    b_half, b_quarter = wo_rows // 2, wo_rows // 4
    b_mine = pl.multiple_of(h * b_half, b_quarter)
    b_mid = pl.multiple_of(h * b_half + b_quarter, b_quarter)
    b_other = pl.multiple_of(hh * b_half, b_quarter)
    b_last = pl.multiple_of(hh * b_half + b_quarter, b_quarter)
    q_mine = pl.multiple_of(h * q_half, LANES)
    kv_mine = pl.multiple_of(h * kv_half, LANES)
    starts = [pl.multiple_of(lax.div(chip_cols * xx, LANES) * LANES, LANES) for xx in (x, xr, xo, xl)]
    x_start, xr_start, xo_start, xl_start = starts
    xr_mid, xo_mid, xl_mid = [pl.multiple_of(xx + win // 2, LANES) for xx in starts[1:]]
    shift = lax.rem(chip_cols * x, LANES)
    wd_mine = pl.ds(pl.multiple_of(shift + wd_rows * c, 32), wd_rows)
    wd_twin = pl.ds(pl.multiple_of(shift + wd_rows * cc, 32), wd_rows)

    msg_ids = {}
    pending = {}

    def copy_of(name, src, dst, dev):
        i = msg_ids.setdefault(name, len(msg_ids))
        return pltpu.make_async_remote_copy(src, dst, send_sem.at[i], recv_sem.at[i], device_id=dev, device_id_type=MESH)

    def send(name, pairs, dev, view=None):
        for src, dst in pairs:
            copy_of(name, src, dst, dev).start()
        pending[name] = pairs[0][0] if view is None else view

    arrived = set()

    def got(name, view):
        if name not in arrived:
            arrived.add(name)
            copy_of(name, view, view, right).wait_recv()

    def drain(names):
        for name in names:
            view = pending.pop(name)
            copy_of(name, view, view, right).wait_send()

    def local_start(sem, pairs):
        for src, dst in pairs:
            pltpu.make_async_copy(src, dst, loc_sem.at[sem]).start()

    def local_wait(sem, view):
        if sem not in arrived:
            arrived.add(sem)
            pltpu.make_async_copy(view, view, loc_sem.at[sem]).wait()

    def kv_copies(i, slot):
        layer, group = lax.div(i, groups), lax.rem(i, groups)
        seqs = pl.ds(group * SEQ_GROUP, SEQ_GROUP)
        return (
            pltpu.make_async_copy(kc_ref.at[layer, seqs, 0], kbuf.at[slot], kv_sem.at[slot, 0]),
            pltpu.make_async_copy(vc_ref.at[layer, seqs, 0], vbuf.at[slot], kv_sem.at[slot, 1]),
        )

    def kv_start(i, slot):
        for copy in kv_copies(i, slot):
            copy.start()

    def a_pairs(l, hf, q_lo, kv_lo):
        dst = abuf_w.at[l, hf, x, c]
        return [
            (wq_ref.at[l, :, pl.ds(q_lo, q_half)], dst.at[:, pl.ds(0, q_half)]),
            (wk_ref.at[l, :, pl.ds(kv_lo, kv_half)], dst.at[:, pl.ds(q_half, kv_half)]),
            (wv_ref.at[l, :, pl.ds(kv_lo, kv_half)], dst.at[:, pl.ds(q_half + kv_half, kv_half)]),
        ]

    def a_both(l):
        return a_pairs(l, 0, 0, 0) + a_pairs(l, 1, q_half, kv_half)

    def a_block(l, xx):
        return abuf_w.at[l, h, xx, c] if SHARE_A[l] else abuf_w.at[l, :, xx, c]

    def a_lead(l, xx):
        return abuf_w.at[l, h, xx, c, :, pl.ds(0, a_cols // 2)] if SHARE_A[l] else abuf_w.at[l, 0, xx, c]

    def a_tail(l, xx):
        return abuf_w.at[l, h, xx, c, :, pl.ds(a_cols // 2, a_cols // 2)] if SHARE_A[l] else abuf_w.at[l, 1, xx, c]

    def ao(l):
        pairs = a_pairs(l, h, q_mine, kv_mine) if SHARE_A[l] else a_both(l)
        send(f"aR{l}", pairs, right, a_block(l, x))
        send(f"aL{l}", pairs, left, a_block(l, x))

    def to_pair(name, view):
        send(name, [(view, view)], pair)

    def a_near(l):
        got(f"aR{l}", a_block(l, xl))
        got(f"aL{l}", a_block(l, xr))

    def a_far(l):
        got(f"afR{l}", a_lead(l, xo))
        got(f"afL{l}", a_tail(l, xo))

    def af(l):
        a_near(l)
        send(f"afR{l}", [(a_lead(l, xl), a_lead(l, xl))], right)
        send(f"afL{l}", [(a_tail(l, xr), a_tail(l, xr))], left)

    def ap(l):
        a_near(l)
        to_pair(f"paR{l}", a_block(l, xl))
        to_pair(f"paL{l}", a_block(l, xr))

    def ax(l):
        a_far(l)
        if SHARE_A[l]:
            to_pair(f"paF{l}", a_block(l, xo))

    def at(l):
        a_near(l)
        a_far(l)
        local_wait(4 * l, abuf_w.at[l, :, x, c])
        view = abuf_w.at[l, h, :, c] if SHARE_A[l] else abuf_w.at[l, :, :, c]
        send(f"aT{l}", [(view, view)], twin)

    def aw(l):
        for name, xx in (("paR", xl), ("paL", xr), ("paF", xo)):
            got(f"{name}{l}", abuf_w.at[l, hh, xx, c])
        local_wait(4 * l, abuf_w.at[l, :, x, c])
        view = abuf_w.at[l, hh, :, c]
        send(f"aT1{l}", [(view, view)], twin)

    def a_ready(l):
        if SHARE_A[l]:
            got(f"aT{l}", abuf_w.at[l, h, :, cc])
            got(f"aT1{l}", abuf_w.at[l, hh, :, cc])
        else:
            got(f"aT{l}", abuf_w.at[l, :, :, cc])

    def b_block(l, xx):
        return bbuf_w.at[l, xx, c, pl.ds(b_mine, b_half)] if SHARE_B[l] else bbuf_w.at[l, xx, c]

    def b_lead(l, xx):
        return bbuf_w.at[l, xx, c, pl.ds(b_mine, b_quarter)] if SHARE_B[l] else bbuf_w.at[l, xx, c, pl.ds(0, b_half)]

    def b_tail(l, xx):
        return bbuf_w.at[l, xx, c, pl.ds(b_mid, b_quarter)] if SHARE_B[l] else bbuf_w.at[l, xx, c, pl.ds(b_half, b_half)]

    def bo(l):
        if not SHARE_B[l]:
            send(f"bR{l}", [(wo_ref.at[l], b_block(l, x))], right)
            send(f"bL{l}", [(wo_ref.at[l], b_block(l, x))], left)
            return
        for name, start, view in (("b", b_mine, b_lead(l, x)), ("bb", b_mid, b_tail(l, x))):
            src = wo_ref.at[l, pl.ds(start, b_quarter)]
            send(f"{name}R{l}", [(src, view)], right)
            send(f"{name}L{l}", [(src, view)], left)

    def b_near_lead(l):
        got(f"bR{l}", b_lead(l, xl))
        got(f"bL{l}", b_lead(l, xr))

    def b_near_tail(l):
        got(f"bbR{l}", b_tail(l, xl))
        got(f"bbL{l}", b_tail(l, xr))

    def b_near(l):
        if SHARE_B[l]:
            b_near_lead(l)
            b_near_tail(l)
        else:
            got(f"bR{l}", b_block(l, xl))
            got(f"bL{l}", b_block(l, xr))

    def b_far(l):
        got(f"bfR{l}", b_lead(l, xo))
        got(f"bfL{l}", b_tail(l, xo))

    def bf(l):
        b_near(l)
        send(f"bfR{l}", [(b_lead(l, xl), b_lead(l, xl))], right)
        send(f"bfL{l}", [(b_tail(l, xr), b_tail(l, xr))], left)

    def bp(l):
        b_near_lead(l)
        to_pair(f"pbR{l}", b_lead(l, xl))
        to_pair(f"pbL{l}", b_lead(l, xr))

    def bq(l):
        b_near_tail(l)
        to_pair(f"pbbR{l}", b_tail(l, xl))
        to_pair(f"pbbL{l}", b_tail(l, xr))

    def bx(l):
        b_far(l)
        if SHARE_B[l]:
            to_pair(f"pbF{l}", b_block(l, xo))

    def bt(l):
        b_near(l)
        b_far(l)
        local_wait(4 * l + 1, bbuf_w.at[l, x, c])
        view = bbuf_w.at[l, :, c, pl.ds(b_mine, b_half)] if SHARE_B[l] else bbuf_w.at[l, :, c]
        send(f"bT{l}", [(view, view)], twin)

    def bw(l):
        for name, xx in (("R", xl), ("L", xr)):
            got(f"pb{name}{l}", bbuf_w.at[l, xx, c, pl.ds(b_other, b_quarter)])
            got(f"pbb{name}{l}", bbuf_w.at[l, xx, c, pl.ds(b_last, b_quarter)])
        got(f"pbF{l}", bbuf_w.at[l, xo, c, pl.ds(b_other, b_half)])
        local_wait(4 * l + 1, bbuf_w.at[l, x, c])
        view = bbuf_w.at[l, :, c, pl.ds(b_other, b_half)]
        send(f"bT1{l}", [(view, view)], twin)

    def b_ready(l):
        if SHARE_B[l]:
            got(f"bT{l}", bbuf_w.at[l, :, cc, pl.ds(b_mine, b_half)])
            got(f"bT1{l}", bbuf_w.at[l, :, cc, pl.ds(b_other, b_half)])
        else:
            got(f"bT{l}", bbuf_w.at[l, :, cc])

    def by_matrix(l, name, lo, size, dst, dev):
        for value, ref in ((0, wg_ref), (1, wu_ref)):
            @pl.when(h == value)
            def _():
                copy_of(name, ref.at[l, :, pl.ds(lo, size)], dst, dev).start()
        pending[name] = dst

    fore, aft = pl.ds(0, win // 2), pl.ds(win // 2, win // 2)

    def cd(l):
        by_matrix(l, f"cR{l}", xr_start, win // 2, gu_w.at[l, h, x, c, :, fore], right)
        by_matrix(l, f"cL{l}", xl_start, win // 2, gu_w.at[l, h, x, c, :, fore], left)

    def ce(l):
        by_matrix(l, f"dR{l}", xr_mid, win // 2, gu_w.at[l, h, x, c, :, aft], right)
        by_matrix(l, f"dL{l}", xl_mid, win // 2, gu_w.at[l, h, x, c, :, aft], left)

    def ct(l):
        by_matrix(l, f"tR{l}", xo_start, win // 2, tr_w.at[l, 0], right)
        by_matrix(l, f"tL{l}", xo_mid, win // 2, tr_w.at[l, 1], left)

    def cf(l):
        got(f"tR{l}", tr_w.at[l, 0])
        send(f"cfR{l}", [(tr_w.at[l, 0], gu_w.at[l, h, xl, c, :, fore])], right)
        got(f"tL{l}", tr_w.at[l, 1])
        send(f"cfL{l}", [(tr_w.at[l, 1], gu_w.at[l, h, xr, c, :, aft])], left)

    def c_near(l, part_name, cols):
        got(f"{part_name}R{l}", gu_w.at[l, h, xl, c, :, cols])
        got(f"{part_name}L{l}", gu_w.at[l, h, xr, c, :, cols])

    def c_far(l):
        got(f"cfR{l}", gu_w.at[l, h, xo, c, :, fore])
        got(f"cfL{l}", gu_w.at[l, h, xo, c, :, aft])

    def cn(l):
        c_near(l, "c", fore)
        to_pair(f"pcR{l}", gu_w.at[l, h, xl, c, :, fore])
        to_pair(f"pcL{l}", gu_w.at[l, h, xr, c, :, fore])

    def cm(l):
        c_near(l, "d", aft)
        to_pair(f"pdR{l}", gu_w.at[l, h, xl, c, :, aft])
        to_pair(f"pdL{l}", gu_w.at[l, h, xr, c, :, aft])

    def cx(l):
        c_far(l)
        to_pair(f"pcF{l}", gu_w.at[l, h, xo, c])

    def cu(l):
        c_near(l, "c", fore)
        c_near(l, "d", aft)
        c_far(l)
        local_wait(4 * l + 2, gu_w.at[l, :, x, c])
        view = gu_w.at[l, h, :, c]
        send(f"cT{l}", [(view, view)], twin)

    def cw(l):
        for name, xx, cols in (("pcR", xl, fore), ("pcL", xr, fore), ("pdR", xl, aft), ("pdL", xr, aft)):
            got(f"{name}{l}", gu_w.at[l, hh, xx, c, :, cols])
        got(f"pcF{l}", gu_w.at[l, hh, xo, c])
        local_wait(4 * l + 2, gu_w.at[l, :, x, c])
        view = gu_w.at[l, hh, :, c]
        send(f"cT1{l}", [(view, view)], twin)

    def c_ready(l):
        got(f"cT{l}", gu_w.at[l, h, :, cc])
        got(f"cT1{l}", gu_w.at[l, hh, :, cc])

    def dt(l):
        send(f"dT{l}", [(wd_ref.at[l], wd_w.at[l, wd_mine])], twin)

    def d_ready(l):
        local_wait(4 * l + 3, wd_w.at[l, wd_mine])
        got(f"dT{l}", wd_w.at[l, wd_twin])

    small = [(an_ref, an_buf), (mn_ref, mn_buf), (freq_ref, freq_buf), (pos_ref, pos_in)]
    for i, (src, dst) in enumerate(small):
        pltpu.make_async_copy(src, dst, in_sem.at[i]).start()
    barrier = pltpu.get_barrier_semaphore()
    for i in range(1, n_dev):
        pl.semaphore_signal(barrier, inc=1, device_id=(dp, lax.rem(w + i, n_dev)), device_id_type=MESH)
    pl.semaphore_signal(barrier, inc=1, device_id=pair, device_id_type=MESH)
    pl.semaphore_wait(barrier, n_dev)

    def entry(_):
        hid_copy = pltpu.make_async_copy(hid_ref, hbuf, in_sem.at[len(small)])
        hid_copy.start()
        for i in range(KV_SLOTS):
            kv_start(i, i)
        for l in range(layers):
            local_start(4 * l, a_both(l))
            local_start(4 * l + 1, [(wo_ref.at[l], bbuf_w.at[l, x, c])])
            cols = pl.ds(x_start, win)
            local_start(4 * l + 2, [(wg_ref.at[l, :, cols], gu_w.at[l, 0, x, c]), (wu_ref.at[l, :, cols], gu_w.at[l, 1, x, c])])
            local_start(4 * l + 3, [(wd_ref.at[l], wd_w.at[l, wd_mine])])
        for i, (src, dst) in enumerate(small):
            pltpu.make_async_copy(src, dst, in_sem.at[i]).wait()
        gsrc[...] = jnp.zeros_like(gsrc)
        gsrc[0:layers, 0:piece] = an_buf[...]
        gsrc[layers:2 * layers, 0:piece] = mn_buf[...]
        own_gain = pltpu.roll(gsrc[...], lax.rem(w * piece, LANES), 1)
        gsrc[...] = own_gain
        gbuf[w] = own_gain
        for l in range(layers):
            start = pl.multiple_of(jnp.where(lax.rem(x, 2) == 0, chip_cols, 0), 64)
            wd_w[l, pl.ds(start, pad), :] = jnp.zeros((pad, width), BF16)
        pos_rows[...] = jnp.broadcast_to(pos_in[...].astype(F32), (rows, rows)).T
        angles = pos_rows[...] * freq_buf[...]
        cos_buf[...] = jnp.cos(angles)
        sin_buf[...] = jnp.sin(angles)
        for i in range(1, n_dev):
            copy_of("gain", gsrc, gbuf.at[w], (dp, lax.rem(w + i, n_dev))).start()
        pending["gain"] = gbuf.at[pl.ds(0, n_dev - 1)]
        hid_copy.wait()

    def all_gains():
        tiles = []
        for j in range(width // LANES):
            total = None
            for s in range(n_dev):
                lo = (s * piece) // LANES
                for k in range(2):
                    if lo + k == j:
                        block = gbuf[s, :, k * LANES:(k + 1) * LANES]
                        total = block if total is None else total + block
            tiles.append(total)
        return 1.0 + jnp.concatenate(tiles, axis=1)

    def rms(hid, row):
        mean_sq = jnp.sum(hid * hid, axis=-1, keepdims=True) / width
        return (hid * lax.rsqrt(mean_sq + EPS) * all_gains()[row:row + 1, :]).astype(BF16)

    chunk = 4

    def attend(l, group):
        row_seq = lax.rem(lax.broadcasted_iota(jnp.int32, (LANES, cache_len), 0), SEQ_GROUP)
        place = lax.broadcasted_iota(jnp.int32, (LANES, cache_len), 1).astype(F32)
        i = l * groups + group
        slot = lax.rem(i, KV_SLOTS)
        for copy in kv_copies(i, slot):
            copy.wait()
        seqs = pl.ds(pl.multiple_of(group * SEQ_GROUP, SEQ_GROUP), SEQ_GROUP)
        query = jnp.concatenate([qbuf[j, seqs, :] for j in range(heads)], axis=0)
        scores = jnp.zeros((LANES, cache_len), F32)
        for b in range(0, SEQ_GROUP, chunk):
            prod = dot_t(query, kbuf[slot, b:b + chunk].reshape(chunk * cache_len, head_dim))
            for j in range(chunk):
                scores = jnp.where(row_seq == b + j, prod[:, j * cache_len:(j + 1) * cache_len], scores)
        k_rep = jnp.concatenate([know[l, seqs, :]] * heads, axis=0)
        v_rep = jnp.concatenate([vnow[l, seqs, :]] * heads, axis=0)
        new_score = jnp.sum(query.astype(F32) * k_rep, axis=1, keepdims=True)
        pos = jnp.concatenate([pos_rows[seqs, :]] * heads, axis=0)
        scores = jnp.where(place < pos, scores, -1e30)
        top = jnp.maximum(jnp.max(scores, axis=1, keepdims=True), new_score)
        prob = jnp.exp(scores - top)
        prob_new = jnp.exp(new_score - top)
        total = jnp.sum(prob, axis=1, keepdims=True) + prob_new
        acc = prob_new.astype(BF16).astype(F32) * v_rep
        for b in range(0, SEQ_GROUP, chunk):
            spread = jnp.concatenate([jnp.where(row_seq == b + j, prob, 0.0).astype(BF16) for j in range(chunk)], axis=1)
            acc = acc + dot(spread, vbuf[slot, b:b + chunk].reshape(chunk * cache_len, head_dim))
        attn = (acc / total).astype(BF16)
        for j in range(heads):
            abuf[seqs, j * head_dim:(j + 1) * head_dim] = attn[j * SEQ_GROUP:(j + 1) * SEQ_GROUP, :]

        @pl.when(i + KV_SLOTS < layers * groups)
        def _():
            kv_start(i + KV_SLOTS, slot)

    last = layers - 1
    exports = []

    def export(src, dst):
        pltpu.make_async_copy(src, dst, out_sem.at[len(exports)]).start()
        exports.append((src, dst))

    def qkv(l):
        a_ready(l)
        if l == 0:
            got("gain", gbuf.at[pl.ds(0, n_dev - 1)])
        cos_tab, sin_tab = cos_buf[...], sin_buf[...]
        normed = rms(hbuf[...].astype(F32), l)
        halves = [dot(normed, abuf_w[l, hf].reshape(width, a_cols)) for hf in range(2)]

        def rope(lead, tail):
            return jnp.concatenate([lead * cos_tab - tail * sin_tab, tail * cos_tab + lead * sin_tab], axis=1)

        for j in range(heads):
            out, lo = halves[j // (heads // 2)], (j % (heads // 2)) * head_dim
            qbuf[j] = (rope(out[:, lo:lo + half], out[:, lo + half:lo + head_dim]) * head_dim ** -0.5).astype(BF16)
        know[l] = rope(halves[0][:, q_half:q_half + half], halves[1][:, q_half:q_half + half]).astype(BF16).astype(F32)
        vnow[l] = jnp.concatenate([hv[:, q_half + half:q_half + 2 * half] for hv in halves], axis=1).astype(BF16).astype(F32)
        export(know.at[l], knew_ref.at[l])
        export(vnow.at[l], vnew_ref.at[l])

    r2 = rows // 2
    upper, lower = pl.ds(0, r2), pl.ds(r2, r2)

    def mix(l):
        b_ready(l)
        mixed = dot(abuf[...], bbuf_w[l].reshape(heads * head_dim, width))
        hid_mid = (hbuf[...].astype(F32) + mixed).astype(BF16)
        hbuf[...] = hid_mid
        y_all[l, x] = rms(hid_mid.astype(F32), layers + l)
        top, bottom = y_all.at[l, x, upper], y_all.at[l, x, lower]
        send(f"yR1{l}", [(top, top)], right)
        send(f"yL1{l}", [(bottom, bottom)], left)
        send(f"yR2{l}", [(bottom, bottom)], right)
        send(f"yL2{l}", [(top, top)], left)

    def yf(l):
        view = y_all.at[l, xl, upper]
        got(f"yR1{l}", view)
        send(f"yfR{l}", [(view, view)], right)
        view = y_all.at[l, xr, lower]
        got(f"yL1{l}", view)
        send(f"yfL{l}", [(view, view)], left)

    n_tile = 2 * LANES

    def gate_up(l, blocks):
        span = slice(0, len(blocks) * rows)

        def at_tile(n):
            return pl.ds(pl.multiple_of(n * n_tile, n_tile), n_tile)

        def multiply(n, slot):
            act = jnp.concatenate([y_all[l, b] for b in blocks], axis=0)
            for k in range(2):
                act_buf[slot, k, span] = dot(act, gu_w[l, k, :, :, :, at_tile(n)].reshape(width, n_tile))

        def activate(n, slot):
            mid = (jax.nn.gelu(act_buf[slot, 0, span], approximate=True) * act_buf[slot, 1, span]).astype(BF16)
            for k, b in enumerate(blocks):
                m_buf[b, :, at_tile(n)] = mid[k * rows:(k + 1) * rows]

        tiles = win // n_tile
        assert tiles % 2 == 1
        multiply(0, 0)

        @pl.loop(0, tiles // 2)
        def _(k):
            multiply(2 * k + 1, 1)
            activate(2 * k, 0)
            multiply(2 * k + 2, 0)
            activate(2 * k + 1, 1)

        activate(tiles - 1, 0)

    def guo(l):
        if l:
            c_ready(l)
        gate_up(l, (x,))

    def gua(l):
        got(f"yR2{l}", y_all.at[l, xl, lower])
        got(f"yL2{l}", y_all.at[l, xr, upper])
        if not l:
            c_ready(l)
        gate_up(l, (xl, xr))

    def gub(l):
        got(f"yfR{l}", y_all.at[l, xo, upper])
        got(f"yfL{l}", y_all.at[l, xo, lower])
        gate_up(l, (xo,))

    def down(l, xx):
        part[xx] = dot(m_buf[xx], wd_w[l])

    def near(l):
        if l:
            drain([f"{name}{l - 1}" for name in ("eR2", "eL2", "eR3", "eL3")])
        both = dot(jnp.concatenate([m_buf[xr], m_buf[xl]], axis=0), wd_w[l])
        part[xr] = both[:rows]
        part[xl] = both[rows:]
        if l == last:
            export(part.at[xr, lower], first_r.at[lower])
            export(part.at[xl, upper], first_l.at[upper])
            export(part.at[xr, upper], next_r)
            export(part.at[xl, lower], next_l)
        else:
            send(f"eR2{l}", [(part.at[xr, lower], r_f.at[l, 0, lower])], right)
            send(f"eL2{l}", [(part.at[xl, upper], r_f.at[l, 1, upper])], left)

    def far(l):
        if l:
            drain([f"{name}{l - 1}" for name in ("eR1", "eL1")])
        down(l, xo)
        if l == last:
            export(part.at[xo, upper], first_r.at[upper])
            export(part.at[xo, lower], first_l.at[lower])
        else:
            send(f"eR1{l}", [(part.at[xo, upper], r_t.at[l, 0])], right)
            send(f"eL1{l}", [(part.at[xo, lower], r_t.at[l, 1])], left)

    def er(l):
        got(f"eR1{l}", r_t.at[l, 0])
        part[xr, 0:r2] = part[xr, 0:r2] + r_t[l, 0]
        send(f"eR3{l}", [(part.at[xr, upper], r_f.at[l, 0, upper])], right)
        got(f"eL1{l}", r_t.at[l, 1])
        part[xl, r2:rows] = part[xl, r2:rows] + r_t[l, 1]
        send(f"eL3{l}", [(part.at[xl, lower], r_f.at[l, 1, lower])], left)

    def own(l):
        down(l, x)
        if l == last:
            export(part.at[x], own_out)
            export(hbuf, hid_out)

    def done(l):
        got(f"eR2{l}", r_f.at[l, 0, lower])
        got(f"eL2{l}", r_f.at[l, 1, upper])
        got(f"eR3{l}", r_f.at[l, 0, upper])
        got(f"eL3{l}", r_f.at[l, 1, lower])
        hbuf[...] = (hbuf[...].astype(F32) + (part[x] + r_f[l, 0] + r_f[l, 1])).astype(BF16)

    table = dict(
        ao=ao, af=af, ap=ap, ax=ax, at=at, aw=aw, bo=bo, bf=bf, bp=bp, bq=bq, bx=bx, bt=bt, bw=bw, cd=cd, ce=ce, ct=ct, cf=cf,
        cn=cn, cm=cm, cx=cx, cu=cu, cw=cw, dt=dt, **{"in": entry},
        qkv=qkv, mix=mix, yf=yf, guo=guo, gua=gua, gub=gub, dr=d_ready, near=near, far=far, er=er, own=own, done=done,
    )

    def run(step):
        table[step[:-1]](int(step[-1]))

    here = 0
    reached = [0] * layers
    while here < len(ORDER):
        step = ORDER[here]
        if not step.startswith("att"):
            run(step)
            here += 1
            continue
        l, count = int(step[-1]), 0
        while ORDER[here] == step:
            count += 1
            here += 1
        first = reached[l]
        reached[l] += count

        @pl.loop(first, first + count)
        def _(group):
            attend(l, group)

    drain(list(pending))
    for i, (src, dst) in enumerate(exports):
        pltpu.make_async_copy(src, dst, out_sem.at[i]).wait()
    assert len(msg_ids) <= send_sem.shape[0]


def decode(hidden, positions, k_cache, v_cache, attn_norm, w_query, w_key, w_value, w_out, mlp_norm, w_gate, w_up, w_down):
    layers, rows, _, cache_len, head_dim = k_cache.shape
    width = hidden.shape[1]
    n_dev = lax.axis_size("w")
    ff = w_gate.shape[-1]
    heads = w_query.shape[-1] // head_dim
    chip_cols = ff // CHIPS
    win = -(-(chip_cols + LANES // 2) // LANES) * LANES
    piece = width // n_dev
    groups = rows // SEQ_GROUP
    assert n_dev == CHIPS * CORES and heads * SEQ_GROUP == LANES and cache_len == LANES and rows == LANES
    assert lax.axis_size("dp") % 2 == 0
    inv_freq = np.float32(ROPE_BASE) ** (np.float32(-2.0) * np.arange(head_dim // 2, dtype=np.float32) / np.float32(head_dim))
    dims = (layers, rows, width, heads, head_dim, cache_len, n_dev, ff)
    anym = pl.BlockSpec(memory_space=pl.ANY)
    new_shape = jax.ShapeDtypeStruct((layers, rows, head_dim), F32)
    whole_sum = jax.ShapeDtypeStruct(hidden.shape, F32)
    half_sum = jax.ShapeDtypeStruct((rows // 2, width), F32)
    n_msg = 96
    return pl.pallas_call(
        functools.partial(decode_kernel, dims),
        out_shape=(jax.ShapeDtypeStruct(hidden.shape, BF16), new_shape, new_shape) + (whole_sum, whole_sum, half_sum, half_sum, whole_sum),
        in_specs=[anym] * 14,
        out_specs=(anym,) * 8,
        scratch_shapes=[
            pltpu.VMEM((rows, head_dim // 2), F32),
            pltpu.VMEM((rows, head_dim // 2), F32),
            pltpu.VMEM((2, 2, 2 * rows, 2 * LANES), F32),
            pltpu.VMEM(attn_norm.shape, F32),
            pltpu.VMEM(mlp_norm.shape, F32),
            pltpu.VMEM((1, head_dim // 2), F32),
            pltpu.VMEM((1, rows), jnp.int32),
            pltpu.VMEM((layers, rows, head_dim), F32),
            pltpu.VMEM((layers, rows, head_dim), F32),
            pltpu.VMEM((8, 2 * LANES), F32),
            pltpu.VMEM((n_dev, 8, 2 * LANES), F32),
            pltpu.VMEM((rows, LANES), F32),
            pltpu.VMEM((layers, 2, CHIPS, CORES, piece, w_query.shape[-1] // 2 + head_dim), BF16),
            pltpu.VMEM((layers, CHIPS, CORES, w_out.shape[1], width), BF16),
            pltpu.VMEM((layers, 2, CHIPS, CORES, piece, win), BF16),
            pltpu.VMEM((layers, win, width), BF16),
            pltpu.VMEM((layers, 2, piece, win // 2), BF16),
            pltpu.VMEM((layers, CHIPS, rows, width), BF16),
            pltpu.VMEM((CHIPS, rows, win), BF16),
            pltpu.VMEM((CHIPS, rows, width), F32),
            pltpu.VMEM((layers - 1, 2, rows // 2, width), F32),
            pltpu.VMEM((layers - 1, 2, rows, width), F32),
            pltpu.VMEM((KV_SLOTS, SEQ_GROUP, cache_len, head_dim), BF16),
            pltpu.VMEM((KV_SLOTS, SEQ_GROUP, cache_len, head_dim), BF16),
            pltpu.VMEM((heads, rows, head_dim), BF16),
            pltpu.VMEM((rows, heads * head_dim), BF16),
            pltpu.VMEM((rows, width), BF16),
            pltpu.SemaphoreType.DMA((n_msg,)),
            pltpu.SemaphoreType.DMA((n_msg,)),
            pltpu.SemaphoreType.DMA((4 * layers,)),
            pltpu.SemaphoreType.DMA((KV_SLOTS, 2)),
            pltpu.SemaphoreType.DMA((16,)),
            pltpu.SemaphoreType.DMA((8,)),
        ],
        compiler_params=pltpu.CompilerParams(collective_id=0, has_side_effects=True, vmem_limit_bytes=67043328),
        name="decode",
    )(hidden, jnp.asarray(inv_freq).reshape(1, head_dim // 2), attn_norm, mlp_norm, positions.reshape(1, rows), k_cache, v_cache, w_query, w_key, w_value, w_out, w_gate, w_up, w_down)


TILE_ROWS = 16
CACHE_BLOCK = 16


def cache_kernel(pos_ref, old_ref, new_ref, out_ref, buf, in_sem, out_sem):
    layers, rows = old_ref.shape[:2]
    blocks = rows // CACHE_BLOCK
    def load(l, b):
        i = l * blocks + b
        return pltpu.make_async_copy(old_ref.at[l, pl.ds(b * CACHE_BLOCK, CACHE_BLOCK), 0], buf.at[i], in_sem.at[i])

    def store(l, b):
        i = l * blocks + b
        return pltpu.make_async_copy(buf.at[i], out_ref.at[l, pl.ds(b * CACHE_BLOCK, CACHE_BLOCK), 0], out_sem.at[i])

    steps = [(l, b) for l in range(layers) for b in range(blocks)]
    for l, b in steps:
        load(l, b).start()
    row = lax.broadcasted_iota(jnp.int32, (TILE_ROWS, buf.shape[-1]), 0)
    for l in range(layers):
        @pl.loop(0, blocks)
        def _(b):
            load(l, b).wait()
            fresh = new_ref[l, pl.ds(pl.multiple_of(b * CACHE_BLOCK, CACHE_BLOCK), CACHE_BLOCK), :]
            tiles = []
            for s in range(CACHE_BLOCK):
                pos = pos_ref[b * CACHE_BLOCK + s]
                base = pl.multiple_of(pos // TILE_ROWS * TILE_ROWS, TILE_ROWS)
                tile = buf[l * blocks + b, s, pl.ds(base, TILE_ROWS), :].astype(F32)
                tiles.append((s, base, jnp.where(row == pos - base, fresh[s:s + 1, :], tile).astype(BF16)))
            for s, base, tile in tiles:
                buf[l * blocks + b, s, pl.ds(base, TILE_ROWS), :] = tile
            store(l, b).start()
    for l, b in steps:
        store(l, b).wait()


def write_cache(positions, cache, new_rows):
    cache_len, head_dim = cache.shape[-2:]
    slots = cache.shape[0] * cache.shape[1] // CACHE_BLOCK
    vmem, anym = pl.BlockSpec(memory_space=pltpu.VMEM), pl.BlockSpec(memory_space=pl.ANY)
    return pl.pallas_call(
        cache_kernel,
        out_shape=jax.ShapeDtypeStruct(cache.shape, BF16),
        in_specs=[pl.BlockSpec(memory_space=pltpu.SMEM), anym, vmem],
        out_specs=anym,
        scratch_shapes=[
            pltpu.VMEM((slots, CACHE_BLOCK, cache_len, head_dim), BF16),
            pltpu.SemaphoreType.DMA((slots,)),
            pltpu.SemaphoreType.DMA((slots,)),
        ],
        cost_estimate=pl.CostEstimate(flops=10**11, bytes_accessed=4 * cache.size, transcendentals=0),
        compiler_params=pltpu.CompilerParams(vmem_limit_bytes=60 * 2**20),
        name="cache",
    )(positions, cache, new_rows)


def solution(mesh):
    batch_spec = P(("dp", "w"))
    cache_spec = P(None, ("dp", "w"))
    gain_spec = P(None, "w")
    weight_spec = P(None, "w", None)

    def per_device(hidden, positions, k_cache, v_cache, *weights):
        hid_mid, k_new, v_new, first_r, first_l, next_r, next_l, own = decode(hidden, positions, k_cache, v_cache, *weights)
        n_dev, half = mesh.shape["w"], hidden.shape[0] // 2
        ahead = [(i, (i + CORES) % n_dev) for i in range(n_dev)]
        back = [(i, (i - CORES) % n_dev) for i in range(n_dev)]
        got_r = lax.ppermute(first_r, "w", ahead)
        got_l = lax.ppermute(first_l, "w", back)
        k_out = write_cache(positions, k_cache, k_new)
        upper = lax.ppermute(next_r + got_r[:half], "w", ahead)
        lower = lax.ppermute(next_l + got_l[half:], "w", back)
        v_out = write_cache(positions, v_cache, v_new)
        is_upper = lax.broadcasted_iota(jnp.int32, own.shape, 0) < half
        total = own + jnp.where(is_upper, got_l, got_r) + jnp.concatenate([upper, lower], axis=0)
        hidden_out = (hid_mid.astype(F32) + total).astype(BF16)
        return hidden_out, k_out, v_out

    in_specs = (batch_spec, batch_spec, cache_spec, cache_spec, gain_spec, weight_spec, weight_spec, weight_spec, weight_spec, gain_spec, weight_spec, weight_spec, weight_spec)
    out_specs = (batch_spec, cache_spec, cache_spec)
    return jax.shard_map(per_device, mesh=mesh, in_specs=in_specs, out_specs=out_specs, check_vma=False)
```

```python
import functools

import jax
import jax.numpy as jnp
import numpy as np
from jax import lax
from jax.experimental import pallas as pl
from jax.experimental.pallas import tpu as pltpu
from jax.sharding import PartitionSpec as P

EPS = 1e-6
ROPE_BASE = 10000.0
LANES = 128
CORES = 2
CHIPS = 4
SEQ_GROUP = 32
KV_SLOTS = 3
MESH = pl.DeviceIdType.MESH
F32 = jnp.float32
BF16 = jnp.bfloat16


def dot(a, b):
    return jnp.dot(a, b, preferred_element_type=F32)


def dot_t(a, b):
    return lax.dot_general(a, b, (((1,), (1,)), ((), ())), preferred_element_type=F32)


ORDER = (
    "bo0", "ao0", "in0", "bp0", "bq0", "bf0", "ct0", "ap0", "af0", "cd0", "ce0", "cf0", "ax0", "cd1", "bx0", "at0",
    "ao1", "cn0", "aw0", "ce1", "bw0", "bt0", "qkv0", "att0", "ct1", "cx0", "att0", "att0", "af1", "att0", "cm0", "mix0",
    "cu0", "ax1", "ap1", "yf0", "bo1", "dt0", "cw0", "cf1", "at1", "cm1", "gua0", "dr0", "near0", "gub0", "dt1", "cx1",
    "far0", "cn1", "er0", "guo0", "bf1", "own0", "aw1", "cu1", "done0", "qkv1", "att1", "att1", "bx1", "bt1", "att1", "att1",
    "mix1", "cw1", "yf1", "guo1", "dr1", "own1", "gua1", "near1", "gub1", "far1",
)
SHARE_A = (True, True)
SHARE_B = (True, False)


def decode_kernel(
    dims,
    hid_ref, freq_ref, an_ref, mn_ref, pos_ref, kc_ref, vc_ref,
    wq_ref, wk_ref, wv_ref, wo_ref, wg_ref, wu_ref, wd_ref,
    hid_out, knew_ref, vnew_ref, first_r, first_l, next_r, next_l, own_out,
    cos_buf, sin_buf, act_buf, an_buf, mn_buf, freq_buf, pos_in, know, vnow, gsrc, gbuf, pos_rows, abuf_w, bbuf_w, gu_w, wd_w, tr_w, y_all, m_buf, part, r_t, r_f,
    kbuf, vbuf, qbuf, abuf, hbuf,
    send_sem, recv_sem, loc_sem, kv_sem, out_sem, in_sem,
):
    layers, rows, width, heads, head_dim, cache_len, n_dev, ff = dims
    half = head_dim // 2
    piece = width // n_dev
    chip_cols = ff // CHIPS
    win = gu_w.shape[-1]
    pad = win - chip_cols
    wd_rows = wd_ref.shape[1]
    wo_rows = wo_ref.shape[1]
    q_half = wq_ref.shape[-1] // 2
    kv_half = half
    a_cols = abuf_w.shape[-1]
    groups = rows // SEQ_GROUP
    w = lax.axis_index("w")
    dp = lax.axis_index("dp")
    x, c = lax.div(w, CORES), lax.rem(w, CORES)
    h = lax.rem(dp, 2)
    xr, xo, xl = lax.rem(x + 1, CHIPS), lax.rem(x + 2, CHIPS), lax.rem(x + 3, CHIPS)
    cc = 1 - c
    hh = 1 - h
    right, left = (dp, xr * CORES + c), (dp, xl * CORES + c)
    twin = (dp, x * CORES + cc)
    pair = (dp + 1 - 2 * h, w)
    b_half, b_quarter = wo_rows // 2, wo_rows // 4
    b_mine = pl.multiple_of(h * b_half, b_quarter)
    b_mid = pl.multiple_of(h * b_half + b_quarter, b_quarter)
    b_other = pl.multiple_of(hh * b_half, b_quarter)
    b_last = pl.multiple_of(hh * b_half + b_quarter, b_quarter)
    q_mine = pl.multiple_of(h * q_half, LANES)
    kv_mine = pl.multiple_of(h * kv_half, LANES)
    starts = [pl.multiple_of(lax.div(chip_cols * xx, LANES) * LANES, LANES) for xx in (x, xr, xo, xl)]
    x_start, xr_start, xo_start, xl_start = starts
    xr_mid, xo_mid, xl_mid = [pl.multiple_of(xx + win // 2, LANES) for xx in starts[1:]]
    shift = lax.rem(chip_cols * x, LANES)
    wd_mine = pl.ds(pl.multiple_of(shift + wd_rows * c, 32), wd_rows)
    wd_twin = pl.ds(pl.multiple_of(shift + wd_rows * cc, 32), wd_rows)

    msg_ids = {}
    pending = {}

    def copy_of(name, src, dst, dev):
        i = msg_ids.setdefault(name, len(msg_ids))
        return pltpu.make_async_remote_copy(src, dst, send_sem.at[i], recv_sem.at[i], device_id=dev, device_id_type=MESH)

    def send(name, pairs, dev, view=None):
        for src, dst in pairs:
            copy_of(name, src, dst, dev).start()
        pending[name] = pairs[0][0] if view is None else view

    arrived = set()

    def got(name, view):
        if name not in arrived:
            arrived.add(name)
            copy_of(name, view, view, right).wait_recv()

    def drain(names):
        for name in names:
            view = pending.pop(name)
            copy_of(name, view, view, right).wait_send()

    def local_start(sem, pairs):
        for src, dst in pairs:
            pltpu.make_async_copy(src, dst, loc_sem.at[sem]).start()

    def local_wait(sem, view):
        if sem not in arrived:
            arrived.add(sem)
            pltpu.make_async_copy(view, view, loc_sem.at[sem]).wait()

    def kv_copies(i, slot):
        layer, group = lax.div(i, groups), lax.rem(i, groups)
        seqs = pl.ds(group * SEQ_GROUP, SEQ_GROUP)
        return (
            pltpu.make_async_copy(kc_ref.at[layer, seqs, 0], kbuf.at[slot], kv_sem.at[slot, 0]),
            pltpu.make_async_copy(vc_ref.at[layer, seqs, 0], vbuf.at[slot], kv_sem.at[slot, 1]),
        )

    def kv_start(i, slot):
        for copy in kv_copies(i, slot):
            copy.start()

    def a_pairs(l, hf, q_lo, kv_lo):
        dst = abuf_w.at[l, hf, x, c]
        return [
            (wq_ref.at[l, :, pl.ds(q_lo, q_half)], dst.at[:, pl.ds(0, q_half)]),
            (wk_ref.at[l, :, pl.ds(kv_lo, kv_half)], dst.at[:, pl.ds(q_half, kv_half)]),
            (wv_ref.at[l, :, pl.ds(kv_lo, kv_half)], dst.at[:, pl.ds(q_half + kv_half, kv_half)]),
        ]

    def a_both(l):
        return a_pairs(l, 0, 0, 0) + a_pairs(l, 1, q_half, kv_half)

    def a_block(l, xx):
        return abuf_w.at[l, h, xx, c] if SHARE_A[l] else abuf_w.at[l, :, xx, c]

    def a_lead(l, xx):
        return abuf_w.at[l, h, xx, c, :, pl.ds(0, a_cols // 2)] if SHARE_A[l] else abuf_w.at[l, 0, xx, c]

    def a_tail(l, xx):
        return abuf_w.at[l, h, xx, c, :, pl.ds(a_cols // 2, a_cols // 2)] if SHARE_A[l] else abuf_w.at[l, 1, xx, c]

    def ao(l):
        pairs = a_pairs(l, h, q_mine, kv_mine) if SHARE_A[l] else a_both(l)
        send(f"aR{l}", pairs, right, a_block(l, x))
        send(f"aL{l}", pairs, left, a_block(l, x))

    def to_pair(name, view):
        send(name, [(view, view)], pair)

    def a_near(l):
        got(f"aR{l}", a_block(l, xl))
        got(f"aL{l}", a_block(l, xr))

    def a_far(l):
        got(f"afR{l}", a_lead(l, xo))
        got(f"afL{l}", a_tail(l, xo))

    def af(l):
        a_near(l)
        send(f"afR{l}", [(a_lead(l, xl), a_lead(l, xl))], right)
        send(f"afL{l}", [(a_tail(l, xr), a_tail(l, xr))], left)

    def ap(l):
        a_near(l)
        to_pair(f"paR{l}", a_block(l, xl))
        to_pair(f"paL{l}", a_block(l, xr))

    def ax(l):
        a_far(l)
        if SHARE_A[l]:
            to_pair(f"paF{l}", a_block(l, xo))

    def at(l):
        a_near(l)
        a_far(l)
        local_wait(4 * l, abuf_w.at[l, :, x, c])
        view = abuf_w.at[l, h, :, c] if SHARE_A[l] else abuf_w.at[l, :, :, c]
        send(f"aT{l}", [(view, view)], twin)

    def aw(l):
        for name, xx in (("paR", xl), ("paL", xr), ("paF", xo)):
            got(f"{name}{l}", abuf_w.at[l, hh, xx, c])
        local_wait(4 * l, abuf_w.at[l, :, x, c])
        view = abuf_w.at[l, hh, :, c]
        send(f"aT1{l}", [(view, view)], twin)

    def a_ready(l):
        if SHARE_A[l]:
            got(f"aT{l}", abuf_w.at[l, h, :, cc])
            got(f"aT1{l}", abuf_w.at[l, hh, :, cc])
        else:
            got(f"aT{l}", abuf_w.at[l, :, :, cc])

    def b_block(l, xx):
        return bbuf_w.at[l, xx, c, pl.ds(b_mine, b_half)] if SHARE_B[l] else bbuf_w.at[l, xx, c]

    def b_lead(l, xx):
        return bbuf_w.at[l, xx, c, pl.ds(b_mine, b_quarter)] if SHARE_B[l] else bbuf_w.at[l, xx, c, pl.ds(0, b_half)]

    def b_tail(l, xx):
        return bbuf_w.at[l, xx, c, pl.ds(b_mid, b_quarter)] if SHARE_B[l] else bbuf_w.at[l, xx, c, pl.ds(b_half, b_half)]

    def bo(l):
        if not SHARE_B[l]:
            send(f"bR{l}", [(wo_ref.at[l], b_block(l, x))], right)
            send(f"bL{l}", [(wo_ref.at[l], b_block(l, x))], left)
            return
        for name, start, view in (("b", b_mine, b_lead(l, x)), ("bb", b_mid, b_tail(l, x))):
            src = wo_ref.at[l, pl.ds(start, b_quarter)]
            send(f"{name}R{l}", [(src, view)], right)
            send(f"{name}L{l}", [(src, view)], left)

    def b_near_lead(l):
        got(f"bR{l}", b_lead(l, xl))
        got(f"bL{l}", b_lead(l, xr))

    def b_near_tail(l):
        got(f"bbR{l}", b_tail(l, xl))
        got(f"bbL{l}", b_tail(l, xr))

    def b_near(l):
        if SHARE_B[l]:
            b_near_lead(l)
            b_near_tail(l)
        else:
            got(f"bR{l}", b_block(l, xl))
            got(f"bL{l}", b_block(l, xr))

    def b_far(l):
        got(f"bfR{l}", b_lead(l, xo))
        got(f"bfL{l}", b_tail(l, xo))

    def bf(l):
        b_near(l)
        send(f"bfR{l}", [(b_lead(l, xl), b_lead(l, xl))], right)
        send(f"bfL{l}", [(b_tail(l, xr), b_tail(l, xr))], left)

    def bp(l):
        b_near_lead(l)
        to_pair(f"pbR{l}", b_lead(l, xl))
        to_pair(f"pbL{l}", b_lead(l, xr))

    def bq(l):
        b_near_tail(l)
        to_pair(f"pbbR{l}", b_tail(l, xl))
        to_pair(f"pbbL{l}", b_tail(l, xr))

    def bx(l):
        b_far(l)
        if SHARE_B[l]:
            to_pair(f"pbF{l}", b_block(l, xo))

    def bt(l):
        b_near(l)
        b_far(l)
        local_wait(4 * l + 1, bbuf_w.at[l, x, c])
        view = bbuf_w.at[l, :, c, pl.ds(b_mine, b_half)] if SHARE_B[l] else bbuf_w.at[l, :, c]
        send(f"bT{l}", [(view, view)], twin)

    def bw(l):
        for name, xx in (("R", xl), ("L", xr)):
            got(f"pb{name}{l}", bbuf_w.at[l, xx, c, pl.ds(b_other, b_quarter)])
            got(f"pbb{name}{l}", bbuf_w.at[l, xx, c, pl.ds(b_last, b_quarter)])
        got(f"pbF{l}", bbuf_w.at[l, xo, c, pl.ds(b_other, b_half)])
        local_wait(4 * l + 1, bbuf_w.at[l, x, c])
        view = bbuf_w.at[l, :, c, pl.ds(b_other, b_half)]
        send(f"bT1{l}", [(view, view)], twin)

    def b_ready(l):
        if SHARE_B[l]:
            got(f"bT{l}", bbuf_w.at[l, :, cc, pl.ds(b_mine, b_half)])
            got(f"bT1{l}", bbuf_w.at[l, :, cc, pl.ds(b_other, b_half)])
        else:
            got(f"bT{l}", bbuf_w.at[l, :, cc])

    def by_matrix(l, name, lo, size, dst, dev):
        for value, ref in ((0, wg_ref), (1, wu_ref)):
            @pl.when(h == value)
            def _():
                copy_of(name, ref.at[l, :, pl.ds(lo, size)], dst, dev).start()
        pending[name] = dst

    fore, aft = pl.ds(0, win // 2), pl.ds(win // 2, win // 2)

    def cd(l):
        by_matrix(l, f"cR{l}", xr_start, win // 2, gu_w.at[l, h, x, c, :, fore], right)
        by_matrix(l, f"cL{l}", xl_start, win // 2, gu_w.at[l, h, x, c, :, fore], left)

    def ce(l):
        by_matrix(l, f"dR{l}", xr_mid, win // 2, gu_w.at[l, h, x, c, :, aft], right)
        by_matrix(l, f"dL{l}", xl_mid, win // 2, gu_w.at[l, h, x, c, :, aft], left)

    def ct(l):
        by_matrix(l, f"tR{l}", xo_start, win // 2, tr_w.at[l, 0], right)
        by_matrix(l, f"tL{l}", xo_mid, win // 2, tr_w.at[l, 1], left)

    def cf(l):
        got(f"tR{l}", tr_w.at[l, 0])
        send(f"cfR{l}", [(tr_w.at[l, 0], gu_w.at[l, h, xl, c, :, fore])], right)
        got(f"tL{l}", tr_w.at[l, 1])
        send(f"cfL{l}", [(tr_w.at[l, 1], gu_w.at[l, h, xr, c, :, aft])], left)

    def c_near(l, part_name, cols):
        got(f"{part_name}R{l}", gu_w.at[l, h, xl, c, :, cols])
        got(f"{part_name}L{l}", gu_w.at[l, h, xr, c, :, cols])

    def c_far(l):
        got(f"cfR{l}", gu_w.at[l, h, xo, c, :, fore])
        got(f"cfL{l}", gu_w.at[l, h, xo, c, :, aft])

    def cn(l):
        c_near(l, "c", fore)
        to_pair(f"pcR{l}", gu_w.at[l, h, xl, c, :, fore])
        to_pair(f"pcL{l}", gu_w.at[l, h, xr, c, :, fore])

    def cm(l):
        c_near(l, "d", aft)
        to_pair(f"pdR{l}", gu_w.at[l, h, xl, c, :, aft])
        to_pair(f"pdL{l}", gu_w.at[l, h, xr, c, :, aft])

    def cx(l):
        c_far(l)
        to_pair(f"pcF{l}", gu_w.at[l, h, xo, c])

    def cu(l):
        c_near(l, "c", fore)
        c_near(l, "d", aft)
        c_far(l)
        local_wait(4 * l + 2, gu_w.at[l, :, x, c])
        view = gu_w.at[l, h, :, c]
        send(f"cT{l}", [(view, view)], twin)

    def cw(l):
        for name, xx, cols in (("pcR", xl, fore), ("pcL", xr, fore), ("pdR", xl, aft), ("pdL", xr, aft)):
            got(f"{name}{l}", gu_w.at[l, hh, xx, c, :, cols])
        got(f"pcF{l}", gu_w.at[l, hh, xo, c])
        local_wait(4 * l + 2, gu_w.at[l, :, x, c])
        view = gu_w.at[l, hh, :, c]
        send(f"cT1{l}", [(view, view)], twin)

    def c_ready(l):
        got(f"cT{l}", gu_w.at[l, h, :, cc])
        got(f"cT1{l}", gu_w.at[l, hh, :, cc])

    def dt(l):
        send(f"dT{l}", [(wd_ref.at[l], wd_w.at[l, wd_mine])], twin)

    def d_ready(l):
        local_wait(4 * l + 3, wd_w.at[l, wd_mine])
        got(f"dT{l}", wd_w.at[l, wd_twin])

    small = [(an_ref, an_buf), (mn_ref, mn_buf), (freq_ref, freq_buf), (pos_ref, pos_in)]
    for i, (src, dst) in enumerate(small):
        pltpu.make_async_copy(src, dst, in_sem.at[i]).start()
    barrier = pltpu.get_barrier_semaphore()
    for i in range(1, n_dev):
        pl.semaphore_signal(barrier, inc=1, device_id=(dp, lax.rem(w + i, n_dev)), device_id_type=MESH)
    pl.semaphore_signal(barrier, inc=1, device_id=pair, device_id_type=MESH)
    pl.semaphore_wait(barrier, n_dev)

    def entry(_):
        hid_copy = pltpu.make_async_copy(hid_ref, hbuf, in_sem.at[len(small)])
        hid_copy.start()
        for i in range(KV_SLOTS):
            kv_start(i, i)
        for l in range(layers):
            local_start(4 * l, a_both(l))
            local_start(4 * l + 1, [(wo_ref.at[l], bbuf_w.at[l, x, c])])
            cols = pl.ds(x_start, win)
            local_start(4 * l + 2, [(wg_ref.at[l, :, cols], gu_w.at[l, 0, x, c]), (wu_ref.at[l, :, cols], gu_w.at[l, 1, x, c])])
            local_start(4 * l + 3, [(wd_ref.at[l], wd_w.at[l, wd_mine])])
        for i, (src, dst) in enumerate(small):
            pltpu.make_async_copy(src, dst, in_sem.at[i]).wait()
        gsrc[...] = jnp.zeros_like(gsrc)
        gsrc[0:layers, 0:piece] = an_buf[...]
        gsrc[layers:2 * layers, 0:piece] = mn_buf[...]
        own_gain = pltpu.roll(gsrc[...], lax.rem(w * piece, LANES), 1)
        gsrc[...] = own_gain
        gbuf[w] = own_gain
        for l in range(layers):
            start = pl.multiple_of(jnp.where(lax.rem(x, 2) == 0, chip_cols, 0), 64)
            wd_w[l, pl.ds(start, pad), :] = jnp.zeros((pad, width), BF16)
        pos_rows[...] = jnp.broadcast_to(pos_in[...].astype(F32), (rows, rows)).T
        angles = pos_rows[...] * freq_buf[...]
        cos_buf[...] = jnp.cos(angles)
        sin_buf[...] = jnp.sin(angles)
        for i in range(1, n_dev):
            copy_of("gain", gsrc, gbuf.at[w], (dp, lax.rem(w + i, n_dev))).start()
        pending["gain"] = gbuf.at[pl.ds(0, n_dev - 1)]
        hid_copy.wait()

    def all_gains():
        tiles = []
        for j in range(width // LANES):
            total = None
            for s in range(n_dev):
                lo = (s * piece) // LANES
                for k in range(2):
                    if lo + k == j:
                        block = gbuf[s, :, k * LANES:(k + 1) * LANES]
                        total = block if total is None else total + block
            tiles.append(total)
        return 1.0 + jnp.concatenate(tiles, axis=1)

    def rms(hid, row):
        mean_sq = jnp.sum(hid * hid, axis=-1, keepdims=True) / width
        return (hid * lax.rsqrt(mean_sq + EPS) * all_gains()[row:row + 1, :]).astype(BF16)

    chunk = 4

    def attend(l, group):
        row_seq = lax.rem(lax.broadcasted_iota(jnp.int32, (LANES, cache_len), 0), SEQ_GROUP)
        place = lax.broadcasted_iota(jnp.int32, (LANES, cache_len), 1).astype(F32)
        i = l * groups + group
        slot = lax.rem(i, KV_SLOTS)
        for copy in kv_copies(i, slot):
            copy.wait()
        seqs = pl.ds(pl.multiple_of(group * SEQ_GROUP, SEQ_GROUP), SEQ_GROUP)
        query = jnp.concatenate([qbuf[j, seqs, :] for j in range(heads)], axis=0)
        scores = jnp.zeros((LANES, cache_len), F32)
        for b in range(0, SEQ_GROUP, chunk):
            prod = dot_t(query, kbuf[slot, b:b + chunk].reshape(chunk * cache_len, head_dim))
            for j in range(chunk):
                scores = jnp.where(row_seq == b + j, prod[:, j * cache_len:(j + 1) * cache_len], scores)
        k_rep = jnp.concatenate([know[l, seqs, :]] * heads, axis=0)
        v_rep = jnp.concatenate([vnow[l, seqs, :]] * heads, axis=0)
        new_score = jnp.sum(query.astype(F32) * k_rep, axis=1, keepdims=True)
        pos = jnp.concatenate([pos_rows[seqs, :]] * heads, axis=0)
        scores = jnp.where(place < pos, scores, -1e30)
        top = jnp.maximum(jnp.max(scores, axis=1, keepdims=True), new_score)
        prob = jnp.exp(scores - top)
        prob_new = jnp.exp(new_score - top)
        total = jnp.sum(prob, axis=1, keepdims=True) + prob_new
        acc = prob_new.astype(BF16).astype(F32) * v_rep
        for b in range(0, SEQ_GROUP, chunk):
            spread = jnp.concatenate([jnp.where(row_seq == b + j, prob, 0.0).astype(BF16) for j in range(chunk)], axis=1)
            acc = acc + dot(spread, vbuf[slot, b:b + chunk].reshape(chunk * cache_len, head_dim))
        attn = (acc / total).astype(BF16)
        for j in range(heads):
            abuf[seqs, j * head_dim:(j + 1) * head_dim] = attn[j * SEQ_GROUP:(j + 1) * SEQ_GROUP, :]

        @pl.when(i + KV_SLOTS < layers * groups)
        def _():
            kv_start(i + KV_SLOTS, slot)

    last = layers - 1
    exports = []

    def export(src, dst):
        pltpu.make_async_copy(src, dst, out_sem.at[len(exports)]).start()
        exports.append((src, dst))

    def qkv(l):
        a_ready(l)
        if l == 0:
            got("gain", gbuf.at[pl.ds(0, n_dev - 1)])
        cos_tab, sin_tab = cos_buf[...], sin_buf[...]
        normed = rms(hbuf[...].astype(F32), l)
        halves = [dot(normed, abuf_w[l, hf].reshape(width, a_cols)) for hf in range(2)]

        def rope(lead, tail):
            return jnp.concatenate([lead * cos_tab - tail * sin_tab, tail * cos_tab + lead * sin_tab], axis=1)

        for j in range(heads):
            out, lo = halves[j // (heads // 2)], (j % (heads // 2)) * head_dim
            qbuf[j] = (rope(out[:, lo:lo + half], out[:, lo + half:lo + head_dim]) * head_dim ** -0.5).astype(BF16)
        know[l] = rope(halves[0][:, q_half:q_half + half], halves[1][:, q_half:q_half + half]).astype(BF16).astype(F32)
        vnow[l] = jnp.concatenate([hv[:, q_half + half:q_half + 2 * half] for hv in halves], axis=1).astype(BF16).astype(F32)
        export(know.at[l], knew_ref.at[l])
        export(vnow.at[l], vnew_ref.at[l])

    r2 = rows // 2
    upper, lower = pl.ds(0, r2), pl.ds(r2, r2)

    def mix(l):
        b_ready(l)
        mixed = dot(abuf[...], bbuf_w[l].reshape(heads * head_dim, width))
        hid_mid = (hbuf[...].astype(F32) + mixed).astype(BF16)
        hbuf[...] = hid_mid
        y_all[l, x] = rms(hid_mid.astype(F32), layers + l)
        top, bottom = y_all.at[l, x, upper], y_all.at[l, x, lower]
        send(f"yR1{l}", [(top, top)], right)
        send(f"yL1{l}", [(bottom, bottom)], left)
        send(f"yR2{l}", [(bottom, bottom)], right)
        send(f"yL2{l}", [(top, top)], left)

    def yf(l):
        view = y_all.at[l, xl, upper]
        got(f"yR1{l}", view)
        send(f"yfR{l}", [(view, view)], right)
        view = y_all.at[l, xr, lower]
        got(f"yL1{l}", view)
        send(f"yfL{l}", [(view, view)], left)

    n_tile = 2 * LANES

    def gate_up(l, blocks):
        span = slice(0, len(blocks) * rows)

        def at_tile(n):
            return pl.ds(pl.multiple_of(n * n_tile, n_tile), n_tile)

        def multiply(n, slot):
            act = jnp.concatenate([y_all[l, b] for b in blocks], axis=0)
            for k in range(2):
                act_buf[slot, k, span] = dot(act, gu_w[l, k, :, :, :, at_tile(n)].reshape(width, n_tile))

        def activate(n, slot):
            mid = (jax.nn.gelu(act_buf[slot, 0, span], approximate=True) * act_buf[slot, 1, span]).astype(BF16)
            for k, b in enumerate(blocks):
                m_buf[b, :, at_tile(n)] = mid[k * rows:(k + 1) * rows]

        tiles = win // n_tile
        assert tiles % 2 == 1
        multiply(0, 0)

        @pl.loop(0, tiles // 2)
        def _(k):
            multiply(2 * k + 1, 1)
            activate(2 * k, 0)
            multiply(2 * k + 2, 0)
            activate(2 * k + 1, 1)

        activate(tiles - 1, 0)

    def guo(l):
        if l:
            c_ready(l)
        gate_up(l, (x,))

    def gua(l):
        got(f"yR2{l}", y_all.at[l, xl, lower])
        got(f"yL2{l}", y_all.at[l, xr, upper])
        if not l:
            c_ready(l)
        gate_up(l, (xl, xr))

    def gub(l):
        got(f"yfR{l}", y_all.at[l, xo, upper])
        got(f"yfL{l}", y_all.at[l, xo, lower])
        gate_up(l, (xo,))

    def down(l, xx):
        part[xx] = dot(m_buf[xx], wd_w[l])

    def near(l):
        if l:
            drain([f"{name}{l - 1}" for name in ("eR2", "eL2", "eR3", "eL3")])
        both = dot(jnp.concatenate([m_buf[xr], m_buf[xl]], axis=0), wd_w[l])
        part[xr] = both[:rows]
        part[xl] = both[rows:]
        if l == last:
            export(part.at[xr, lower], first_r.at[lower])
            export(part.at[xl, upper], first_l.at[upper])
            export(part.at[xr, upper], next_r)
            export(part.at[xl, lower], next_l)
        else:
            send(f"eR2{l}", [(part.at[xr, lower], r_f.at[l, 0, lower])], right)
            send(f"eL2{l}", [(part.at[xl, upper], r_f.at[l, 1, upper])], left)

    def far(l):
        if l:
            drain([f"{name}{l - 1}" for name in ("eR1", "eL1")])
        down(l, xo)
        if l == last:
            export(part.at[xo, upper], first_r.at[upper])
            export(part.at[xo, lower], first_l.at[lower])
        else:
            send(f"eR1{l}", [(part.at[xo, upper], r_t.at[l, 0])], right)
            send(f"eL1{l}", [(part.at[xo, lower], r_t.at[l, 1])], left)

    def er(l):
        got(f"eR1{l}", r_t.at[l, 0])
        part[xr, 0:r2] = part[xr, 0:r2] + r_t[l, 0]
        send(f"eR3{l}", [(part.at[xr, upper], r_f.at[l, 0, upper])], right)
        got(f"eL1{l}", r_t.at[l, 1])
        part[xl, r2:rows] = part[xl, r2:rows] + r_t[l, 1]
        send(f"eL3{l}", [(part.at[xl, lower], r_f.at[l, 1, lower])], left)

    def own(l):
        down(l, x)
        if l == last:
            export(part.at[x], own_out)
            export(hbuf, hid_out)

    def done(l):
        got(f"eR2{l}", r_f.at[l, 0, lower])
        got(f"eL2{l}", r_f.at[l, 1, upper])
        got(f"eR3{l}", r_f.at[l, 0, upper])
        got(f"eL3{l}", r_f.at[l, 1, lower])
        hbuf[...] = (hbuf[...].astype(F32) + (part[x] + r_f[l, 0] + r_f[l, 1])).astype(BF16)

    table = dict(
        ao=ao, af=af, ap=ap, ax=ax, at=at, aw=aw, bo=bo, bf=bf, bp=bp, bq=bq, bx=bx, bt=bt, bw=bw, cd=cd, ce=ce, ct=ct, cf=cf,
        cn=cn, cm=cm, cx=cx, cu=cu, cw=cw, dt=dt, **{"in": entry},
        qkv=qkv, mix=mix, yf=yf, guo=guo, gua=gua, gub=gub, dr=d_ready, near=near, far=far, er=er, own=own, done=done,
    )

    def run(step):
        table[step[:-1]](int(step[-1]))

    here = 0
    reached = [0] * layers
    while here < len(ORDER):
        step = ORDER[here]
        if not step.startswith("att"):
            run(step)
            here += 1
            continue
        l, count = int(step[-1]), 0
        while ORDER[here] == step:
            count += 1
            here += 1
        first = reached[l]
        reached[l] += count

        @pl.loop(first, first + count)
        def _(group):
            attend(l, group)

    drain(list(pending))
    for i, (src, dst) in enumerate(exports):
        pltpu.make_async_copy(src, dst, out_sem.at[i]).wait()
    assert len(msg_ids) <= send_sem.shape[0]


def decode(hidden, positions, k_cache, v_cache, attn_norm, w_query, w_key, w_value, w_out, mlp_norm, w_gate, w_up, w_down):
    layers, rows, _, cache_len, head_dim = k_cache.shape
    width = hidden.shape[1]
    n_dev = lax.axis_size("w")
    ff = w_gate.shape[-1]
    heads = w_query.shape[-1] // head_dim
    chip_cols = ff // CHIPS
    win = -(-(chip_cols + LANES // 2) // LANES) * LANES
    piece = width // n_dev
    groups = rows // SEQ_GROUP
    assert n_dev == CHIPS * CORES and heads * SEQ_GROUP == LANES and cache_len == LANES and rows == LANES
    assert lax.axis_size("dp") % 2 == 0
    inv_freq = np.float32(ROPE_BASE) ** (np.float32(-2.0) * np.arange(head_dim // 2, dtype=np.float32) / np.float32(head_dim))
    dims = (layers, rows, width, heads, head_dim, cache_len, n_dev, ff)
    anym = pl.BlockSpec(memory_space=pl.ANY)
    new_shape = jax.ShapeDtypeStruct((layers, rows, head_dim), F32)
    whole_sum = jax.ShapeDtypeStruct(hidden.shape, F32)
    half_sum = jax.ShapeDtypeStruct((rows // 2, width), F32)
    n_msg = 96
    return pl.pallas_call(
        functools.partial(decode_kernel, dims),
        out_shape=(jax.ShapeDtypeStruct(hidden.shape, BF16), new_shape, new_shape) + (whole_sum, whole_sum, half_sum, half_sum, whole_sum),
        in_specs=[anym] * 14,
        out_specs=(anym,) * 8,
        scratch_shapes=[
            pltpu.VMEM((rows, head_dim // 2), F32),
            pltpu.VMEM((rows, head_dim // 2), F32),
            pltpu.VMEM((2, 2, 2 * rows, 2 * LANES), F32),
            pltpu.VMEM(attn_norm.shape, F32),
            pltpu.VMEM(mlp_norm.shape, F32),
            pltpu.VMEM((1, head_dim // 2), F32),
            pltpu.VMEM((1, rows), jnp.int32),
            pltpu.VMEM((layers, rows, head_dim), F32),
            pltpu.VMEM((layers, rows, head_dim), F32),
            pltpu.VMEM((8, 2 * LANES), F32),
            pltpu.VMEM((n_dev, 8, 2 * LANES), F32),
            pltpu.VMEM((rows, LANES), F32),
            pltpu.VMEM((layers, 2, CHIPS, CORES, piece, w_query.shape[-1] // 2 + head_dim), BF16),
            pltpu.VMEM((layers, CHIPS, CORES, w_out.shape[1], width), BF16),
            pltpu.VMEM((layers, 2, CHIPS, CORES, piece, win), BF16),
            pltpu.VMEM((layers, win, width), BF16),
            pltpu.VMEM((layers, 2, piece, win // 2), BF16),
            pltpu.VMEM((layers, CHIPS, rows, width), BF16),
            pltpu.VMEM((CHIPS, rows, win), BF16),
            pltpu.VMEM((CHIPS, rows, width), F32),
            pltpu.VMEM((layers - 1, 2, rows // 2, width), F32),
            pltpu.VMEM((layers - 1, 2, rows, width), F32),
            pltpu.VMEM((KV_SLOTS, SEQ_GROUP, cache_len, head_dim), BF16),
            pltpu.VMEM((KV_SLOTS, SEQ_GROUP, cache_len, head_dim), BF16),
            pltpu.VMEM((heads, rows, head_dim), BF16),
            pltpu.VMEM((rows, heads * head_dim), BF16),
            pltpu.VMEM((rows, width), BF16),
            pltpu.SemaphoreType.DMA((n_msg,)),
            pltpu.SemaphoreType.DMA((n_msg,)),
            pltpu.SemaphoreType.DMA((4 * layers,)),
            pltpu.SemaphoreType.DMA((KV_SLOTS, 2)),
            pltpu.SemaphoreType.DMA((16,)),
            pltpu.SemaphoreType.DMA((8,)),
        ],
        compiler_params=pltpu.CompilerParams(collective_id=0, has_side_effects=True, vmem_limit_bytes=67043328),
        name="decode",
    )(hidden, jnp.asarray(inv_freq).reshape(1, head_dim // 2), attn_norm, mlp_norm, positions.reshape(1, rows), k_cache, v_cache, w_query, w_key, w_value, w_out, w_gate, w_up, w_down)


TILE_ROWS = 16
CACHE_BLOCK = 16


def cache_kernel(pos_ref, old_ref, new_ref, out_ref, buf, in_sem, out_sem):
    layers, rows = old_ref.shape[:2]
    blocks = rows // CACHE_BLOCK
    def load(l, b):
        i = l * blocks + b
        return pltpu.make_async_copy(old_ref.at[l, pl.ds(b * CACHE_BLOCK, CACHE_BLOCK), 0], buf.at[i], in_sem.at[i])

    def store(l, b):
        i = l * blocks + b
        return pltpu.make_async_copy(buf.at[i], out_ref.at[l, pl.ds(b * CACHE_BLOCK, CACHE_BLOCK), 0], out_sem.at[i])

    steps = [(l, b) for l in range(layers) for b in range(blocks)]
    for l, b in steps:
        load(l, b).start()
    row = lax.broadcasted_iota(jnp.int32, (TILE_ROWS, buf.shape[-1]), 0)
    for l in range(layers):
        @pl.loop(0, blocks)
        def _(b):
            load(l, b).wait()
            fresh = new_ref[l, pl.ds(pl.multiple_of(b * CACHE_BLOCK, CACHE_BLOCK), CACHE_BLOCK), :]
            tiles = []
            for s in range(CACHE_BLOCK):
                pos = pos_ref[b * CACHE_BLOCK + s]
                base = pl.multiple_of(pos // TILE_ROWS * TILE_ROWS, TILE_ROWS)
                tile = buf[l * blocks + b, s, pl.ds(base, TILE_ROWS), :].astype(F32)
                tiles.append((s, base, jnp.where(row == pos - base, fresh[s:s + 1, :], tile).astype(BF16)))
            for s, base, tile in tiles:
                buf[l * blocks + b, s, pl.ds(base, TILE_ROWS), :] = tile
    for l, b in steps:
        store(l, b).start()
    for l, b in steps:
        store(l, b).wait()


def write_cache(positions, cache, new_rows):
    cache_len, head_dim = cache.shape[-2:]
    slots = cache.shape[0] * cache.shape[1] // CACHE_BLOCK
    vmem, anym = pl.BlockSpec(memory_space=pltpu.VMEM), pl.BlockSpec(memory_space=pl.ANY)
    return pl.pallas_call(
        cache_kernel,
        out_shape=jax.ShapeDtypeStruct(cache.shape, BF16),
        in_specs=[pl.BlockSpec(memory_space=pltpu.SMEM), anym, vmem],
        out_specs=anym,
        scratch_shapes=[
            pltpu.VMEM((slots, CACHE_BLOCK, cache_len, head_dim), BF16),
            pltpu.SemaphoreType.DMA((slots,)),
            pltpu.SemaphoreType.DMA((slots,)),
        ],
        cost_estimate=pl.CostEstimate(flops=10**11, bytes_accessed=4 * cache.size, transcendentals=0),
        compiler_params=pltpu.CompilerParams(vmem_limit_bytes=60 * 2**20),
        name="cache",
    )(positions, cache, new_rows)


def solution(mesh):
    batch_spec = P(("dp", "w"))
    cache_spec = P(None, ("dp", "w"))
    gain_spec = P(None, "w")
    weight_spec = P(None, "w", None)

    def per_device(hidden, positions, k_cache, v_cache, *weights):
        hid_mid, k_new, v_new, first_r, first_l, next_r, next_l, own = decode(hidden, positions, k_cache, v_cache, *weights)
        n_dev, half = mesh.shape["w"], hidden.shape[0] // 2
        ahead = [(i, (i + CORES) % n_dev) for i in range(n_dev)]
        back = [(i, (i - CORES) % n_dev) for i in range(n_dev)]
        got_r = lax.ppermute(first_r, "w", ahead)
        got_l = lax.ppermute(first_l, "w", back)
        k_out = write_cache(positions, k_cache, k_new)
        upper = lax.ppermute(next_r + got_r[:half], "w", ahead)
        lower = lax.ppermute(next_l + got_l[half:], "w", back)
        v_out = write_cache(positions, v_cache, v_new)
        is_upper = lax.broadcasted_iota(jnp.int32, own.shape, 0) < half
        total = own + jnp.where(is_upper, got_l, got_r) + jnp.concatenate([upper, lower], axis=0)
        hidden_out = (hid_mid.astype(F32) + total).astype(BF16)
        return hidden_out, k_out, v_out

    in_specs = (batch_spec, batch_spec, cache_spec, cache_spec, gain_spec, weight_spec, weight_spec, weight_spec, weight_spec, gain_spec, weight_spec, weight_spec, weight_spec)
    out_specs = (batch_spec, cache_spec, cache_spec)
    return jax.shard_map(per_device, mesh=mesh, in_specs=in_specs, out_specs=out_specs, check_vma=False)
```

```python
import functools

import jax
import jax.numpy as jnp
import numpy as np
from jax import lax
from jax.experimental import pallas as pl
from jax.experimental.pallas import tpu as pltpu
from jax.sharding import PartitionSpec as P

EPS = 1e-6
ROPE_BASE = 10000.0
LANES = 128
CORES = 2
CHIPS = 4
SEQ_GROUP = 32
KV_SLOTS = 3
MESH = pl.DeviceIdType.MESH
F32 = jnp.float32
BF16 = jnp.bfloat16


def dot(a, b):
    return jnp.dot(a, b, preferred_element_type=F32)


def dot_t(a, b):
    return lax.dot_general(a, b, (((1,), (1,)), ((), ())), preferred_element_type=F32)


ORDER = (
    "bo0", "ao0", "in0", "bp0", "bq0", "bf0", "ct0", "ap0", "af0", "cd0", "ce0", "cf0", "ax0", "cd1", "bx0", "at0",
    "ao1", "cn0", "aw0", "ce1", "bw0", "bt0", "qkv0", "att0", "ct1", "cx0", "att0", "att0", "af1", "att0", "cm0", "mix0",
    "cu0", "cv0", "ax1", "ap1", "yf0", "bo1", "dt0", "cw0", "cf1", "at1", "cm1", "gua0", "dr0", "near0", "gub0", "dt1",
    "cx1", "far0", "cn1", "er0", "guo0", "bf1", "own0", "aw1", "cu1", "done0", "qkv1", "att1", "att1", "bx1", "bt1", "cv1",
    "att1", "att1", "mix1", "cw1", "yf1", "guo1", "dr1", "own1", "gua1", "near1", "gub1", "far1",
)
SHARE_A = (True, True)
SHARE_B = (True, False)


def decode_kernel(
    dims,
    hid_ref, freq_ref, an_ref, mn_ref, pos_ref, kc_ref, vc_ref,
    wq_ref, wk_ref, wv_ref, wo_ref, wg_ref, wu_ref, wd_ref,
    hid_out, knew_ref, vnew_ref, first_r, first_l, next_r, next_l, own_out,
    cos_buf, sin_buf, act_buf, an_buf, mn_buf, freq_buf, pos_in, know, vnow, gsrc, gbuf, pos_rows, abuf_w, bbuf_w, gu_w, wd_w, tr_w, y_all, m_buf, part, r_t, r_f,
    kbuf, vbuf, qbuf, abuf, hbuf,
    send_sem, recv_sem, loc_sem, kv_sem, out_sem, in_sem,
):
    layers, rows, width, heads, head_dim, cache_len, n_dev, ff = dims
    half = head_dim // 2
    piece = width // n_dev
    chip_cols = ff // CHIPS
    win = gu_w.shape[-1]
    pad = win - chip_cols
    wd_rows = wd_ref.shape[1]
    wo_rows = wo_ref.shape[1]
    q_half = wq_ref.shape[-1] // 2
    kv_half = half
    a_cols = abuf_w.shape[-1]
    groups = rows // SEQ_GROUP
    w = lax.axis_index("w")
    dp = lax.axis_index("dp")
    x, c = lax.div(w, CORES), lax.rem(w, CORES)
    h = lax.rem(dp, 2)
    xr, xo, xl = lax.rem(x + 1, CHIPS), lax.rem(x + 2, CHIPS), lax.rem(x + 3, CHIPS)
    cc = 1 - c
    hh = 1 - h
    right, left = (dp, xr * CORES + c), (dp, xl * CORES + c)
    twin = (dp, x * CORES + cc)
    pair = (dp + 1 - 2 * h, w)
    b_half, b_quarter = wo_rows // 2, wo_rows // 4
    b_mine = pl.multiple_of(h * b_half, b_quarter)
    b_mid = pl.multiple_of(h * b_half + b_quarter, b_quarter)
    b_other = pl.multiple_of(hh * b_half, b_quarter)
    b_last = pl.multiple_of(hh * b_half + b_quarter, b_quarter)
    q_mine = pl.multiple_of(h * q_half, LANES)
    kv_mine = pl.multiple_of(h * kv_half, LANES)
    starts = [pl.multiple_of(lax.div(chip_cols * xx, LANES) * LANES, LANES) for xx in (x, xr, xo, xl)]
    x_start, xr_start, xo_start, xl_start = starts
    xr_mid, xo_mid, xl_mid = [pl.multiple_of(xx + win // 2, LANES) for xx in starts[1:]]
    shift = lax.rem(chip_cols * x, LANES)
    wd_mine = pl.ds(pl.multiple_of(shift + wd_rows * c, 32), wd_rows)
    wd_twin = pl.ds(pl.multiple_of(shift + wd_rows * cc, 32), wd_rows)

    msg_ids = {}
    pending = {}

    def copy_of(name, src, dst, dev):
        i = msg_ids.setdefault(name, len(msg_ids))
        return pltpu.make_async_remote_copy(src, dst, send_sem.at[i], recv_sem.at[i], device_id=dev, device_id_type=MESH)

    def send(name, pairs, dev, view=None):
        for src, dst in pairs:
            copy_of(name, src, dst, dev).start()
        pending[name] = pairs[0][0] if view is None else view

    arrived = set()

    def got(name, view):
        if name not in arrived:
            arrived.add(name)
            copy_of(name, view, view, right).wait_recv()

    def drain(names):
        for name in names:
            view = pending.pop(name)
            copy_of(name, view, view, right).wait_send()

    def local_start(sem, pairs):
        for src, dst in pairs:
            pltpu.make_async_copy(src, dst, loc_sem.at[sem]).start()

    def local_wait(sem, view):
        if sem not in arrived:
            arrived.add(sem)
            pltpu.make_async_copy(view, view, loc_sem.at[sem]).wait()

    def kv_copies(i, slot):
        layer, group = lax.div(i, groups), lax.rem(i, groups)
        seqs = pl.ds(group * SEQ_GROUP, SEQ_GROUP)
        return (
            pltpu.make_async_copy(kc_ref.at[layer, seqs, 0], kbuf.at[slot], kv_sem.at[slot, 0]),
            pltpu.make_async_copy(vc_ref.at[layer, seqs, 0], vbuf.at[slot], kv_sem.at[slot, 1]),
        )

    def kv_start(i, slot):
        for copy in kv_copies(i, slot):
            copy.start()

    def a_pairs(l, hf, q_lo, kv_lo):
        dst = abuf_w.at[l, hf, x, c]
        return [
            (wq_ref.at[l, :, pl.ds(q_lo, q_half)], dst.at[:, pl.ds(0, q_half)]),
            (wk_ref.at[l, :, pl.ds(kv_lo, kv_half)], dst.at[:, pl.ds(q_half, kv_half)]),
            (wv_ref.at[l, :, pl.ds(kv_lo, kv_half)], dst.at[:, pl.ds(q_half + kv_half, kv_half)]),
        ]

    def a_both(l):
        return a_pairs(l, 0, 0, 0) + a_pairs(l, 1, q_half, kv_half)

    def a_block(l, xx):
        return abuf_w.at[l, h, xx, c] if SHARE_A[l] else abuf_w.at[l, :, xx, c]

    def a_lead(l, xx):
        return abuf_w.at[l, h, xx, c, :, pl.ds(0, a_cols // 2)] if SHARE_A[l] else abuf_w.at[l, 0, xx, c]

    def a_tail(l, xx):
        return abuf_w.at[l, h, xx, c, :, pl.ds(a_cols // 2, a_cols // 2)] if SHARE_A[l] else abuf_w.at[l, 1, xx, c]

    def ao(l):
        pairs = a_pairs(l, h, q_mine, kv_mine) if SHARE_A[l] else a_both(l)
        send(f"aR{l}", pairs, right, a_block(l, x))
        send(f"aL{l}", pairs, left, a_block(l, x))

    def to_pair(name, view):
        send(name, [(view, view)], pair)

    def a_near(l):
        got(f"aR{l}", a_block(l, xl))
        got(f"aL{l}", a_block(l, xr))

    def a_far(l):
        got(f"afR{l}", a_lead(l, xo))
        got(f"afL{l}", a_tail(l, xo))

    def af(l):
        a_near(l)
        send(f"afR{l}", [(a_lead(l, xl), a_lead(l, xl))], right)
        send(f"afL{l}", [(a_tail(l, xr), a_tail(l, xr))], left)

    def ap(l):
        a_near(l)
        to_pair(f"paR{l}", a_block(l, xl))
        to_pair(f"paL{l}", a_block(l, xr))

    def ax(l):
        a_far(l)
        if SHARE_A[l]:
            to_pair(f"paF{l}", a_block(l, xo))

    def at(l):
        a_near(l)
        a_far(l)
        local_wait(4 * l, abuf_w.at[l, :, x, c])
        view = abuf_w.at[l, h, :, c] if SHARE_A[l] else abuf_w.at[l, :, :, c]
        send(f"aT{l}", [(view, view)], twin)

    def aw(l):
        for name, xx in (("paR", xl), ("paL", xr), ("paF", xo)):
            got(f"{name}{l}", abuf_w.at[l, hh, xx, c])
        local_wait(4 * l, abuf_w.at[l, :, x, c])
        view = abuf_w.at[l, hh, :, c]
        send(f"aT1{l}", [(view, view)], twin)

    def a_ready(l):
        if SHARE_A[l]:
            got(f"aT{l}", abuf_w.at[l, h, :, cc])
            got(f"aT1{l}", abuf_w.at[l, hh, :, cc])
        else:
            got(f"aT{l}", abuf_w.at[l, :, :, cc])

    def b_block(l, xx):
        return bbuf_w.at[l, xx, c, pl.ds(b_mine, b_half)] if SHARE_B[l] else bbuf_w.at[l, xx, c]

    def b_lead(l, xx):
        return bbuf_w.at[l, xx, c, pl.ds(b_mine, b_quarter)] if SHARE_B[l] else bbuf_w.at[l, xx, c, pl.ds(0, b_half)]

    def b_tail(l, xx):
        return bbuf_w.at[l, xx, c, pl.ds(b_mid, b_quarter)] if SHARE_B[l] else bbuf_w.at[l, xx, c, pl.ds(b_half, b_half)]

    def bo(l):
        if not SHARE_B[l]:
            send(f"bR{l}", [(wo_ref.at[l], b_block(l, x))], right)
            send(f"bL{l}", [(wo_ref.at[l], b_block(l, x))], left)
            return
        for name, start, view in (("b", b_mine, b_lead(l, x)), ("bb", b_mid, b_tail(l, x))):
            src = wo_ref.at[l, pl.ds(start, b_quarter)]
            send(f"{name}R{l}", [(src, view)], right)
            send(f"{name}L{l}", [(src, view)], left)

    def b_near_lead(l):
        got(f"bR{l}", b_lead(l, xl))
        got(f"bL{l}", b_lead(l, xr))

    def b_near_tail(l):
        got(f"bbR{l}", b_tail(l, xl))
        got(f"bbL{l}", b_tail(l, xr))

    def b_near(l):
        if SHARE_B[l]:
            b_near_lead(l)
            b_near_tail(l)
        else:
            got(f"bR{l}", b_block(l, xl))
            got(f"bL{l}", b_block(l, xr))

    def b_far(l):
        got(f"bfR{l}", b_lead(l, xo))
        got(f"bfL{l}", b_tail(l, xo))

    def bf(l):
        b_near(l)
        send(f"bfR{l}", [(b_lead(l, xl), b_lead(l, xl))], right)
        send(f"bfL{l}", [(b_tail(l, xr), b_tail(l, xr))], left)

    def bp(l):
        b_near_lead(l)
        to_pair(f"pbR{l}", b_lead(l, xl))
        to_pair(f"pbL{l}", b_lead(l, xr))

    def bq(l):
        b_near_tail(l)
        to_pair(f"pbbR{l}", b_tail(l, xl))
        to_pair(f"pbbL{l}", b_tail(l, xr))

    def bx(l):
        b_far(l)
        if SHARE_B[l]:
            to_pair(f"pbF{l}", b_block(l, xo))

    def bt(l):
        b_near(l)
        b_far(l)
        local_wait(4 * l + 1, bbuf_w.at[l, x, c])
        view = bbuf_w.at[l, :, c, pl.ds(b_mine, b_half)] if SHARE_B[l] else bbuf_w.at[l, :, c]
        send(f"bT{l}", [(view, view)], twin)

    def bw(l):
        for name, xx in (("R", xl), ("L", xr)):
            got(f"pb{name}{l}", bbuf_w.at[l, xx, c, pl.ds(b_other, b_quarter)])
            got(f"pbb{name}{l}", bbuf_w.at[l, xx, c, pl.ds(b_last, b_quarter)])
        got(f"pbF{l}", bbuf_w.at[l, xo, c, pl.ds(b_other, b_half)])
        local_wait(4 * l + 1, bbuf_w.at[l, x, c])
        view = bbuf_w.at[l, :, c, pl.ds(b_other, b_half)]
        send(f"bT1{l}", [(view, view)], twin)

    def b_ready(l):
        if SHARE_B[l]:
            got(f"bT{l}", bbuf_w.at[l, :, cc, pl.ds(b_mine, b_half)])
            got(f"bT1{l}", bbuf_w.at[l, :, cc, pl.ds(b_other, b_half)])
        else:
            got(f"bT{l}", bbuf_w.at[l, :, cc])

    def by_matrix(l, name, lo, size, dst, dev):
        for value, ref in ((0, wg_ref), (1, wu_ref)):
            @pl.when(h == value)
            def _():
                copy_of(name, ref.at[l, :, pl.ds(lo, size)], dst, dev).start()
        pending[name] = dst

    fore, aft = pl.ds(0, win // 2), pl.ds(win // 2, win // 2)

    def cd(l):
        by_matrix(l, f"cR{l}", xr_start, win // 2, gu_w.at[l, h, x, c, :, fore], right)
        by_matrix(l, f"cL{l}", xl_start, win // 2, gu_w.at[l, h, x, c, :, fore], left)

    def ce(l):
        by_matrix(l, f"dR{l}", xr_mid, win // 2, gu_w.at[l, h, x, c, :, aft], right)
        by_matrix(l, f"dL{l}", xl_mid, win // 2, gu_w.at[l, h, x, c, :, aft], left)

    def ct(l):
        by_matrix(l, f"tR{l}", xo_start, win // 2, tr_w.at[l, 0], right)
        by_matrix(l, f"tL{l}", xo_mid, win // 2, tr_w.at[l, 1], left)

    def cf(l):
        got(f"tR{l}", tr_w.at[l, 0])
        send(f"cfR{l}", [(tr_w.at[l, 0], gu_w.at[l, h, xl, c, :, fore])], right)
        got(f"tL{l}", tr_w.at[l, 1])
        send(f"cfL{l}", [(tr_w.at[l, 1], gu_w.at[l, h, xr, c, :, aft])], left)

    def c_near(l, part_name, cols):
        got(f"{part_name}R{l}", gu_w.at[l, h, xl, c, :, cols])
        got(f"{part_name}L{l}", gu_w.at[l, h, xr, c, :, cols])

    def c_far(l):
        got(f"cfR{l}", gu_w.at[l, h, xo, c, :, fore])
        got(f"cfL{l}", gu_w.at[l, h, xo, c, :, aft])

    def cn(l):
        c_near(l, "c", fore)
        to_pair(f"pcR{l}", gu_w.at[l, h, xl, c, :, fore])
        to_pair(f"pcL{l}", gu_w.at[l, h, xr, c, :, fore])

    def cm(l):
        c_near(l, "d", aft)
        to_pair(f"pdR{l}", gu_w.at[l, h, xl, c, :, aft])
        to_pair(f"pdL{l}", gu_w.at[l, h, xr, c, :, aft])

    def cx(l):
        c_far(l)
        to_pair(f"pcF{l}", gu_w.at[l, h, xo, c])

    def cu(l):
        c_near(l, "c", fore)
        c_near(l, "d", aft)
        c_far(l)
        local_wait(4 * l + 2, gu_w.at[l, :, x, c])
        view = gu_w.at[l, h, :, c]
        send(f"cT{l}", [(view, view)], twin)

    def late_half(l):
        return ("pd", aft) if l == 0 else ("pc", fore)

    def early_half(l):
        return ("pc", fore) if l == 0 else ("pd", aft)

    def cv(l):
        name, cols = early_half(l)
        got(f"{name}R{l}", gu_w.at[l, hh, xl, c, :, cols])
        got(f"{name}L{l}", gu_w.at[l, hh, xr, c, :, cols])
        got(f"pcF{l}", gu_w.at[l, hh, xo, c])
        local_wait(4 * l + 2, gu_w.at[l, :, x, c])
        views = [gu_w.at[l, hh, xx, c] for xx in (x, xo)] + [gu_w.at[l, hh, xx, c, :, cols] for xx in (xl, xr)]
        send(f"cT1{l}", [(view, view) for view in views], twin, gu_w.at[l, hh, pl.ds(0, 3), c])

    def cw(l):
        name, cols = late_half(l)
        got(f"{name}R{l}", gu_w.at[l, hh, xl, c, :, cols])
        got(f"{name}L{l}", gu_w.at[l, hh, xr, c, :, cols])
        views = [gu_w.at[l, hh, xx, c, :, cols] for xx in (xl, xr)]
        send(f"cT2{l}", [(view, view) for view in views], twin, gu_w.at[l, hh, xo, c])

    def c_ready(l):
        got(f"cT{l}", gu_w.at[l, h, :, cc])
        got(f"cT1{l}", gu_w.at[l, hh, pl.ds(0, 3), cc])
        got(f"cT2{l}", gu_w.at[l, hh, xo, cc])

    def dt(l):
        send(f"dT{l}", [(wd_ref.at[l], wd_w.at[l, wd_mine])], twin)

    def d_ready(l):
        local_wait(4 * l + 3, wd_w.at[l, wd_mine])
        got(f"dT{l}", wd_w.at[l, wd_twin])

    small = [(an_ref, an_buf), (mn_ref, mn_buf), (freq_ref, freq_buf), (pos_ref, pos_in)]
    for i, (src, dst) in enumerate(small):
        pltpu.make_async_copy(src, dst, in_sem.at[i]).start()
    barrier = pltpu.get_barrier_semaphore()
    for i in range(1, n_dev):
        pl.semaphore_signal(barrier, inc=1, device_id=(dp, lax.rem(w + i, n_dev)), device_id_type=MESH)
    pl.semaphore_signal(barrier, inc=1, device_id=pair, device_id_type=MESH)
    pl.semaphore_wait(barrier, n_dev)

    def entry(_):
        hid_copy = pltpu.make_async_copy(hid_ref, hbuf, in_sem.at[len(small)])
        hid_copy.start()
        for i in range(KV_SLOTS):
            kv_start(i, i)
        for l in range(layers):
            local_start(4 * l, a_both(l))
            local_start(4 * l + 1, [(wo_ref.at[l], bbuf_w.at[l, x, c])])
            cols = pl.ds(x_start, win)
            local_start(4 * l + 2, [(wg_ref.at[l, :, cols], gu_w.at[l, 0, x, c]), (wu_ref.at[l, :, cols], gu_w.at[l, 1, x, c])])
            local_start(4 * l + 3, [(wd_ref.at[l], wd_w.at[l, wd_mine])])
        for i, (src, dst) in enumerate(small):
            pltpu.make_async_copy(src, dst, in_sem.at[i]).wait()
        gsrc[...] = jnp.zeros_like(gsrc)
        gsrc[0:layers, 0:piece] = an_buf[...]
        gsrc[layers:2 * layers, 0:piece] = mn_buf[...]
        own_gain = pltpu.roll(gsrc[...], lax.rem(w * piece, LANES), 1)
        gsrc[...] = own_gain
        gbuf[w] = own_gain
        for l in range(layers):
            start = pl.multiple_of(jnp.where(lax.rem(x, 2) == 0, chip_cols, 0), 64)
            wd_w[l, pl.ds(start, pad), :] = jnp.zeros((pad, width), BF16)
        pos_rows[...] = jnp.broadcast_to(pos_in[...].astype(F32), (rows, rows)).T
        angles = pos_rows[...] * freq_buf[...]
        cos_buf[...] = jnp.cos(angles)
        sin_buf[...] = jnp.sin(angles)
        for i in range(1, n_dev):
            copy_of("gain", gsrc, gbuf.at[w], (dp, lax.rem(w + i, n_dev))).start()
        pending["gain"] = gbuf.at[pl.ds(0, n_dev - 1)]
        hid_copy.wait()

    def all_gains():
        tiles = []
        for j in range(width // LANES):
            total = None
            for s in range(n_dev):
                lo = (s * piece) // LANES
                for k in range(2):
                    if lo + k == j:
                        block = gbuf[s, :, k * LANES:(k + 1) * LANES]
                        total = block if total is None else total + block
            tiles.append(total)
        return 1.0 + jnp.concatenate(tiles, axis=1)

    def rms(hid, row):
        mean_sq = jnp.sum(hid * hid, axis=-1, keepdims=True) / width
        return (hid * lax.rsqrt(mean_sq + EPS) * all_gains()[row:row + 1, :]).astype(BF16)

    chunk = 4

    def attend(l, group):
        row_seq = lax.rem(lax.broadcasted_iota(jnp.int32, (LANES, cache_len), 0), SEQ_GROUP)
        place = lax.broadcasted_iota(jnp.int32, (LANES, cache_len), 1).astype(F32)
        i = l * groups + group
        slot = lax.rem(i, KV_SLOTS)
        for copy in kv_copies(i, slot):
            copy.wait()
        seqs = pl.ds(pl.multiple_of(group * SEQ_GROUP, SEQ_GROUP), SEQ_GROUP)
        query = jnp.concatenate([qbuf[j, seqs, :] for j in range(heads)], axis=0)
        scores = jnp.zeros((LANES, cache_len), F32)
        for b in range(0, SEQ_GROUP, chunk):
            prod = dot_t(query, kbuf[slot, b:b + chunk].reshape(chunk * cache_len, head_dim))
            for j in range(chunk):
                scores = jnp.where(row_seq == b + j, prod[:, j * cache_len:(j + 1) * cache_len], scores)
        k_rep = jnp.concatenate([know[l, seqs, :]] * heads, axis=0)
        v_rep = jnp.concatenate([vnow[l, seqs, :]] * heads, axis=0)
        new_score = jnp.sum(query.astype(F32) * k_rep, axis=1, keepdims=True)
        pos = jnp.concatenate([pos_rows[seqs, :]] * heads, axis=0)
        scores = jnp.where(place < pos, scores, -1e30)
        top = jnp.maximum(jnp.max(scores, axis=1, keepdims=True), new_score)
        prob = jnp.exp(scores - top)
        prob_new = jnp.exp(new_score - top)
        total = jnp.sum(prob, axis=1, keepdims=True) + prob_new
        acc = prob_new.astype(BF16).astype(F32) * v_rep
        for b in range(0, SEQ_GROUP, chunk):
            spread = jnp.concatenate([jnp.where(row_seq == b + j, prob, 0.0).astype(BF16) for j in range(chunk)], axis=1)
            acc = acc + dot(spread, vbuf[slot, b:b + chunk].reshape(chunk * cache_len, head_dim))
        attn = (acc / total).astype(BF16)
        for j in range(heads):
            abuf[seqs, j * head_dim:(j + 1) * head_dim] = attn[j * SEQ_GROUP:(j + 1) * SEQ_GROUP, :]

        @pl.when(i + KV_SLOTS < layers * groups)
        def _():
            kv_start(i + KV_SLOTS, slot)

    last = layers - 1
    exports = []

    def export(src, dst):
        pltpu.make_async_copy(src, dst, out_sem.at[len(exports)]).start()
        exports.append((src, dst))

    def qkv(l):
        a_ready(l)
        if l == 0:
            got("gain", gbuf.at[pl.ds(0, n_dev - 1)])
        cos_tab, sin_tab = cos_buf[...], sin_buf[...]
        normed = rms(hbuf[...].astype(F32), l)
        halves = [dot(normed, abuf_w[l, hf].reshape(width, a_cols)) for hf in range(2)]

        def rope(lead, tail):
            return jnp.concatenate([lead * cos_tab - tail * sin_tab, tail * cos_tab + lead * sin_tab], axis=1)

        for j in range(heads):
            out, lo = halves[j // (heads // 2)], (j % (heads // 2)) * head_dim
            qbuf[j] = (rope(out[:, lo:lo + half], out[:, lo + half:lo + head_dim]) * head_dim ** -0.5).astype(BF16)
        know[l] = rope(halves[0][:, q_half:q_half + half], halves[1][:, q_half:q_half + half]).astype(BF16).astype(F32)
        vnow[l] = jnp.concatenate([hv[:, q_half + half:q_half + 2 * half] for hv in halves], axis=1).astype(BF16).astype(F32)
        export(know.at[l], knew_ref.at[l])
        export(vnow.at[l], vnew_ref.at[l])

    r2 = rows // 2
    upper, lower = pl.ds(0, r2), pl.ds(r2, r2)

    def mix(l):
        b_ready(l)
        mixed = dot(abuf[...], bbuf_w[l].reshape(heads * head_dim, width))
        hid_mid = (hbuf[...].astype(F32) + mixed).astype(BF16)
        hbuf[...] = hid_mid
        y_all[l, x] = rms(hid_mid.astype(F32), layers + l)
        top, bottom = y_all.at[l, x, upper], y_all.at[l, x, lower]
        send(f"yR1{l}", [(top, top)], right)
        send(f"yL1{l}", [(bottom, bottom)], left)
        send(f"yR2{l}", [(bottom, bottom)], right)
        send(f"yL2{l}", [(top, top)], left)

    def yf(l):
        view = y_all.at[l, xl, upper]
        got(f"yR1{l}", view)
        send(f"yfR{l}", [(view, view)], right)
        view = y_all.at[l, xr, lower]
        got(f"yL1{l}", view)
        send(f"yfL{l}", [(view, view)], left)

    n_tile = 2 * LANES

    def gate_up(l, blocks):
        span = slice(0, len(blocks) * rows)

        def at_tile(n):
            return pl.ds(pl.multiple_of(n * n_tile, n_tile), n_tile)

        def multiply(n, slot):
            act = jnp.concatenate([y_all[l, b] for b in blocks], axis=0)
            for k in range(2):
                act_buf[slot, k, span] = dot(act, gu_w[l, k, :, :, :, at_tile(n)].reshape(width, n_tile))

        def activate(n, slot):
            mid = (jax.nn.gelu(act_buf[slot, 0, span], approximate=True) * act_buf[slot, 1, span]).astype(BF16)
            for k, b in enumerate(blocks):
                m_buf[b, :, at_tile(n)] = mid[k * rows:(k + 1) * rows]

        tiles = win // n_tile
        assert tiles % 2 == 1
        multiply(0, 0)

        @pl.loop(0, tiles // 2)
        def _(k):
            multiply(2 * k + 1, 1)
            activate(2 * k, 0)
            multiply(2 * k + 2, 0)
            activate(2 * k + 1, 1)

        activate(tiles - 1, 0)

    def guo(l):
        if l:
            c_ready(l)
        gate_up(l, (x,))

    def gua(l):
        got(f"yR2{l}", y_all.at[l, xl, lower])
        got(f"yL2{l}", y_all.at[l, xr, upper])
        if not l:
            c_ready(l)
        gate_up(l, (xl, xr))

    def gub(l):
        got(f"yfR{l}", y_all.at[l, xo, upper])
        got(f"yfL{l}", y_all.at[l, xo, lower])
        gate_up(l, (xo,))

    def down(l, xx):
        part[xx] = dot(m_buf[xx], wd_w[l])

    def near(l):
        if l:
            drain([f"{name}{l - 1}" for name in ("eR2", "eL2", "eR3", "eL3")])
        both = dot(jnp.concatenate([m_buf[xr], m_buf[xl]], axis=0), wd_w[l])
        part[xr] = both[:rows]
        part[xl] = both[rows:]
        if l == last:
            export(part.at[xr, lower], first_r.at[lower])
            export(part.at[xl, upper], first_l.at[upper])
            export(part.at[xr, upper], next_r)
            export(part.at[xl, lower], next_l)
        else:
            send(f"eR2{l}", [(part.at[xr, lower], r_f.at[l, 0, lower])], right)
            send(f"eL2{l}", [(part.at[xl, upper], r_f.at[l, 1, upper])], left)

    def far(l):
        if l:
            drain([f"{name}{l - 1}" for name in ("eR1", "eL1")])
        down(l, xo)
        if l == last:
            export(part.at[xo, upper], first_r.at[upper])
            export(part.at[xo, lower], first_l.at[lower])
        else:
            send(f"eR1{l}", [(part.at[xo, upper], r_t.at[l, 0])], right)
            send(f"eL1{l}", [(part.at[xo, lower], r_t.at[l, 1])], left)

    def er(l):
        got(f"eR1{l}", r_t.at[l, 0])
        part[xr, 0:r2] = part[xr, 0:r2] + r_t[l, 0]
        send(f"eR3{l}", [(part.at[xr, upper], r_f.at[l, 0, upper])], right)
        got(f"eL1{l}", r_t.at[l, 1])
        part[xl, r2:rows] = part[xl, r2:rows] + r_t[l, 1]
        send(f"eL3{l}", [(part.at[xl, lower], r_f.at[l, 1, lower])], left)

    def own(l):
        down(l, x)
        if l == last:
            export(part.at[x], own_out)
            export(hbuf, hid_out)

    def done(l):
        got(f"eR2{l}", r_f.at[l, 0, lower])
        got(f"eL2{l}", r_f.at[l, 1, upper])
        got(f"eR3{l}", r_f.at[l, 0, upper])
        got(f"eL3{l}", r_f.at[l, 1, lower])
        hbuf[...] = (hbuf[...].astype(F32) + (part[x] + r_f[l, 0] + r_f[l, 1])).astype(BF16)

    table = dict(
        ao=ao, af=af, ap=ap, ax=ax, at=at, aw=aw, bo=bo, bf=bf, bp=bp, bq=bq, bx=bx, bt=bt, bw=bw, cd=cd, ce=ce, ct=ct, cf=cf,
        cn=cn, cm=cm, cx=cx, cu=cu, cv=cv, cw=cw, dt=dt, **{"in": entry},
        qkv=qkv, mix=mix, yf=yf, guo=guo, gua=gua, gub=gub, dr=d_ready, near=near, far=far, er=er, own=own, done=done,
    )

    def run(step):
        table[step[:-1]](int(step[-1]))

    here = 0
    reached = [0] * layers
    while here < len(ORDER):
        step = ORDER[here]
        if not step.startswith("att"):
            run(step)
            here += 1
            continue
        l, count = int(step[-1]), 0
        while ORDER[here] == step:
            count += 1
            here += 1
        first = reached[l]
        reached[l] += count

        @pl.loop(first, first + count)
        def _(group):
            attend(l, group)

    drain(list(pending))
    for i, (src, dst) in enumerate(exports):
        pltpu.make_async_copy(src, dst, out_sem.at[i]).wait()
    assert len(msg_ids) <= send_sem.shape[0]


def decode(hidden, positions, k_cache, v_cache, attn_norm, w_query, w_key, w_value, w_out, mlp_norm, w_gate, w_up, w_down):
    layers, rows, _, cache_len, head_dim = k_cache.shape
    width = hidden.shape[1]
    n_dev = lax.axis_size("w")
    ff = w_gate.shape[-1]
    heads = w_query.shape[-1] // head_dim
    chip_cols = ff // CHIPS
    win = -(-(chip_cols + LANES // 2) // LANES) * LANES
    piece = width // n_dev
    groups = rows // SEQ_GROUP
    assert n_dev == CHIPS * CORES and heads * SEQ_GROUP == LANES and cache_len == LANES and rows == LANES
    assert lax.axis_size("dp") % 2 == 0
    inv_freq = np.float32(ROPE_BASE) ** (np.float32(-2.0) * np.arange(head_dim // 2, dtype=np.float32) / np.float32(head_dim))
    dims = (layers, rows, width, heads, head_dim, cache_len, n_dev, ff)
    anym = pl.BlockSpec(memory_space=pl.ANY)
    new_shape = jax.ShapeDtypeStruct((layers, rows, head_dim), F32)
    whole_sum = jax.ShapeDtypeStruct(hidden.shape, F32)
    half_sum = jax.ShapeDtypeStruct((rows // 2, width), F32)
    n_msg = 96
    return pl.pallas_call(
        functools.partial(decode_kernel, dims),
        out_shape=(jax.ShapeDtypeStruct(hidden.shape, BF16), new_shape, new_shape) + (whole_sum, whole_sum, half_sum, half_sum, whole_sum),
        in_specs=[anym] * 14,
        out_specs=(anym,) * 8,
        scratch_shapes=[
            pltpu.VMEM((rows, head_dim // 2), F32),
            pltpu.VMEM((rows, head_dim // 2), F32),
            pltpu.VMEM((2, 2, 2 * rows, 2 * LANES), F32),
            pltpu.VMEM(attn_norm.shape, F32),
            pltpu.VMEM(mlp_norm.shape, F32),
            pltpu.VMEM((1, head_dim // 2), F32),
            pltpu.VMEM((1, rows), jnp.int32),
            pltpu.VMEM((layers, rows, head_dim), F32),
            pltpu.VMEM((layers, rows, head_dim), F32),
            pltpu.VMEM((8, 2 * LANES), F32),
            pltpu.VMEM((n_dev, 8, 2 * LANES), F32),
            pltpu.VMEM((rows, LANES), F32),
            pltpu.VMEM((layers, 2, CHIPS, CORES, piece, w_query.shape[-1] // 2 + head_dim), BF16),
            pltpu.VMEM((layers, CHIPS, CORES, w_out.shape[1], width), BF16),
            pltpu.VMEM((layers, 2, CHIPS, CORES, piece, win), BF16),
            pltpu.VMEM((layers, win, width), BF16),
            pltpu.VMEM((layers, 2, piece, win // 2), BF16),
            pltpu.VMEM((layers, CHIPS, rows, width), BF16),
            pltpu.VMEM((CHIPS, rows, win), BF16),
            pltpu.VMEM((CHIPS, rows, width), F32),
            pltpu.VMEM((layers - 1, 2, rows // 2, width), F32),
            pltpu.VMEM((layers - 1, 2, rows, width), F32),
            pltpu.VMEM((KV_SLOTS, SEQ_GROUP, cache_len, head_dim), BF16),
            pltpu.VMEM((KV_SLOTS, SEQ_GROUP, cache_len, head_dim), BF16),
            pltpu.VMEM((heads, rows, head_dim), BF16),
            pltpu.VMEM((rows, heads * head_dim), BF16),
            pltpu.VMEM((rows, width), BF16),
            pltpu.SemaphoreType.DMA((n_msg,)),
            pltpu.SemaphoreType.DMA((n_msg,)),
            pltpu.SemaphoreType.DMA((4 * layers,)),
            pltpu.SemaphoreType.DMA((KV_SLOTS, 2)),
            pltpu.SemaphoreType.DMA((16,)),
            pltpu.SemaphoreType.DMA((8,)),
        ],
        compiler_params=pltpu.CompilerParams(collective_id=0, has_side_effects=True, vmem_limit_bytes=67043328),
        name="decode",
    )(hidden, jnp.asarray(inv_freq).reshape(1, head_dim // 2), attn_norm, mlp_norm, positions.reshape(1, rows), k_cache, v_cache, w_query, w_key, w_value, w_out, w_gate, w_up, w_down)


TILE_ROWS = 16
CACHE_BLOCK = 16


def cache_kernel(pos_ref, old_ref, new_ref, out_ref, buf, in_sem, out_sem):
    layers, rows = old_ref.shape[:2]
    blocks = rows // CACHE_BLOCK
    def load(l, b):
        i = l * blocks + b
        return pltpu.make_async_copy(old_ref.at[l, pl.ds(b * CACHE_BLOCK, CACHE_BLOCK), 0], buf.at[i], in_sem.at[i])

    def store(l, b):
        i = l * blocks + b
        return pltpu.make_async_copy(buf.at[i], out_ref.at[l, pl.ds(b * CACHE_BLOCK, CACHE_BLOCK), 0], out_sem.at[i])

    steps = [(l, b) for l in range(layers) for b in range(blocks)]
    for l, b in steps:
        load(l, b).start()
    row = lax.broadcasted_iota(jnp.int32, (TILE_ROWS, buf.shape[-1]), 0)
    for l in range(layers):
        @pl.loop(0, blocks)
        def _(b):
            load(l, b).wait()
            fresh = new_ref[l, pl.ds(pl.multiple_of(b * CACHE_BLOCK, CACHE_BLOCK), CACHE_BLOCK), :]
            tiles = []
            for s in range(CACHE_BLOCK):
                pos = pos_ref[b * CACHE_BLOCK + s]
                base = pl.multiple_of(pos // TILE_ROWS * TILE_ROWS, TILE_ROWS)
                tile = buf[l * blocks + b, s, pl.ds(base, TILE_ROWS), :].astype(F32)
                tiles.append((s, base, jnp.where(row == pos - base, fresh[s:s + 1, :], tile).astype(BF16)))
            for s, base, tile in tiles:
                buf[l * blocks + b, s, pl.ds(base, TILE_ROWS), :] = tile
    for l, b in steps:
        store(l, b).start()
    for l, b in steps:
        store(l, b).wait()


def write_cache(positions, cache, new_rows):
    cache_len, head_dim = cache.shape[-2:]
    slots = cache.shape[0] * cache.shape[1] // CACHE_BLOCK
    vmem, anym = pl.BlockSpec(memory_space=pltpu.VMEM), pl.BlockSpec(memory_space=pl.ANY)
    return pl.pallas_call(
        cache_kernel,
        out_shape=jax.ShapeDtypeStruct(cache.shape, BF16),
        in_specs=[pl.BlockSpec(memory_space=pltpu.SMEM), anym, vmem],
        out_specs=anym,
        scratch_shapes=[
            pltpu.VMEM((slots, CACHE_BLOCK, cache_len, head_dim), BF16),
            pltpu.SemaphoreType.DMA((slots,)),
            pltpu.SemaphoreType.DMA((slots,)),
        ],
        cost_estimate=pl.CostEstimate(flops=10**11, bytes_accessed=4 * cache.size, transcendentals=0),
        compiler_params=pltpu.CompilerParams(vmem_limit_bytes=60 * 2**20),
        name="cache",
    )(positions, cache, new_rows)


def solution(mesh):
    batch_spec = P(("dp", "w"))
    cache_spec = P(None, ("dp", "w"))
    gain_spec = P(None, "w")
    weight_spec = P(None, "w", None)

    def per_device(hidden, positions, k_cache, v_cache, *weights):
        hid_mid, k_new, v_new, first_r, first_l, next_r, next_l, own = decode(hidden, positions, k_cache, v_cache, *weights)
        n_dev, half = mesh.shape["w"], hidden.shape[0] // 2
        ahead = [(i, (i + CORES) % n_dev) for i in range(n_dev)]
        back = [(i, (i - CORES) % n_dev) for i in range(n_dev)]
        got_r = lax.ppermute(first_r, "w", ahead)
        got_l = lax.ppermute(first_l, "w", back)
        k_out = write_cache(positions, k_cache, k_new)
        upper = lax.ppermute(next_r + got_r[:half], "w", ahead)
        lower = lax.ppermute(next_l + got_l[half:], "w", back)
        v_out = write_cache(positions, v_cache, v_new)
        is_upper = lax.broadcasted_iota(jnp.int32, own.shape, 0) < half
        total = own + jnp.where(is_upper, got_l, got_r) + jnp.concatenate([upper, lower], axis=0)
        hidden_out = (hid_mid.astype(F32) + total).astype(BF16)
        return hidden_out, k_out, v_out

    in_specs = (batch_spec, batch_spec, cache_spec, cache_spec, gain_spec, weight_spec, weight_spec, weight_spec, weight_spec, gain_spec, weight_spec, weight_spec, weight_spec)
    out_specs = (batch_spec, cache_spec, cache_spec)
    return jax.shard_map(per_device, mesh=mesh, in_specs=in_specs, out_specs=out_specs, check_vma=False)
```
